32 devices in a mesh: clip: 2 (over x), slab: 16 (over z, y, core).
Axes of the slice: x: 2, y: 2, z: 4, core: 2. Of those that a mesh axis runs over, the one named last changes fastest.
Arguments:
- mask_field: float32 [4096, 2048], P(('clip', 'slab')), parts along dimension 0, may hold values from -1.8 to 2.9
- target_print: int32 [4096, 2048], P(('clip', 'slab')), parts along dimension 0, may hold values from 0 to 1
- source_points: int32 [32, 2], P('clip'), parts along dimension 0, may hold values from 0 to 60
- source_groups: int32 [32], P('clip'), parts along dimension 0, may hold values from 0 to 7
- group_logits: float32 [16], P('clip'), parts along dimension 0, may hold values from -1 to 1
- pupil_radius: int32 [2], P('clip'), parts along dimension 0, may hold values from 32 to 127
Outputs:
- loss_value: float32 [2], P('clip'), parts along dimension 0
- mask_grad: float32 [4096, 2048], P(('clip', 'slab')), parts along dimension 0
- group_grad: float32 [16], P('clip'), parts along dimension 0
The draws below stay inside these ranges and needn't reach their ends.
There are 2 independent parts, one for each index of `clip`. The reference program is written for one: setup_inputs(seed, part) draws one part's arguments, and reference() takes and returns one part's arrays. A program takes and returns all parts, laid end to end along the dimension named above; each array names one. Nothing has to cross between parts.
All inputs are finite; a program needn't handle non-finite values.
Results may differ from the reference program's by a relative error of at most 0.0003.
Values sent between devices are 32-bit elements; how exact they have to be, the bound alone decides.
A program may use at most 128 MiB of HBM per device.

```python
import math
import jax
import jax.numpy as jnp
from jax import lax

N = 2048
K = 256
GRID = 61
NS = 16
NG = 8


def draw_mask_field(key, part):
    keys = jax.random.split(key, 5)
    rough = jax.random.uniform(keys[0], (N, N), jnp.float32)
    amplitude = jax.random.uniform(keys[1], (16,), jnp.float32, -1.0, 1.0)
    offset = 0.5
    wave_limit = 15 * K // 32
    first_wave = jax.random.randint(keys[2], (16,), -wave_limit, wave_limit + 1)
    second_wave = jax.random.randint(keys[3], (16,), -wave_limit, wave_limit + 1)
    phase_shift = jax.random.uniform(keys[4], (16,), jnp.float32, 0.0, 2.0 * math.pi)
    row_index = jnp.arange(N, dtype=jnp.int32)[:, None]
    col_index = jnp.arange(N, dtype=jnp.int32)[None, :]
    smooth = jnp.zeros((N, N), jnp.float32)
    for member in range(16):
        wrapped = jnp.mod(first_wave[member] * row_index + second_wave[member] * col_index, N)
        angles = 2.0 * math.pi * wrapped.astype(jnp.float32) / N + phase_shift[member]
        smooth = smooth + amplitude[member] * jnp.cos(angles)
    return offset + 0.12 * smooth + 0.3 * (2.0 * rough - 1.0)


def draw_target_print(key, part):
    row_index = jnp.arange(N, dtype=jnp.int32)[:, None]
    numbers = jax.random.randint(key, (N, N), 0, 1000)
    limit = 200 + 600 * row_index // N
    return (numbers < limit).astype(jnp.int32)


def with_ends(values, key, low, top_value):
    longest = values.shape.index(max(values.shape))
    spots = []
    for shift in (0, 1):
        where = [jax.random.randint(jax.random.fold_in(key, axis), (), 0, length) for axis, length in enumerate(values.shape)]
        where[longest] = (where[longest] + shift) % values.shape[longest]
        spots.append(tuple(where))
    return values.at[spots[0]].set(low).at[spots[1]].set(top_value)


def setup_inputs(seed: int = 0, part: int = 0) -> dict:
    key_of = jax.random.split(jax.random.key(seed), 7)
    part_keys = jax.random.split(jax.random.fold_in(key_of[6], part), 7)
    mask_field = draw_mask_field(jax.random.fold_in(jax.random.fold_in(key_of[6], part), 71), part)
    target_print = draw_target_print(jax.random.fold_in(jax.random.fold_in(key_of[6], part), 71), part)
    source_points = with_ends(jax.random.randint(part_keys[2], (NS, 2), 0, GRID), jax.random.fold_in(part_keys[2], 1), 0, GRID - 1).astype(jnp.int32)
    source_groups = with_ends(jax.random.randint(part_keys[3], (NS,), 0, NG), jax.random.fold_in(part_keys[3], 1), 0, NG - 1).astype(jnp.int32)
    group_logits = jnp.clip(jax.random.uniform(part_keys[4], (NG,), jnp.float32, -1.0, 1.0), -1.0, 1.0)
    pupil_radius = jax.random.randint(part_keys[5], (1,), K // 8, K // 2).astype(jnp.int32)
    return {"mask_field": mask_field, "target_print": target_print, "source_points": source_points, "source_groups": source_groups, "group_logits": group_logits, "pupil_radius": pupil_radius}


steepness = 8.0
threshold = 0.3
shift_scale = 45

def reference(mask_field, target_print, source_points, source_groups, group_logits, pupil_radius):
    half_band = K // 2
    frequency = jnp.arange(K, dtype=jnp.int32) - half_band
    band_index = jnp.mod(frequency, N).astype(jnp.int32)
    cutoff = pupil_radius[0].astype(jnp.int32)
    shifted = (source_points.astype(jnp.int32) - GRID // 2) * cutoff // shift_scale
    desired = target_print.astype(mask_field.dtype)

    def objective(field, logits):
        spectrum = jnp.fft.fft2(field)
        band = jnp.take(jnp.take(spectrum, band_index, axis=0), band_index, axis=1)
        weights = jnp.exp(logits[source_groups])
        total_weight = jnp.sum(weights)

        def add_source(running, source_item):
            offset, weight = source_item
            first_axis = frequency[:, None] + offset[0]
            second_axis = frequency[None, :] + offset[1]
            passed = first_axis * first_axis + second_axis * second_axis <= cutoff * cutoff
            clipped = jnp.where(passed, band, jnp.zeros_like(band))
            embedded = jnp.zeros((N, N), band.dtype).at[band_index[:, None], band_index[None, :]].set(clipped)
            image_field = jnp.fft.ifft2(embedded)
            bright = jnp.real(image_field) * jnp.real(image_field) + jnp.imag(image_field) * jnp.imag(image_field)
            return (running + weight * bright, None)
        running, unused = lax.scan(add_source, jnp.zeros((N, N), field.dtype), (shifted, weights))
        intensity = running / total_weight
        resist = jax.nn.sigmoid(steepness * (intensity - threshold))
        misfit = resist - desired
        return jnp.sum(misfit * misfit)
    total_sq, pullback = jax.vjp(objective, mask_field, group_logits)
    mask_grad, logit_grad = pullback(jnp.ones_like(total_sq))
    norming = 1.0 / (N * N)
    return ((total_sq * norming).reshape(1), mask_grad, logit_grad * norming)
```

```python
import functools
import math

import jax
import jax.numpy as jnp
import numpy as np
from jax import lax
from jax.experimental import pallas as pl
from jax.experimental.pallas import tpu as pltpu
from jax.sharding import PartitionSpec as P

K = 256
GRID = 61
NG = 8

steepness = 8.0
threshold = 0.3
shift_scale = 45
F32 = jnp.float32
BF16 = jnp.bfloat16
LANES = 128
SUB = 8


def angles(left, right, length):
    turns = np.mod(np.asarray(left)[:, None] * np.asarray(right)[None, :], length)
    return 2.0 * math.pi * turns.astype(np.float64) / length


def halves(table):
    table = np.asarray(table, np.float32)
    high = table.astype(BF16)
    low = (table - high.astype(np.float32)).astype(BF16)
    return np.stack([high, low])


def split(value):
    high = value.astype(BF16)
    return high, (value - high.astype(F32)).astype(BF16)


def product(left, right, flip=False):
    dims = (((1,), (1 if flip else 0,)), ((), ()))
    one = lambda a, b: lax.dot_general(a, b, dims, preferred_element_type=F32)
    return one(left[0], right[0]) + one(left[1], right[0]) + one(left[0], right[1])


def tables(n, rows, devices):
    h = K // 2
    coarse = 2 * K
    step = n // coarse
    freq = np.arange(h)
    near = np.arange(rows)
    wave_y = angles(freq, np.arange(n), n)
    wave_y = np.concatenate([np.cos(wave_y), np.sin(wave_y)], 0)
    wave_x = angles(near, freq, n)
    wave_x = np.concatenate([np.cos(wave_x), np.sin(wave_x)], 1)
    half_x = angles(near, 2 * freq + 1, 2 * n)
    half_x = np.concatenate([np.cos(half_x), -np.sin(half_x)], 1)
    half_y = angles(2 * freq + 1, step * np.arange(coarse), 2 * n)
    half_y = np.concatenate([np.cos(half_y), np.sin(half_y)], 0)
    far = angles(rows * np.arange(devices), freq, n)
    far = np.stack([np.cos(far), np.sin(far)])[:, :, None, :].astype(np.float32)
    half_far = angles(rows * np.arange(devices), 2 * freq + 1, 2 * n)
    half_far = np.stack([np.cos(half_far), np.sin(half_far)]) / (n * n)
    half_far = half_far[:, :, None, :].astype(np.float32)
    block = 2 * LANES
    extra = n // step - block // step
    lag = np.mod(np.arange(block)[None, :] - step * (np.arange(coarse + extra) - extra)[:, None], n)
    kernel = np.ones(n)
    for f in range(1, K):
        kernel += 2.0 * np.cos(2.0 * math.pi * np.mod(f * np.arange(n), n) / n)
    up = (kernel / coarse)[lag]
    edge = angles([h], np.arange(LANES), n)
    edge = np.concatenate([np.cos(edge), np.sin(edge)], 0)
    edge = np.concatenate([edge, np.zeros((SUB - 2, LANES))], 0)
    return {
        "wave_y": halves(wave_y),
        "wave_x": halves(wave_x),
        "half_x": halves(half_x),
        "half_xt": halves(half_x.T),
        "half_y": halves(half_y),
        "half_yt": halves(half_y.T),
        "up": halves(up),
        "far": far,
        "half_far": half_far,
        "edge": edge.astype(np.float32),
    }


NAMES = ("wave_y", "wave_x", "half_x", "half_xt", "half_y", "half_yt", "up", "far", "half_far", "edge")


def kernel(devices, n, *refs):
    points, groups, logits, radius, mask_hbm, target_hbm = refs[:6]
    sources_in = dict(zip(NAMES, refs[6 : 6 + len(NAMES)]))
    refs = refs[6 + len(NAMES) :]
    loss_ref, grad_hbm, group_ref = refs[:3]
    refs = refs[3:]
    tab = dict(zip(NAMES, refs[: len(NAMES)]))
    refs = refs[len(NAMES) :]
    (mask, target, rows_t, edge_out, rows_in, edge_in, chunk, edge_all, ext, band, data, fields, image, pull,
     grads, grad_t, edge_back, grad_in, edge_back_in, edge_back_all, back_rows, back_in, spread, out,
     local_sem, out_sem, send_sem, recv_sem) = refs
    h = K // 2
    coarse = 2 * K
    sources = points.shape[0]
    rows = mask.shape[0]
    block = 2 * LANES
    blocks = n // block
    step = n // coarse
    me = lax.axis_index("slab")
    norming = 1.0 / (n * n)

    loads = {}
    for i, (name, src, dst) in enumerate(
        [("mask", mask_hbm, mask), ("wave_y", sources_in["wave_y"], tab["wave_y"])]
        + [(k, sources_in[k], tab[k]) for k in ("edge", "wave_x", "far", "half_far", "half_x", "half_y")]
        + [("up", sources_in["up"], tab["up"]), ("target", target_hbm, target)]
        + [(k, sources_in[k], tab[k]) for k in ("half_yt", "half_xt")]
    ):
        loads[name] = pltpu.make_async_copy(src, dst, local_sem.at[i])
        loads[name].start()

    barrier = pltpu.get_barrier_semaphore()

    def greet(i, carry):
        pl.semaphore_signal(barrier, inc=1, device_id={"slab": lax.rem(me + i, devices)})
        return carry

    lax.fori_loop(1, devices, greet, 0)

    def both(name):
        return tab[name][0], tab[name][1]

    def copy_to(phase, peer, src, dst):
        return pltpu.make_async_remote_copy(
            src_ref=src, dst_ref=dst, send_sem=send_sem.at[phase, peer], recv_sem=recv_sem.at[phase, me],
            device_id={"slab": peer},
        )

    def send_all(phase, src_of, dst):
        def body(i, carry):
            peer = lax.rem(me + i, devices)
            copy_to(phase, peer, src_of(peer), dst).start()
            return carry

        lax.fori_loop(1, devices, body, 0)

    def wait_all(phase, src, dst_of):
        def body(i, carry):
            peer = lax.rem(me + i, devices)
            pltpu.make_async_remote_copy(
                src_ref=src, dst_ref=dst_of(peer), send_sem=send_sem.at[phase, peer],
                recv_sem=recv_sem.at[phase, peer], device_id={"slab": peer},
            ).wait_recv()
            return carry

        lax.fori_loop(1, devices, body, 0)

    def drain(phase, src, dst):
        def body(i, carry):
            peer = lax.rem(me + i, devices)
            copy_to(phase, peer, src, dst).wait_send()
            return carry

        lax.fori_loop(1, devices, body, 0)

    lane = lax.broadcasted_iota(jnp.int32, (1, LANES), 1)

    def column(row):
        return jnp.broadcast_to(row, (LANES, LANES)).T

    logit_row = jnp.full((1, LANES), 0.0, F32)
    group_row = jnp.full((1, LANES), -1, jnp.int32)
    for s in range(sources):
        g = groups[s]
        logit_row = jnp.where(lane == s, logits[g], logit_row)
        group_row = jnp.where(lane == s, g, group_row)
    weight_row = jnp.where(lane < sources, jnp.exp(logit_row), 0.0)
    share_row = weight_row / jnp.sum(weight_row, axis=1, keepdims=True)

    loads["mask"].wait()
    loads["wave_y"].wait()
    transformed = product(split(mask[...]), both("wave_y"), flip=True)
    rows_t[0] = transformed[:, :h].T
    rows_t[1] = transformed[:, h:].T
    loads["edge"].wait()
    loads["wave_x"].wait()
    loads["far"].wait()
    edge_rows = tab["edge"][...]
    edge_pair = split(edge_rows)
    summed = mask[:, :LANES]
    for b in range(1, n // LANES):
        summed = summed + mask[:, b * LANES : (b + 1) * LANES]
    side_x = product(edge_pair, split(transformed))
    last = product(edge_pair, split(summed), flip=True)
    side_y = product(split(last), both("wave_x"))
    far_c, far_s = tab["far"][0, me], tab["far"][1, me]
    side_c = far_c * side_y[:2, :h] - far_s * side_y[:2, h:]
    side_s = far_s * side_y[:2, :h] + far_c * side_y[:2, h:]

    def mixes(cc, cs, sc, ss):
        return cc - ss, cc + ss, sc + cs, sc - cs

    edges = mixes(side_x[0:1, :h], side_x[0:1, h:], side_x[1:2, :h], side_x[1:2, h:])
    edges = edges + mixes(side_c[0:1], side_c[1:2], side_s[0:1], side_s[1:2])

    def lane_sum(value):
        return jnp.sum(value, axis=1, keepdims=True)

    corner = mixes(
        lane_sum(last[0:1] * edge_rows[0:1]), lane_sum(last[1:2] * edge_rows[0:1]),
        lane_sum(last[0:1] * edge_rows[1:2]), lane_sum(last[1:2] * edge_rows[1:2]),
    )
    corner_row = jnp.zeros((1, LANES), F32)
    for i in range(4):
        corner_row = jnp.where(lane == i, corner[i], corner_row)
    for i in range(8):
        edge_out[i] = edges[i]
    edge_out[8] = corner_row
    for i in range(9, devices):
        edge_out[i] = jnp.zeros((1, LANES), F32)

    pl.semaphore_wait(barrier, devices - 1)
    send_all(0, lambda p: rows_t.at[:, pl.ds(p * SUB, SUB), :], rows_in.at[me])
    send_all(1, lambda p: edge_out.at[p], edge_in.at[me])
    rows_in[me] = rows_t[:, pl.ds(me * SUB, SUB), :]
    edge_in[me] = edge_out[me]

    wait_all(0, rows_t.at[:, pl.ds(0, SUB), :], lambda p: rows_in.at[p])
    gathered = rows_in[...].reshape(devices * 2 * SUB, rows)
    turned = product(split(gathered), both("wave_x")).reshape(devices, 2 * SUB, 2 * h)
    far_c, far_s = tab["far"][0], tab["far"][1]
    turned_c, turned_s = turned[:, :, :h], turned[:, :, h:]
    sum_c = jnp.sum(far_c * turned_c - far_s * turned_s, 0)
    sum_s = jnp.sum(far_s * turned_c + far_c * turned_s, 0)
    for i, value in enumerate(mixes(sum_c[:SUB], sum_c[SUB:], sum_s[:SUB], sum_s[SUB:])):
        chunk[me, i] = value
    send_all(2, lambda p: chunk.at[me], chunk.at[me])
    wait_all(1, edge_out.at[0], lambda p: edge_in.at[p])
    edge_all[me] = jnp.sum(edge_in[...], 0)
    send_all(3, lambda p: edge_all.at[me], edge_all.at[me])

    loads["half_far"].wait()
    loads["half_x"].wait()
    loads["half_y"].wait()
    turn_c = column(tab["half_far"][0, me])
    turn_s = column(tab["half_far"][1, me])

    wait_all(2, chunk.at[me], lambda p: chunk.at[p])
    wait_all(3, edge_all.at[me], lambda p: edge_all.at[p])
    shifted = []
    plain = []
    for i in range(4):
        ext[:h, :h] = chunk[:, i].reshape(h, h).T
        ext[h : h + 1, :h] = edge_all[i]
        ext[:h, h:] = column(edge_all[4 + i])
        ext[h : h + 1, h:] = jnp.broadcast_to(lane_sum(jnp.where(lane == i, edge_all[8], 0.0)), (1, LANES))
        plain = ext[...]
        moved = pltpu.roll(plain, 2 * h - 1, 1)
        if i in (0, 2):
            first, second = ext[:h, :h], None
            ext[...] = moved
            second = ext[1 : h + 1, :h]
        else:
            second = ext[1 : h + 1, :h]
            ext[...] = moved
            first = ext[:h, :h]
        data[i, 0] = first
        data[i, 1] = second

    def turn(slot, re, im, sign):
        s = turn_s if sign > 0 else -turn_s
        band[slot, 0] = re * turn_c - im * s
        band[slot, 1] = re * s + im * turn_c

    turn(0, data[0, 0], -data[2, 0], 1)
    turn(1, data[1, 0], -data[3, 0], 1)
    turn(2, data[1, 1], data[3, 1], -1)
    turn(3, data[0, 1], data[2, 1], -1)

    cutoff = radius[0]
    limit = (cutoff * cutoff).astype(F32)
    row_index = lax.broadcasted_iota(jnp.int32, (h, h), 0).astype(F32)
    lane_index = lane.astype(F32)

    def masks(s):
        first = ((points[s, 0] - GRID // 2) * cutoff // shift_scale).astype(F32)
        second = ((points[s, 1] - GRID // 2) * cutoff // shift_scale).astype(F32)
        row_p, row_m = row_index + first, first - 1.0 - row_index
        col_p, col_m = lane_index + second, second - 1.0 - lane_index
        room_p, room_m = limit - row_p * row_p, limit - row_m * row_m
        col_p, col_m = col_p * col_p, col_m * col_m
        return col_p <= room_p, col_m <= room_p, col_p <= room_m, col_m <= room_m

    def share_of(s):
        return lane_sum(jnp.where(lane == s, share_row, 0.0))

    image[...] = jnp.zeros_like(image)

    def forward(s, carry):
        kept = masks(s)
        quads = []
        for part in range(2):
            pp, pm, mp, mm = (jnp.where(kept[q], band[q, part], 0.0) for q in range(4))
            ep, op, em, om = pp + mp, pp - mp, pm + mm, pm - mm
            quads.append((ep + em, ep - em, op + om, op - om))
        (ee_r, eo_r, oe_r, oo_r), (ee_i, eo_i, oe_i, oo_i) = quads
        top = jnp.concatenate([ee_r, -eo_i, ee_i, eo_r], 1)
        low = jnp.concatenate([oe_i, oo_r, -oe_r, oo_i], 1)
        wide = product(both("half_x"), split(jnp.concatenate([top, low], 0)))
        wide = jnp.concatenate([wide[:, : 2 * h], wide[:, 2 * h :]], 0)
        field = product(split(wide), both("half_y"))
        fields[s] = field
        re, im = field[:rows], field[rows:]
        image[...] += share_of(s) * (re * re + im * im)
        return carry

    lax.fori_loop(0, sources, forward, 0)

    loads["up"].wait()
    loads["target"].wait()
    pull[...] = jnp.zeros_like(pull)
    squares = jnp.zeros((rows, LANES), F32)
    image_pair = split(image[...])
    extra = (n - block) // step
    for b in range(blocks):
        start = extra - b * (block // step)
        up = (tab["up"][0, start : start + coarse, :], tab["up"][1, start : start + coarse, :])
        intensity = product(image_pair, up)
        resist = 1.0 / (1.0 + jnp.exp(-steepness * (intensity - threshold)))
        misfit = resist - target[:, b * block : (b + 1) * block].astype(F32)
        slope = (2.0 * steepness) * misfit * resist * (1.0 - resist)
        square = misfit * misfit
        squares = squares + square[:, :LANES] + square[:, LANES:]
        pull[...] += product(split(slope), up, flip=True)
    squares = lane_sum(jnp.sum(squares, 0, keepdims=True))

    loads["half_yt"].wait()
    loads["half_xt"].wait()
    grads[...] = jnp.zeros_like(grads)

    def backward(s, sums):
        kept = masks(s)
        re, im = fields[s, :rows], fields[s, rows:]
        weak = pull[...]
        down_r, down_i = weak * re, weak * im
        total = lane_sum(jnp.sum(down_r * re + down_i * im, 0, keepdims=True))
        sums = jnp.where(lane == s, total, sums)
        scale = 2.0 * share_of(s)
        back = jnp.concatenate([down_r, down_i], 0)
        settle = product(split(back), both("half_yt")) * scale
        settle = jnp.concatenate([settle[:rows], settle[rows:]], 1)
        full = product(both("half_xt"), split(settle))
        ee_r, eo_i, ee_i, eo_r = full[:h, :h], -full[:h, h : 2 * h], full[:h, 2 * h : 3 * h], full[:h, 3 * h :]
        oe_i, oo_r, oe_r, oo_i = full[h:, :h], full[h:, h : 2 * h], -full[h:, 2 * h : 3 * h], full[h:, 3 * h :]
        for part, (ee, eo, oe, oo) in enumerate(((ee_r, eo_r, oe_r, oo_r), (ee_i, eo_i, oe_i, oo_i))):
            ep, em, op, om = ee + eo, ee - eo, oe + oo, oe - oo
            for q, value in enumerate((ep + op, em + om, ep - op, em - om)):
                grads[q, part] += jnp.where(kept[q], value, 0.0)
        return sums

    sums = lax.fori_loop(0, sources, backward, jnp.zeros((1, LANES), F32))
    sums = jnp.where(lane == sources, squares, sums)

    def unturn(slot, sign):
        s = turn_s if sign > 0 else -turn_s
        re, im = grads[slot, 0], grads[slot, 1]
        return re * turn_c + im * s, im * turn_c - re * s

    pp, pm, mp, mm = unturn(0, 1), unturn(1, 1), unturn(2, -1), unturn(3, -1)
    pieces = ((pp[0], mm[0]), (pm[0], mp[0]), (-pp[1], mm[1]), (-pm[1], mp[1]))
    last_row = jnp.zeros((1, LANES), F32)
    for i, (first, second) in enumerate(pieces):
        ext[...] = jnp.zeros_like(ext)
        if i in (0, 2):
            ext[1 : h + 1, :h] = second
            moved = pltpu.roll(ext[...], 1, 1)
            ext[...] = moved
            ext[:h, :h] += first
        else:
            ext[:h, :h] = first
            moved = pltpu.roll(ext[...], 1, 1)
            ext[...] = moved
            ext[1 : h + 1, :h] += second
        grad_t[i] = ext[:h, :h].T
        edge_back[i] = ext[h : h + 1, :h]
        edge_back[4 + i] = ext[:h, h:].T[0:1, :]
        last_row = jnp.where(lane == i, ext[h : h + 1, h : h + 1], last_row)
    edge_back[8] = last_row
    edge_back[9] = sums
    for i in range(10, devices):
        edge_back[i] = jnp.zeros((1, LANES), F32)

    send_all(4, lambda p: grad_t.at[:, pl.ds(p * SUB, SUB), :], grad_in.at[me])
    send_all(5, lambda p: edge_back.at[p], edge_back_in.at[me])
    grad_in[me] = grad_t[:, pl.ds(me * SUB, SUB), :]
    edge_back_in[me] = edge_back[me]
    wait_all(4, grad_t.at[:, pl.ds(0, SUB), :], lambda p: grad_in.at[p])

    def unmix(u, v, wp, wm):
        return u + v, wp - wm, wp + wm, v - u

    mine = jnp.sum(grad_in[...], 0)
    cc, cs, sc, ss = unmix(mine[0], mine[1], mine[2], mine[3])
    sum_c = jnp.concatenate([cc, cs], 0)[None]
    sum_s = jnp.concatenate([sc, ss], 0)[None]
    back_c = far_c * sum_c + far_s * sum_s
    back_s = far_c * sum_s - far_s * sum_c
    turned = jnp.concatenate([back_c, back_s], 2).reshape(devices * 2 * SUB, 2 * h)
    gathered = product(split(turned), both("wave_x"), flip=True)
    back_rows[...] = gathered.reshape(devices, 2, SUB, rows)
    send_all(6, lambda p: back_rows.at[p], back_in.at[:, pl.ds(me * SUB, SUB), :])
    back_in[:, pl.ds(me * SUB, SUB), :] = back_rows[me]
    wait_all(5, edge_back.at[0], lambda p: edge_back_in.at[p])
    edge_back_all[me] = jnp.sum(edge_back_in[...], 0)
    send_all(7, lambda p: edge_back_all.at[me], edge_back_all.at[me])
    wait_all(7, edge_back_all.at[me], lambda p: edge_back_all.at[p])

    sums = edge_back_all[9]
    loss_ref[0] = jnp.sum(jnp.where(lane == sources, sums, 0.0)) * norming
    sums = jnp.where(lane < sources, sums, 0.0)
    source_pull = share_row * (sums - lane_sum(share_row * sums))
    for g in range(NG):
        group_ref[g] = jnp.sum(jnp.where(group_row == g, source_pull, 0.0)) * norming

    side_x = unmix(*(edge_back_all[i] for i in range(4)))
    side_y = unmix(*(edge_back_all[4 + i] for i in range(4)))
    corner = unmix(*(lane_sum(jnp.where(lane == i, edge_back_all[8], 0.0)) for i in range(4)))
    far_c, far_s = tab["far"][0, me], tab["far"][1, me]
    near = []
    for c, s in ((side_y[0], side_y[2]), (side_y[1], side_y[3])):
        near.append(jnp.concatenate([far_c * c + far_s * s, far_c * s - far_s * c], 1))
    near = jnp.concatenate(near + [jnp.zeros((SUB - 2, 2 * h), F32)], 0)
    last = product(split(near), both("wave_x"), flip=True)
    edge_c, edge_s = edge_rows[0:1], edge_rows[1:2]
    last_c = last[0:1] + corner[0] * edge_c + corner[2] * edge_s
    last_s = last[1:2] + corner[1] * edge_c + corner[3] * edge_s
    spread[...] = column(last_c) * edge_c + column(last_s) * edge_s
    col_c, col_s = column(edge_c), column(edge_s)

    wait_all(6, back_rows.at[0], lambda p: back_in.at[:, pl.ds(p * SUB, SUB), :])
    part_c = back_in[0].T + col_c * side_x[0] + col_s * side_x[2]
    part_s = back_in[1].T + col_c * side_x[1] + col_s * side_x[3]
    pair = split(jnp.concatenate([part_c, part_s], 1))
    adds = jnp.concatenate([spread[...], spread[...]], 1)
    stores = []
    for b in range(blocks):
        where = slice(b * block, (b + 1) * block)
        out[:, where] = product(pair, (tab["wave_y"][0, :, where], tab["wave_y"][1, :, where])) + adds
        stores.append(pltpu.make_async_copy(out.at[:, where], grad_hbm.at[:, where], out_sem.at[b]))
        stores[-1].start()
    drain(0, rows_t.at[:, pl.ds(0, SUB), :], rows_in.at[me])
    drain(1, edge_out.at[0], edge_in.at[me])
    drain(2, chunk.at[me], chunk.at[me])
    drain(3, edge_all.at[me], edge_all.at[me])
    drain(4, grad_t.at[:, pl.ds(0, SUB), :], grad_in.at[me])
    drain(5, edge_back.at[0], edge_back_in.at[me])
    drain(6, back_rows.at[0], back_in.at[:, pl.ds(0, SUB), :])
    drain(7, edge_back_all.at[me], edge_back_all.at[me])
    for store in stores:
        store.wait()


def fused(devices, mask_field, target_print, source_points, source_groups, group_logits, pupil_radius):
    rows, n = mask_field.shape
    h = K // 2
    coarse = 2 * K
    sources = source_points.shape[0]
    consts = tables(n, rows, devices)
    smem = pl.BlockSpec(memory_space=pltpu.SMEM)
    anywhere = pl.BlockSpec(memory_space=pl.ANY)
    vmem = lambda *shape: pltpu.VMEM(shape, F32)
    scratch = [pltpu.VMEM(consts[k].shape, consts[k].dtype) for k in NAMES] + [
        vmem(rows, n), pltpu.VMEM((rows, n), jnp.int32),
        vmem(2, h, rows), vmem(devices, 1, LANES), vmem(devices, 2, SUB, rows), vmem(devices, 1, LANES),
        vmem(devices, 4, SUB, h), vmem(devices, 1, LANES), vmem(h + SUB, 2 * h), vmem(4, 2, h, h),
        vmem(4, 2, h, h), vmem(sources, 2 * rows, coarse), vmem(rows, coarse), vmem(rows, coarse),
        vmem(4, 2, h, h), vmem(4, h, h), vmem(devices, 1, LANES), vmem(devices, 4, SUB, h),
        vmem(devices, 1, LANES), vmem(devices, 1, LANES), vmem(devices, 2, SUB, rows), vmem(2, h, rows),
        vmem(rows, LANES), vmem(rows, n),
        pltpu.SemaphoreType.DMA((12,)), pltpu.SemaphoreType.DMA((n // (2 * LANES),)),
        pltpu.SemaphoreType.DMA((8, devices)), pltpu.SemaphoreType.DMA((8, devices)),
    ]
    return pl.pallas_call(
        functools.partial(kernel, devices, n),
        out_shape=(
            jax.ShapeDtypeStruct((1,), F32),
            jax.ShapeDtypeStruct((rows, n), F32),
            jax.ShapeDtypeStruct((NG,), F32),
        ),
        in_specs=[smem] * 4 + [anywhere] * (2 + len(NAMES)),
        out_specs=(smem, anywhere, smem),
        scratch_shapes=scratch,
        compiler_params=pltpu.CompilerParams(
            collective_id=0, has_side_effects=True, vmem_limit_bytes=60 * 1024 * 1024
        ),
    )(source_points, source_groups, group_logits, pupil_radius, mask_field, target_print,
      *(jnp.asarray(consts[k]) for k in NAMES))


HIGH = lax.Precision.HIGH


def dot(form, left, right):
    return jnp.einsum(form, left, right, precision=HIGH, preferred_element_type=F32)


def waves(left, right, length):
    turns = angles(left, right, length)
    return np.cos(turns), np.sin(turns)


def shifted_waves(count, freq, length, device, devices):
    near = np.stack(waves(np.arange(count), freq, length)).astype(np.float32)
    far = np.stack(waves(np.arange(devices) * count, freq, length)).astype(np.float32)
    far = lax.dynamic_slice_in_dim(jnp.asarray(far), device, 1, axis=1)
    return far[0] * near[0] - far[1] * near[1], far[1] * near[0] + far[0] * near[1]


def exchange(blocks):
    return lax.all_to_all(blocks, "slab", 0, 0)


def plain(devices, mask_field, target_print, source_points, source_groups, group_logits, pupil_radius):
    rows, n = mask_field.shape
    sources = source_points.shape[0]
    coarse = 2 * K
    step = n // coarse
    cols = coarse // devices
    half = n // 2
    device = lax.axis_index("slab")
    freq = np.arange(K, dtype=np.int64) - K // 2
    order = np.concatenate([freq[freq % 2 == 0], freq[freq % 2 == 1]])
    kh = K // 2
    norming = 1.0 / (n * n)

    cos_y, sin_y = waves(np.arange(half), order, n)
    fold = [
        jnp.asarray(np.concatenate([t[:, p * kh : (p + 1) * kh] for t in (cos_y, sin_y)], 1), F32)
        for p in (0, 1)
    ]
    lag = np.mod(np.arange(n)[None, :] - step * np.arange(coarse)[:, None], n)
    response = np.zeros(n)
    for f in range(1, K):
        response += 2.0 * np.cos(2.0 * math.pi * np.mod(f * np.arange(n), n) / n)
    response = (response + 1.0) / coarse
    up = jnp.asarray(response[lag], F32)
    cos_c, sin_c = waves(freq, np.arange(coarse), coarse)
    wave_x = jnp.asarray(np.concatenate([cos_c, sin_c], 1), F32)
    loc_c, loc_s = shifted_waves(rows, freq, n, device, devices)
    loc = jnp.concatenate([loc_c, loc_s], 1)
    a, b = shifted_waves(cols, order, coarse, device, devices)
    lift = jnp.concatenate([jnp.concatenate([a, -b], 1), jnp.concatenate([b, a], 1)], 0)

    cutoff = pupil_radius[0]
    shifted = (source_points - GRID // 2) * cutoff // shift_scale
    first = jnp.asarray(freq, jnp.int32)[None, None, :] + shifted[:, 0, None, None]
    second = jnp.asarray(np.tile(order, 2), jnp.int32)[None, :, None] + shifted[:, 1, None, None]
    passed = first * first + second * second <= cutoff * cutoff

    near, away = mask_field[:, :half], mask_field[:, half:]
    even = dot("xy,yq->xq", near + away, fold[0])
    odd = dot("xy,yq->xq", near - away, fold[1])
    part_c = jnp.concatenate([even[:, :kh], odd[:, :kh]], 1)
    part_s = jnp.concatenate([even[:, kh:], odd[:, kh:]], 1)
    spec = dot("xq,xk->qk", jnp.concatenate([part_c, part_s], 1), loc)
    band = jnp.concatenate([spec[:K, :K] - spec[K:, K:], -(spec[:K, K:] + spec[K:, :K])], 0)
    band = jnp.sum(exchange(band.reshape(devices, 2 * K // devices, K)), 0)
    band = lax.all_gather(band, "slab", tiled=True)

    kept = jnp.where(passed, band[None], 0.0)
    wide = dot("aq,sqk->sak", lift, kept)
    both = dot("ak,kx->ax", wide.reshape(sources * 2 * cols, K), wave_x)
    both = both.reshape(sources, 2, cols, 2 * coarse)
    field_re = (both[:, 0, :, :coarse] - both[:, 1, :, coarse:]) * norming
    field_im = (both[:, 0, :, coarse:] + both[:, 1, :, :coarse]) * norming
    bright = field_re * field_re + field_im * field_im
    onehot = (source_groups[:, None] == jnp.arange(NG, dtype=jnp.int32)[None, :]).astype(F32)
    weights = jnp.exp(jnp.sum(onehot * group_logits[None, :], 1))
    share = weights / jnp.sum(weights)
    image = jnp.sum(share[:, None, None] * bright, 0)

    tall = dot("cm,mx->cx", image, up)
    tall = lax.all_to_all(tall, "slab", 1, 0, tiled=True)
    intensity = dot("cx,cy->xy", tall, up)
    resist = jax.nn.sigmoid(steepness * (intensity - threshold))
    misfit = resist - target_print.astype(F32)
    slope = (2.0 * steepness) * misfit * resist * (1.0 - resist)
    squares = jnp.sum(misfit * misfit)
    down = dot("xy,cy->cx", slope, up)
    down = lax.all_to_all(down, "slab", 0, 1, tiled=True)
    pull = dot("cx,mx->cm", down, up)

    per_source = jnp.sum(bright * pull[None], (1, 2))
    sums = jnp.concatenate([per_source, squares[None]])
    factor = (2.0 * norming) * share[:, None, None] * pull[None]
    back = jnp.stack([factor * field_re, factor * field_im], 1)
    low = dot("ax,kx->ak", back.reshape(sources * 2 * cols, coarse), wave_x[:, :coarse])
    lows = dot("ax,kx->ak", back.reshape(sources * 2 * cols, coarse), wave_x[:, coarse:])
    low = low.reshape(sources, 2, cols, K)
    lows = lows.reshape(sources, 2, cols, K)
    settle = jnp.concatenate([low[:, 0] + lows[:, 1], low[:, 1] - lows[:, 0]], 1)
    settle = dot("aq,sak->sqk", lift, settle)
    grad_band = jnp.sum(jnp.where(passed, settle, 0.0), 0).reshape(devices, 2 * K // devices, K)
    extra = jnp.pad(sums[None, :], ((0, 7), (0, K - sources - 1)))
    extra = jnp.broadcast_to(extra[None], (devices, 8, K))
    grad_band = jnp.sum(exchange(jnp.concatenate([grad_band, extra], 1)), 0)
    sums = grad_band[-8, : sources + 1]
    grad_band = lax.all_gather(grad_band[:-8], "slab", tiled=True)
    per_source, squares = sums[:-1], sums[-1]
    loss_value = (squares * norming).reshape(1)
    against = jnp.sum(share * per_source)
    source_pull = share * (per_source - against)
    group_grad = jnp.sum(onehot * source_pull[:, None], 0) * norming

    spread = dot("tk,qk->tq", jnp.concatenate([loc_c, loc_s], 0), grad_band)
    spread_re = spread[:rows, :K] - spread[rows:, K:]
    spread_im = spread[:rows, K:] + spread[rows:, :K]
    even = dot("xq,yq->xy", jnp.concatenate([spread_re[:, :kh], -spread_im[:, :kh]], 1), fold[0])
    odd = dot("xq,yq->xy", jnp.concatenate([spread_re[:, kh:], -spread_im[:, kh:]], 1), fold[1])
    mask_grad = jnp.concatenate([even + odd, even - odd], 1)
    return loss_value, mask_grad, group_grad


def on_device(devices, mask_field, *others):
    tiles = mask_field.shape[0] == LANES and K // 2 == LANES == SUB * devices and devices >= 10
    return (fused if tiles else plain)(devices, mask_field, *others)


def solution(mesh):
    in_specs = (
        P(("clip", "slab"), None),
        P(("clip", "slab"), None),
        P("clip", None),
        P("clip"),
        P("clip"),
        P("clip"),
    )
    out_specs = (P("clip"), P(("clip", "slab"), None), P("clip"))
    return jax.shard_map(
        functools.partial(on_device, mesh.shape["slab"]),
        mesh=mesh, in_specs=in_specs, out_specs=out_specs, check_vma=False,
    )
```

```python
import functools
import math

import jax
import jax.numpy as jnp
import numpy as np
from jax import lax
from jax.experimental import pallas as pl
from jax.experimental.pallas import tpu as pltpu
from jax.sharding import PartitionSpec as P

K = 256
GRID = 61
NG = 8

steepness = 8.0
threshold = 0.3
shift_scale = 45
F32 = jnp.float32
BF16 = jnp.bfloat16
LANES = 128
SUB = 8


def angles(left, right, length):
    turns = np.mod(np.asarray(left)[:, None] * np.asarray(right)[None, :], length)
    return 2.0 * math.pi * turns.astype(np.float64) / length


def halves(table):
    table = np.asarray(table, np.float32)
    high = table.astype(BF16)
    low = (table - high.astype(np.float32)).astype(BF16)
    return np.stack([high, low])


def split(value):
    high = value.astype(BF16)
    return high, (value - high.astype(F32)).astype(BF16)


def product(left, right, flip=False):
    dims = (((1,), (1 if flip else 0,)), ((), ()))
    one = lambda a, b: lax.dot_general(a, b, dims, preferred_element_type=F32)
    return one(left[0], right[0]) + one(left[1], right[0]) + one(left[0], right[1])


def tables(n, rows, devices):
    h = K // 2
    coarse = 2 * K
    step = n // coarse
    freq = np.arange(h)
    near = np.arange(rows)
    wave_y = angles(freq, np.arange(n), n)
    wave_y = np.concatenate([np.cos(wave_y), np.sin(wave_y)], 0)
    wave_x = angles(near, freq, n)
    wave_x = np.concatenate([np.cos(wave_x), np.sin(wave_x)], 1)
    half_x = angles(near, 2 * freq + 1, 2 * n)
    half_x = np.concatenate([np.cos(half_x), -np.sin(half_x)], 1)
    half_y = angles(2 * freq + 1, step * np.arange(coarse), 2 * n)
    half_y = np.concatenate([np.cos(half_y), np.sin(half_y)], 0)
    far = angles(rows * np.arange(devices), freq, n)
    far = np.stack([np.cos(far), np.sin(far)])[:, :, None, :].astype(np.float32)
    half_far = angles(rows * np.arange(devices), 2 * freq + 1, 2 * n)
    half_far = np.stack([np.cos(half_far), np.sin(half_far)]) / (n * n)
    half_far = half_far[:, :, None, :].astype(np.float32)
    block = 2 * LANES
    extra = n // step - block // step
    lag = np.mod(np.arange(block)[None, :] - step * (np.arange(coarse + extra) - extra)[:, None], n)
    kernel = np.ones(n)
    for f in range(1, K):
        kernel += 2.0 * np.cos(2.0 * math.pi * np.mod(f * np.arange(n), n) / n)
    up = (kernel / coarse)[lag]
    edge = angles([h], np.arange(LANES), n)
    edge = np.concatenate([np.cos(edge), np.sin(edge)], 0)
    edge = np.concatenate([edge, np.zeros((SUB - 2, LANES))], 0)
    return {
        "wave_y": halves(wave_y),
        "wave_x": halves(wave_x),
        "half_x": halves(half_x),
        "half_xt": np.concatenate(list(halves(half_x.T)[[0, 0, 1]]), 1),
        "half_y": halves(half_y),
        "half_yt": halves(half_y.T),
        "up": halves(up),
        "far": far,
        "half_far": half_far,
        "edge": edge.astype(np.float32),
    }


NAMES = ("wave_y", "wave_x", "half_x", "half_xt", "half_y", "half_yt", "up", "far", "half_far", "edge")


def kernel(devices, n, *refs):
    small_hbm, mask_hbm, target_hbm = refs[:4], refs[4], refs[5]
    sources_in = dict(zip(NAMES, refs[6 : 6 + len(NAMES)]))
    refs = refs[6 + len(NAMES) :]
    result = refs[0]
    refs = refs[1:]
    tab = dict(zip(NAMES, refs[: len(NAMES)]))
    refs = refs[len(NAMES) :]
    (mask, target, rows_t, edge_out, rows_in, edge_in, chunk, edge_all, ext, band, data, fields, image, pull,
     grads, grad_t, edge_back, grad_in, edge_back_in, edge_back_all, back_rows, back_in,
     folded, wides, weighed, settled, totals, points, groups, logits, radius,
     local_sem, send_sem, recv_sem) = refs
    h = K // 2
    coarse = 2 * K
    sources = points.shape[1]
    rows = mask.shape[0]
    block = 2 * LANES
    blocks = n // block
    step = n // coarse
    me = lax.axis_index("slab")
    norming = 1.0 / (n * n)

    loads = {}
    small = (points, groups, logits, radius)
    for i, (name, src, dst) in enumerate(
        [(f"small{k}", small_hbm[k], small[k]) for k in range(4)]
        + [("mask", mask_hbm, mask), ("wave_y", sources_in["wave_y"], tab["wave_y"])]
        + [(k, sources_in[k], tab[k]) for k in ("edge", "wave_x", "far", "half_far", "half_x", "half_y")]
        + [("up", sources_in["up"], tab["up"]), ("target", target_hbm, target)]
        + [(k, sources_in[k], tab[k]) for k in ("half_yt", "half_xt")]
    ):
        loads[name] = pltpu.make_async_copy(src, dst, local_sem.at[i])
        loads[name].start()

    barrier = pltpu.get_barrier_semaphore()

    def greet(i, carry):
        pl.semaphore_signal(barrier, inc=1, device_id={"slab": lax.rem(me + i, devices)})
        return carry

    lax.fori_loop(1, devices, greet, 0)

    def both(name):
        return tab[name][0], tab[name][1]

    def copy_to(phase, peer, src, dst):
        return pltpu.make_async_remote_copy(
            src_ref=src, dst_ref=dst, send_sem=send_sem.at[phase, peer], recv_sem=recv_sem.at[phase, me],
            device_id={"slab": peer},
        )

    def send_all(phase, src_of, dst):
        def body(i, carry):
            peer = lax.rem(me + i, devices)
            copy_to(phase, peer, src_of(peer), dst).start()
            return carry

        lax.fori_loop(1, devices, body, 0)

    def wait_all(phase, src, dst_of):
        def body(i, carry):
            peer = lax.rem(me + i, devices)
            pltpu.make_async_remote_copy(
                src_ref=src, dst_ref=dst_of(peer), send_sem=send_sem.at[phase, peer],
                recv_sem=recv_sem.at[phase, peer], device_id={"slab": peer},
            ).wait_recv()
            return carry

        lax.fori_loop(1, devices, body, 0)

    def drain(phase, src, dst):
        def body(i, carry):
            peer = lax.rem(me + i, devices)
            copy_to(phase, peer, src, dst).wait_send()
            return carry

        lax.fori_loop(1, devices, body, 0)

    lane = lax.broadcasted_iota(jnp.int32, (1, LANES), 1)

    def column(row):
        return jnp.broadcast_to(row, (LANES, LANES)).T

    loads["mask"].wait()
    loads["wave_y"].wait()
    transformed = product(split(mask[...]), both("wave_y"), flip=True)
    rows_t[0] = transformed[:, :h].T
    rows_t[1] = transformed[:, h:].T
    loads["edge"].wait()
    loads["wave_x"].wait()
    loads["far"].wait()
    edge_rows = tab["edge"][...]
    edge_pair = split(edge_rows)
    summed = mask[:, :LANES]
    for b in range(1, n // LANES):
        summed = summed + mask[:, b * LANES : (b + 1) * LANES]
    side_x = product(edge_pair, split(transformed))
    last = product(edge_pair, split(summed), flip=True)
    side_y = product(split(last), both("wave_x"))
    far_c, far_s = tab["far"][0, me], tab["far"][1, me]
    side_c = far_c * side_y[:2, :h] - far_s * side_y[:2, h:]
    side_s = far_s * side_y[:2, :h] + far_c * side_y[:2, h:]

    def mixes(cc, cs, sc, ss):
        return cc - ss, cc + ss, sc + cs, sc - cs

    edges = mixes(side_x[0:1, :h], side_x[0:1, h:], side_x[1:2, :h], side_x[1:2, h:])
    edges = edges + mixes(side_c[0:1], side_c[1:2], side_s[0:1], side_s[1:2])

    def lane_sum(value):
        return jnp.sum(value, axis=1, keepdims=True)

    corner = mixes(
        lane_sum(last[0:1] * edge_rows[0:1]), lane_sum(last[1:2] * edge_rows[0:1]),
        lane_sum(last[0:1] * edge_rows[1:2]), lane_sum(last[1:2] * edge_rows[1:2]),
    )
    corner_row = jnp.zeros((1, LANES), F32)
    for i in range(4):
        corner_row = jnp.where(lane == i, corner[i], corner_row)
    for i in range(8):
        edge_out[i] = edges[i]
    edge_out[8] = corner_row
    for i in range(9, devices):
        edge_out[i] = jnp.zeros((1, LANES), F32)

    pl.semaphore_wait(barrier, devices - 1)
    send_all(0, lambda p: rows_t.at[:, pl.ds(p * SUB, SUB), :], rows_in.at[me])
    send_all(1, lambda p: edge_out.at[p], edge_in.at[me])
    rows_in[me] = rows_t[:, pl.ds(me * SUB, SUB), :]
    edge_in[me] = edge_out[me]

    for k in range(4):
        loads[f"small{k}"].wait()
    logit_row = jnp.full((1, LANES), 0.0, F32)
    group_row = jnp.full((1, LANES), -1, jnp.int32)
    for s in range(sources):
        g = groups[s]
        logit_row = jnp.where(lane == s, logits[g], logit_row)
        group_row = jnp.where(lane == s, g, group_row)
    weight_row = jnp.where(lane < sources, jnp.exp(logit_row), 0.0)
    share_row = weight_row / jnp.sum(weight_row, axis=1, keepdims=True)

    wait_all(0, rows_t.at[:, pl.ds(0, SUB), :], lambda p: rows_in.at[p])
    gathered = rows_in[...].reshape(devices * 2 * SUB, rows)
    turned = product(split(gathered), both("wave_x")).reshape(devices, 2 * SUB, 2 * h)
    far_c, far_s = tab["far"][0], tab["far"][1]
    turned_c, turned_s = turned[:, :, :h], turned[:, :, h:]
    sum_c = jnp.sum(far_c * turned_c - far_s * turned_s, 0)
    sum_s = jnp.sum(far_s * turned_c + far_c * turned_s, 0)
    for i, value in enumerate(mixes(sum_c[:SUB], sum_c[SUB:], sum_s[:SUB], sum_s[SUB:])):
        chunk[me, i] = value
    send_all(2, lambda p: chunk.at[me], chunk.at[me])
    wait_all(1, edge_out.at[0], lambda p: edge_in.at[p])
    edge_all[me] = jnp.sum(edge_in[...], 0)
    send_all(3, lambda p: edge_all.at[me], edge_all.at[me])

    loads["half_far"].wait()
    loads["half_x"].wait()
    loads["half_y"].wait()
    turn_c = column(tab["half_far"][0, me])
    turn_s = column(tab["half_far"][1, me])

    wait_all(2, chunk.at[me], lambda p: chunk.at[p])
    wait_all(3, edge_all.at[me], lambda p: edge_all.at[p])
    shifted = []
    plain = []
    for i in range(4):
        ext[:h, :h] = chunk[:, i].reshape(h, h).T
        ext[h : h + 1, :h] = edge_all[i]
        ext[:h, h:] = column(edge_all[4 + i])
        ext[h : h + 1, h:] = jnp.broadcast_to(lane_sum(jnp.where(lane == i, edge_all[8], 0.0)), (1, LANES))
        plain = ext[...]
        moved = pltpu.roll(plain, 2 * h - 1, 1)
        if i in (0, 2):
            first, second = ext[:h, :h], None
            ext[...] = moved
            second = ext[1 : h + 1, :h]
        else:
            second = ext[1 : h + 1, :h]
            ext[...] = moved
            first = ext[:h, :h]
        data[i, 0] = first
        data[i, 1] = second

    def turn(slot, re, im, sign):
        s = turn_s if sign > 0 else -turn_s
        band[slot, 0] = re * turn_c - im * s
        band[slot, 1] = re * s + im * turn_c

    turn(0, data[0, 0], -data[2, 0], 1)
    turn(1, data[1, 0], -data[3, 0], 1)
    turn(2, data[1, 1], data[3, 1], -1)
    turn(3, data[0, 1], data[2, 1], -1)

    cutoff = radius[0]
    limit = (cutoff * cutoff).astype(F32)
    lane_index = lane.astype(F32)
    chunk_rows = [slice(c, c + 2 * SUB) for c in range(0, h, 2 * SUB)]
    row_index = lax.broadcasted_iota(jnp.int32, (2 * SUB, LANES), 0).astype(F32)

    def masks(s):
        first = ((points[0, s] - GRID // 2) * cutoff // shift_scale).astype(F32)
        second = ((points[1, s] - GRID // 2) * cutoff // shift_scale).astype(F32)
        col_p, col_m = lane_index + second, second - 1.0 - lane_index
        col_p, col_m = col_p * col_p, col_m * col_m

        def of(where):
            row_p = row_index + (first + where.start)
            row_m = (first - 1.0 - where.start) - row_index
            room_p, room_m = limit - row_p * row_p, limit - row_m * row_m
            return col_p <= room_p, col_m <= room_p, col_p <= room_m, col_m <= room_m

        return of

    def share_of(s):
        return lane_sum(jnp.where(lane == s, share_row, 0.0))

    def keep(ref, where, lanes, value):
        high, low = split(value)
        ref[0, where, lanes] = high
        ref[1, where, lanes] = low

    unroll = 8
    quarter = [slice(i * h, (i + 1) * h) for i in range(4)]
    image[...] = jnp.zeros_like(image)

    def mask_band(s, slot):
        kept = masks(s)
        dest = folded.at[slot]
        for where in chunk_rows:
            keeps = kept(where)
            low_where = slice(where.start + h, where.stop + h)
            pp, pm, mp, mm = (jnp.where(keeps[q], band[q, 0, where, :], 0.0) for q in range(4))
            ep, em, op, om = pp + mp, pm + mm, mp - pp, mm - pm
            keep(dest, where, quarter[0], ep + em)
            keep(dest, where, quarter[3], ep - em)
            keep(dest, low_where, quarter[1], om - op)
            keep(dest, low_where, quarter[2], op + om)
            pp, pm, mp, mm = (jnp.where(keeps[q], band[q, 1, where, :], 0.0) for q in range(4))
            ep, em, op, om = pp + mp, pm + mm, pp - mp, pm - mm
            keep(dest, where, quarter[1], em - ep)
            keep(dest, where, quarter[2], ep + em)
            keep(dest, low_where, quarter[0], op + om)
            keep(dest, low_where, quarter[3], op - om)

    def to_rows(slot):
        wide = product(both("half_x"), (folded[slot, 0], folded[slot, 1]))
        keep(wides.at[slot], slice(0, rows), slice(None), wide[:, : 2 * h])
        keep(wides.at[slot], slice(rows, 2 * rows), slice(None), wide[:, 2 * h :])

    def to_field(s, slot):
        field = product((wides[slot, 0], wides[slot, 1]), both("half_y"))
        fields[s] = field
        re, im = field[:rows], field[rows:]
        image[...] += share_of(s) * (re * re + im * im)

    def forward(i, carry):
        base = i * unroll
        for t in range(unroll + 2):
            if t < unroll:
                mask_band(base + t, t)
            if 0 <= t - 1 < unroll:
                to_rows(t - 1)
            if 0 <= t - 2 < unroll:
                to_field(base + t - 2, t - 2)
        return carry

    lax.fori_loop(0, sources // unroll, forward, 0)

    loads["up"].wait()
    loads["target"].wait()
    pull[...] = jnp.zeros_like(pull)
    squares = jnp.zeros((rows, LANES), F32)
    image_pair = split(image[...])
    extra = (n - block) // step
    for b in range(blocks):
        start = extra - b * (block // step)
        up = (tab["up"][0, start : start + coarse, :], tab["up"][1, start : start + coarse, :])
        intensity = product(image_pair, up)
        resist = 1.0 / (1.0 + jnp.exp(-steepness * (intensity - threshold)))
        misfit = resist - target[:, b * block : (b + 1) * block].astype(F32)
        slope = (2.0 * steepness) * misfit * resist * (1.0 - resist)
        square = misfit * misfit
        squares = squares + square[:, :LANES] + square[:, LANES:]
        pull[...] += product(split(slope), up, flip=True)
    squares = lane_sum(jnp.sum(squares, 0, keepdims=True))

    loads["half_yt"].wait()
    loads["half_xt"].wait()
    grads[...] = jnp.zeros_like(grads)
    half_xt = tab["half_xt"]

    def weigh(s, slot):
        dest = weighed.at[slot]
        total = jnp.zeros((2 * SUB, coarse), F32)
        for start in range(0, rows, 2 * SUB):
            where = slice(start, start + 2 * SUB)
            other = slice(start + rows, start + rows + 2 * SUB)
            weak, re, im = pull[where, :], fields[s, where, :], fields[s, other, :]
            down_r, down_i = weak * re, weak * im
            total = total + (down_r * re + down_i * im)
            keep(dest, where, slice(None), down_r)
            keep(dest, other, slice(None), down_i)
        total = total[:SUB] + total[SUB:]
        totals[s] = total[:, :h] + total[:, h : 2 * h] + total[:, 2 * h : 3 * h] + total[:, 3 * h :]

    def from_field(s, slot):
        settle = product((weighed[slot, 0], weighed[slot, 1]), both("half_yt")) * (2.0 * share_of(s))
        for part in range(2):
            high, low = split(settle[part * rows : (part + 1) * rows])
            settled[slot, :rows, part * 2 * h : (part + 1) * 2 * h] = high
            settled[slot, rows:, part * 2 * h : (part + 1) * 2 * h] = low

    def from_rows(s, slot):
        kept = masks(s)
        dims = (((1,), (0,)), ((), ()))
        full = lax.dot_general(half_xt[:, : 2 * rows], settled[slot], dims, preferred_element_type=F32)
        full = full + lax.dot_general(
            half_xt[:, 2 * rows :], settled[slot, :rows], dims, preferred_element_type=F32
        )
        for where in chunk_rows:
            keeps = kept(where)
            top, low = full[where], full[where.start + h : where.stop + h]
            ee_r, no_i, ee_i, eo_r = (top[:, q] for q in quarter)
            oe_i, oo_r, ne_r, oo_i = (low[:, q] for q in quarter)
            ep, em, op, om = ee_r + eo_r, ee_r - eo_r, oo_r - ne_r, -ne_r - oo_r
            for q, value in enumerate((ep + op, em + om, ep - op, em - om)):
                grads[q, 0, where, :] += jnp.where(keeps[q], value, 0.0)
            ep, em, op, om = ee_i - no_i, ee_i + no_i, oe_i + oo_i, oe_i - oo_i
            for q, value in enumerate((ep + op, em + om, ep - op, em - om)):
                grads[q, 1, where, :] += jnp.where(keeps[q], value, 0.0)

    def backward(i, carry):
        base = i * unroll
        for t in range(unroll + 2):
            if t < unroll:
                weigh(base + t, t)
            if 0 <= t - 1 < unroll:
                from_field(base + t - 1, t - 1)
            if 0 <= t - 2 < unroll:
                from_rows(base + t - 2, t - 2)
        return carry

    lax.fori_loop(0, sources // unroll, backward, 0)
    each = lane_sum(jnp.sum(totals[...], 1))
    own = lax.broadcasted_iota(jnp.int32, (sources, LANES), 0) == lane
    sums = jnp.sum(jnp.where(own, each, 0.0), 0, keepdims=True)
    sums = jnp.where(lane == sources, squares, sums)

    def unturn(slot, sign):
        s = turn_s if sign > 0 else -turn_s
        re, im = grads[slot, 0], grads[slot, 1]
        return re * turn_c + im * s, im * turn_c - re * s

    pp, pm, mp, mm = unturn(0, 1), unturn(1, 1), unturn(2, -1), unturn(3, -1)
    pieces = ((pp[0], mm[0]), (pm[0], mp[0]), (-pp[1], mm[1]), (-pm[1], mp[1]))
    last_row = jnp.zeros((1, LANES), F32)
    for i, (first, second) in enumerate(pieces):
        ext[...] = jnp.zeros_like(ext)
        if i in (0, 2):
            ext[1 : h + 1, :h] = second
            moved = pltpu.roll(ext[...], 1, 1)
            ext[...] = moved
            ext[:h, :h] += first
        else:
            ext[:h, :h] = first
            moved = pltpu.roll(ext[...], 1, 1)
            ext[...] = moved
            ext[1 : h + 1, :h] += second
        grad_t[i] = ext[:h, :h].T
        edge_back[i] = ext[h : h + 1, :h]
        edge_back[4 + i] = ext[:h, h:].T[0:1, :]
        last_row = jnp.where(lane == i, ext[h : h + 1, h : h + 1], last_row)
    edge_back[8] = last_row
    edge_back[9] = sums
    for i in range(10, devices):
        edge_back[i] = jnp.zeros((1, LANES), F32)

    send_all(4, lambda p: grad_t.at[:, pl.ds(p * SUB, SUB), :], grad_in.at[me])
    send_all(5, lambda p: edge_back.at[p], edge_back_in.at[me])
    grad_in[me] = grad_t[:, pl.ds(me * SUB, SUB), :]
    edge_back_in[me] = edge_back[me]
    wait_all(4, grad_t.at[:, pl.ds(0, SUB), :], lambda p: grad_in.at[p])

    def unmix(u, v, wp, wm):
        return u + v, wp - wm, wp + wm, v - u

    mine = jnp.sum(grad_in[...], 0)
    cc, cs, sc, ss = unmix(mine[0], mine[1], mine[2], mine[3])
    sum_c = jnp.concatenate([cc, cs], 0)[None]
    sum_s = jnp.concatenate([sc, ss], 0)[None]
    back_c = far_c * sum_c + far_s * sum_s
    back_s = far_c * sum_s - far_s * sum_c
    turned = jnp.concatenate([back_c, back_s], 2).reshape(devices * 2 * SUB, 2 * h)
    gathered = product(split(turned), both("wave_x"), flip=True)
    back_rows[...] = gathered.reshape(devices, 2, SUB, rows)
    send_all(6, lambda p: back_rows.at[p], back_in.at[:, pl.ds(me * SUB, SUB), :])
    back_in[:, pl.ds(me * SUB, SUB), :] = back_rows[me]
    wait_all(5, edge_back.at[0], lambda p: edge_back_in.at[p])
    edge_back_all[me] = jnp.sum(edge_back_in[...], 0)
    send_all(7, lambda p: edge_back_all.at[me], edge_back_all.at[me])
    wait_all(7, edge_back_all.at[me], lambda p: edge_back_all.at[p])

    sums = edge_back_all[9]
    small_at = slice(2 * h + LANES, 2 * h + 2 * LANES)
    result[0:1, small_at] = sums * norming
    sums = jnp.where(lane < sources, sums, 0.0)
    result[1:2, small_at] = share_row * (sums - lane_sum(share_row * sums)) * norming
    result[2:3, small_at] = group_row.astype(F32)

    side_x = unmix(*(edge_back_all[i] for i in range(4)))
    side_y = unmix(*(edge_back_all[4 + i] for i in range(4)))
    corner = unmix(*(lane_sum(jnp.where(lane == i, edge_back_all[8], 0.0)) for i in range(4)))
    far_c, far_s = tab["far"][0, me], tab["far"][1, me]
    near = []
    for c, s in ((side_y[0], side_y[2]), (side_y[1], side_y[3])):
        near.append(jnp.concatenate([far_c * c + far_s * s, far_c * s - far_s * c], 1))
    near = jnp.concatenate(near + [jnp.zeros((SUB - 2, 2 * h), F32)], 0)
    last = product(split(near), both("wave_x"), flip=True)
    edge_c, edge_s = edge_rows[0:1], edge_rows[1:2]
    last_c = last[0:1] + corner[0] * edge_c + corner[2] * edge_s
    last_s = last[1:2] + corner[1] * edge_c + corner[3] * edge_s
    result[:, 2 * h : 2 * h + LANES] = column(last_c) * edge_c + column(last_s) * edge_s
    col_c, col_s = column(edge_c), column(edge_s)

    wait_all(6, back_rows.at[0], lambda p: back_in.at[:, pl.ds(p * SUB, SUB), :])
    part_c = back_in[0].T + col_c * side_x[0] + col_s * side_x[2]
    part_s = back_in[1].T + col_c * side_x[1] + col_s * side_x[3]
    result[:, :h] = part_c
    result[:, h : 2 * h] = part_s
    drain(0, rows_t.at[:, pl.ds(0, SUB), :], rows_in.at[me])
    drain(1, edge_out.at[0], edge_in.at[me])
    drain(2, chunk.at[me], chunk.at[me])
    drain(3, edge_all.at[me], edge_all.at[me])
    drain(4, grad_t.at[:, pl.ds(0, SUB), :], grad_in.at[me])
    drain(5, edge_back.at[0], edge_back_in.at[me])
    drain(6, back_rows.at[0], back_in.at[:, pl.ds(0, SUB), :])
    drain(7, edge_back_all.at[me], edge_back_all.at[me])


def closing(n, sources, result, wave, loss_hbm, grad_hbm, group_hbm, loss, group, out, out_sem):
    block = 2 * LANES
    blocks = n // block
    lane = lax.broadcasted_iota(jnp.int32, (1, LANES), 1)
    h = K // 2
    small = result.at[:, 2 * h + LANES :]
    loss[0] = jnp.sum(jnp.where(lane == sources, small[0:1, :], 0.0))
    for g in range(NG):
        group[g] = jnp.sum(jnp.where(small[2:3, :] == g, small[1:2, :], 0.0))
    stores = [
        pltpu.make_async_copy(loss, loss_hbm, out_sem.at[blocks]),
        pltpu.make_async_copy(group, group_hbm, out_sem.at[blocks + 1]),
    ]
    for store in stores:
        store.start()
    pair = split(result[:, : 2 * h])
    spread = result[:, 2 * h : 2 * h + LANES]
    adds = jnp.concatenate([spread, spread], 1)
    for b in range(blocks):
        where = slice(b * block, (b + 1) * block)
        out[:, where] = product(pair, (wave[0, :, where], wave[1, :, where])) + adds
        stores.append(pltpu.make_async_copy(out.at[:, where], grad_hbm.at[:, where], out_sem.at[b]))
        stores[-1].start()
    for store in stores:
        store.wait()


def fused(devices, mask_field, target_print, source_points, source_groups, group_logits, pupil_radius):
    rows, n = mask_field.shape
    h = K // 2
    coarse = 2 * K
    sources = source_points.shape[0]
    consts = tables(n, rows, devices)
    anywhere = pl.BlockSpec(memory_space=pltpu.HBM)
    vmem = lambda *shape: pltpu.VMEM(shape, F32)
    scratch = [pltpu.VMEM(consts[k].shape, consts[k].dtype) for k in NAMES] + [
        vmem(rows, n), pltpu.VMEM((rows, n), jnp.int32),
        vmem(2, h, rows), vmem(devices, 1, LANES), vmem(devices, 2, SUB, rows), vmem(devices, 1, LANES),
        vmem(devices, 4, SUB, h), vmem(devices, 1, LANES), vmem(h + SUB, 2 * h), vmem(4, 2, h, h),
        vmem(4, 2, h, h), vmem(sources, 2 * rows, coarse), vmem(rows, coarse), vmem(rows, coarse),
        vmem(4, 2, h, h), vmem(4, h, h), vmem(devices, 1, LANES), vmem(devices, 4, SUB, h),
        vmem(devices, 1, LANES), vmem(devices, 1, LANES), vmem(devices, 2, SUB, rows), vmem(2, h, rows),
        pltpu.VMEM((8, 2, 2 * h, coarse), BF16), pltpu.VMEM((8, 2, 2 * rows, 2 * h), BF16),
        pltpu.VMEM((8, 2, 2 * rows, coarse), BF16), pltpu.VMEM((8, 2 * rows, coarse), BF16),
        vmem(sources, SUB, LANES),
        pltpu.SMEM((2, sources), jnp.int32), pltpu.SMEM((sources,), jnp.int32), pltpu.SMEM((NG,), F32),
        pltpu.SMEM((1,), jnp.int32),
        pltpu.SemaphoreType.DMA((16,)),
        pltpu.SemaphoreType.DMA((8, devices)), pltpu.SemaphoreType.DMA((8, devices)),
    ]
    arrays = [jnp.asarray(consts[k]) for k in NAMES]
    inside = pl.BlockSpec(memory_space=pltpu.VMEM)
    (result,) = pl.pallas_call(
        functools.partial(kernel, devices, n),
        out_shape=(
            jax.ShapeDtypeStruct((rows, 2 * h + 2 * LANES), F32),
        ),
        in_specs=[anywhere] * (6 + len(NAMES)),
        out_specs=(inside,),
        scratch_shapes=scratch,
        compiler_params=pltpu.CompilerParams(
            collective_id=0, has_side_effects=True, vmem_limit_bytes=58 * 1024 * 1024
        ),
    )(source_points.T, source_groups, group_logits, pupil_radius, mask_field, target_print, *arrays)
    return pl.pallas_call(
        functools.partial(closing, n, sources),
        out_shape=(
            jax.ShapeDtypeStruct((1,), F32),
            jax.ShapeDtypeStruct((rows, n), F32),
            jax.ShapeDtypeStruct((NG,), F32),
        ),
        in_specs=[inside] * 2,
        out_specs=(anywhere, anywhere, anywhere),
        scratch_shapes=[
            pltpu.SMEM((1,), F32), pltpu.SMEM((NG,), F32), vmem(rows, n),
            pltpu.SemaphoreType.DMA((n // (2 * LANES) + 2,)),
        ],
        compiler_params=pltpu.CompilerParams(vmem_limit_bytes=8 * 1024 * 1024),
    )(result, arrays[0])


HIGH = lax.Precision.HIGH


def dot(form, left, right):
    return jnp.einsum(form, left, right, precision=HIGH, preferred_element_type=F32)


def waves(left, right, length):
    turns = angles(left, right, length)
    return np.cos(turns), np.sin(turns)


def shifted_waves(count, freq, length, device, devices):
    near = np.stack(waves(np.arange(count), freq, length)).astype(np.float32)
    far = np.stack(waves(np.arange(devices) * count, freq, length)).astype(np.float32)
    far = lax.dynamic_slice_in_dim(jnp.asarray(far), device, 1, axis=1)
    return far[0] * near[0] - far[1] * near[1], far[1] * near[0] + far[0] * near[1]


def exchange(blocks):
    return lax.all_to_all(blocks, "slab", 0, 0)


def plain(devices, mask_field, target_print, source_points, source_groups, group_logits, pupil_radius):
    rows, n = mask_field.shape
    sources = source_points.shape[0]
    coarse = 2 * K
    step = n // coarse
    cols = coarse // devices
    half = n // 2
    device = lax.axis_index("slab")
    freq = np.arange(K, dtype=np.int64) - K // 2
    order = np.concatenate([freq[freq % 2 == 0], freq[freq % 2 == 1]])
    kh = K // 2
    norming = 1.0 / (n * n)

    cos_y, sin_y = waves(np.arange(half), order, n)
    fold = [
        jnp.asarray(np.concatenate([t[:, p * kh : (p + 1) * kh] for t in (cos_y, sin_y)], 1), F32)
        for p in (0, 1)
    ]
    lag = np.mod(np.arange(n)[None, :] - step * np.arange(coarse)[:, None], n)
    response = np.zeros(n)
    for f in range(1, K):
        response += 2.0 * np.cos(2.0 * math.pi * np.mod(f * np.arange(n), n) / n)
    response = (response + 1.0) / coarse
    up = jnp.asarray(response[lag], F32)
    cos_c, sin_c = waves(freq, np.arange(coarse), coarse)
    wave_x = jnp.asarray(np.concatenate([cos_c, sin_c], 1), F32)
    loc_c, loc_s = shifted_waves(rows, freq, n, device, devices)
    loc = jnp.concatenate([loc_c, loc_s], 1)
    a, b = shifted_waves(cols, order, coarse, device, devices)
    lift = jnp.concatenate([jnp.concatenate([a, -b], 1), jnp.concatenate([b, a], 1)], 0)

    cutoff = pupil_radius[0]
    shifted = (source_points - GRID // 2) * cutoff // shift_scale
    first = jnp.asarray(freq, jnp.int32)[None, None, :] + shifted[:, 0, None, None]
    second = jnp.asarray(np.tile(order, 2), jnp.int32)[None, :, None] + shifted[:, 1, None, None]
    passed = first * first + second * second <= cutoff * cutoff

    near, away = mask_field[:, :half], mask_field[:, half:]
    even = dot("xy,yq->xq", near + away, fold[0])
    odd = dot("xy,yq->xq", near - away, fold[1])
    part_c = jnp.concatenate([even[:, :kh], odd[:, :kh]], 1)
    part_s = jnp.concatenate([even[:, kh:], odd[:, kh:]], 1)
    spec = dot("xq,xk->qk", jnp.concatenate([part_c, part_s], 1), loc)
    band = jnp.concatenate([spec[:K, :K] - spec[K:, K:], -(spec[:K, K:] + spec[K:, :K])], 0)
    band = jnp.sum(exchange(band.reshape(devices, 2 * K // devices, K)), 0)
    band = lax.all_gather(band, "slab", tiled=True)

    kept = jnp.where(passed, band[None], 0.0)
    wide = dot("aq,sqk->sak", lift, kept)
    both = dot("ak,kx->ax", wide.reshape(sources * 2 * cols, K), wave_x)
    both = both.reshape(sources, 2, cols, 2 * coarse)
    field_re = (both[:, 0, :, :coarse] - both[:, 1, :, coarse:]) * norming
    field_im = (both[:, 0, :, coarse:] + both[:, 1, :, :coarse]) * norming
    bright = field_re * field_re + field_im * field_im
    onehot = (source_groups[:, None] == jnp.arange(NG, dtype=jnp.int32)[None, :]).astype(F32)
    weights = jnp.exp(jnp.sum(onehot * group_logits[None, :], 1))
    share = weights / jnp.sum(weights)
    image = jnp.sum(share[:, None, None] * bright, 0)

    tall = dot("cm,mx->cx", image, up)
    tall = lax.all_to_all(tall, "slab", 1, 0, tiled=True)
    intensity = dot("cx,cy->xy", tall, up)
    resist = jax.nn.sigmoid(steepness * (intensity - threshold))
    misfit = resist - target_print.astype(F32)
    slope = (2.0 * steepness) * misfit * resist * (1.0 - resist)
    squares = jnp.sum(misfit * misfit)
    down = dot("xy,cy->cx", slope, up)
    down = lax.all_to_all(down, "slab", 0, 1, tiled=True)
    pull = dot("cx,mx->cm", down, up)

    per_source = jnp.sum(bright * pull[None], (1, 2))
    sums = jnp.concatenate([per_source, squares[None]])
    factor = (2.0 * norming) * share[:, None, None] * pull[None]
    back = jnp.stack([factor * field_re, factor * field_im], 1)
    low = dot("ax,kx->ak", back.reshape(sources * 2 * cols, coarse), wave_x[:, :coarse])
    lows = dot("ax,kx->ak", back.reshape(sources * 2 * cols, coarse), wave_x[:, coarse:])
    low = low.reshape(sources, 2, cols, K)
    lows = lows.reshape(sources, 2, cols, K)
    settle = jnp.concatenate([low[:, 0] + lows[:, 1], low[:, 1] - lows[:, 0]], 1)
    settle = dot("aq,sak->sqk", lift, settle)
    grad_band = jnp.sum(jnp.where(passed, settle, 0.0), 0).reshape(devices, 2 * K // devices, K)
    extra = jnp.pad(sums[None, :], ((0, 7), (0, K - sources - 1)))
    extra = jnp.broadcast_to(extra[None], (devices, 8, K))
    grad_band = jnp.sum(exchange(jnp.concatenate([grad_band, extra], 1)), 0)
    sums = grad_band[-8, : sources + 1]
    grad_band = lax.all_gather(grad_band[:-8], "slab", tiled=True)
    per_source, squares = sums[:-1], sums[-1]
    loss_value = (squares * norming).reshape(1)
    against = jnp.sum(share * per_source)
    source_pull = share * (per_source - against)
    group_grad = jnp.sum(onehot * source_pull[:, None], 0) * norming

    spread = dot("tk,qk->tq", jnp.concatenate([loc_c, loc_s], 0), grad_band)
    spread_re = spread[:rows, :K] - spread[rows:, K:]
    spread_im = spread[:rows, K:] + spread[rows:, :K]
    even = dot("xq,yq->xy", jnp.concatenate([spread_re[:, :kh], -spread_im[:, :kh]], 1), fold[0])
    odd = dot("xq,yq->xy", jnp.concatenate([spread_re[:, kh:], -spread_im[:, kh:]], 1), fold[1])
    mask_grad = jnp.concatenate([even + odd, even - odd], 1)
    return loss_value, mask_grad, group_grad


def on_device(devices, mask_field, *others):
    tiles = mask_field.shape[0] == LANES and K // 2 == LANES == SUB * devices and devices >= 10
    return (fused if tiles else plain)(devices, mask_field, *others)


def solution(mesh):
    in_specs = (
        P(("clip", "slab"), None),
        P(("clip", "slab"), None),
        P("clip", None),
        P("clip"),
        P("clip"),
        P("clip"),
    )
    out_specs = (P("clip"), P(("clip", "slab"), None), P("clip"))
    return jax.shard_map(
        functools.partial(on_device, mesh.shape["slab"]),
        mesh=mesh, in_specs=in_specs, out_specs=out_specs, check_vma=False,
    )
```

```python
import functools
import math

import jax
import jax.numpy as jnp
import numpy as np
from jax import lax
from jax.experimental import pallas as pl
from jax.experimental.pallas import tpu as pltpu
from jax.sharding import PartitionSpec as P

K = 256
GRID = 61
NG = 8

steepness = 8.0
threshold = 0.3
shift_scale = 45
F32 = jnp.float32
BF16 = jnp.bfloat16
LANES = 128
SUB = 8


def angles(left, right, length):
    turns = np.mod(np.asarray(left)[:, None] * np.asarray(right)[None, :], length)
    return 2.0 * math.pi * turns.astype(np.float64) / length


def halves(table):
    table = np.asarray(table, np.float32)
    high = table.astype(BF16)
    low = (table - high.astype(np.float32)).astype(BF16)
    return np.stack([high, low])


def split(value):
    high = value.astype(BF16)
    return high, (value - high.astype(F32)).astype(BF16)


def product(left, right, flip=False):
    dims = (((1,), (1 if flip else 0,)), ((), ()))
    one = lambda a, b: lax.dot_general(a, b, dims, preferred_element_type=F32)
    return one(left[0], right[0]) + one(left[1], right[0]) + one(left[0], right[1])


def tables(n, rows, devices):
    h = K // 2
    coarse = 2 * K
    step = n // coarse
    freq = np.arange(h)
    near = np.arange(rows)
    wave_y = angles(freq, np.arange(n), n)
    wave_y = np.concatenate([np.cos(wave_y), np.sin(wave_y)], 0)
    wave_x = angles(near, freq, n)
    wave_x = np.concatenate([np.cos(wave_x), np.sin(wave_x)], 1)
    half_x = angles(near, 2 * freq + 1, 2 * n)
    half_x = np.concatenate([np.cos(half_x), -np.sin(half_x)], 1)
    half_y = angles(2 * freq + 1, step * np.arange(coarse), 2 * n)
    half_y = np.concatenate([np.cos(half_y), np.sin(half_y)], 0)
    far = angles(rows * np.arange(devices), freq, n)
    far = np.stack([np.cos(far), np.sin(far)])[:, :, None, :].astype(np.float32)
    half_far = angles(rows * np.arange(devices), 2 * freq + 1, 2 * n)
    half_far = np.stack([np.cos(half_far), np.sin(half_far)]) / (n * n)
    half_far = half_far[:, :, None, :].astype(np.float32)
    block = 2 * LANES
    extra = n // step - block // step
    lag = np.mod(np.arange(block)[None, :] - step * (np.arange(coarse + extra) - extra)[:, None], n)
    kernel = np.ones(n)
    for f in range(1, K):
        kernel += 2.0 * np.cos(2.0 * math.pi * np.mod(f * np.arange(n), n) / n)
    up = (kernel / coarse)[lag]
    edge = angles([h], np.arange(LANES), n)
    edge = np.concatenate([np.cos(edge), np.sin(edge)], 0)
    edge = np.concatenate([edge, np.zeros((SUB - 2, LANES))], 0)
    return {
        "wave_y": halves(wave_y),
        "wave_x": halves(wave_x),
        "half_x": halves(half_x),
        "half_xt": np.concatenate(list(halves(half_x.T)[[0, 0, 1]]), 1),
        "half_y": halves(half_y),
        "half_yt": halves(half_y.T),
        "up": halves(up),
        "far": far,
        "half_far": half_far,
        "edge": edge.astype(np.float32),
    }


NAMES = ("wave_y", "wave_x", "half_x", "half_xt", "half_y", "half_yt", "up", "far", "half_far", "edge")


def kernel(devices, n, *refs):
    small_hbm, mask_hbm, target_hbm = refs[:4], refs[4], refs[5]
    sources_in = dict(zip(NAMES, refs[6 : 6 + len(NAMES)]))
    refs = refs[6 + len(NAMES) :]
    result = refs[0]
    refs = refs[1:]
    tab = dict(zip(NAMES, refs[: len(NAMES)]))
    refs = refs[len(NAMES) :]
    (mask, target, rows_t, edge_out, rows_in, edge_in, chunk, edge_all, ext, band, data, fields, image, pull,
     grads, grad_t, edge_back, grad_in, edge_back_in, edge_back_all, back_rows, back_in,
     folded, wides, weighed, settled, totals, points, groups, logits, radius,
     pair_in, pair_sum, up_t, slopes, local_sem, send_sem, recv_sem, near_sem) = refs
    h = K // 2
    coarse = 2 * K
    sources = points.shape[1]
    rows = mask.shape[0]
    block = 2 * LANES
    blocks = n // block
    step = n // coarse
    me = lax.axis_index("slab")
    norming = 1.0 / (n * n)
    chips = devices // 2
    core, chip = lax.rem(me, 2), me // 2
    partner = me + 1 - 2 * core
    most = pl.ds(0, devices - 1)

    loads = {}
    small = (points, groups, logits, radius)
    pieces = [slice(c, c + n // 4) for c in range(0, n, n // 4)]
    for i, (name, src, dst) in enumerate(
        [
            piece
            for k, where in enumerate(pieces)
            for piece in (
                (f"mask{k}", mask_hbm.at[:, where], mask.at[:, where]),
                (f"wave_y{k}", sources_in["wave_y"].at[:, :, where], tab["wave_y"].at[:, :, where]),
            )
        ]
        + [(f"small{k}", small_hbm[k], small[k]) for k in range(4)]
        + [(k, sources_in[k], tab[k]) for k in ("edge", "wave_x", "far", "half_far", "half_x", "half_y")]
        + [("up", sources_in["up"], tab["up"]), ("target", target_hbm, target)]
        + [(k, sources_in[k], tab[k]) for k in ("half_yt", "half_xt")]
    ):
        loads[name] = pltpu.make_async_copy(src, dst, local_sem.at[i])
        loads[name].start()

    barrier = pltpu.get_barrier_semaphore()

    def greet(i, carry):
        pl.semaphore_signal(barrier, inc=1, device_id={"slab": lax.rem(me + i, devices)})
        return carry

    lax.fori_loop(1, devices, greet, 0)

    def both(name):
        return tab[name][0], tab[name][1]

    def copy_to(phase, peer, src, dst, sem=None):
        return pltpu.make_async_remote_copy(
            src_ref=src, dst_ref=dst, send_sem=send_sem.at[phase],
            recv_sem=recv_sem.at[phase] if sem is None else sem, device_id={"slab": peer},
        )

    def send_all(phase, src_of, dst):
        def body(i, carry):
            peer = lax.rem(me + i, devices)
            copy_to(phase, peer, src_of(peer), dst).start()
            return carry

        lax.fori_loop(1, devices, body, 0)

    def wait_all(phase, ref, sem=None):
        copy_to(phase, partner, ref, ref, sem).wait_recv()

    def drain(phase, ref):
        copy_to(phase, partner, ref, ref).wait_send()

    lane = lax.broadcasted_iota(jnp.int32, (1, LANES), 1)

    def column(row):
        return jnp.broadcast_to(row, (LANES, LANES)).T

    transformed = 0.0
    for k, where in enumerate(pieces):
        loads[f"mask{k}"].wait()
        loads[f"wave_y{k}"].wait()
        wave = (tab["wave_y"][0, :, where], tab["wave_y"][1, :, where])
        transformed = transformed + product(split(mask[:, where]), wave, flip=True)
    rows_t[0] = transformed[:, :h].T
    rows_t[1] = transformed[:, h:].T
    loads["edge"].wait()
    loads["wave_x"].wait()
    loads["far"].wait()
    edge_rows = tab["edge"][...]
    edge_pair = split(edge_rows)
    summed = mask[:, :LANES]
    for b in range(1, n // LANES):
        summed = summed + mask[:, b * LANES : (b + 1) * LANES]
    side_x = product(edge_pair, split(transformed))
    last = product(edge_pair, split(summed), flip=True)
    side_y = product(split(last), both("wave_x"))
    far_c, far_s = tab["far"][0, me], tab["far"][1, me]
    side_c = far_c * side_y[:2, :h] - far_s * side_y[:2, h:]
    side_s = far_s * side_y[:2, :h] + far_c * side_y[:2, h:]

    def mixes(cc, cs, sc, ss):
        return cc - ss, cc + ss, sc + cs, sc - cs

    edges = mixes(side_x[0:1, :h], side_x[0:1, h:], side_x[1:2, :h], side_x[1:2, h:])
    edges = edges + mixes(side_c[0:1], side_c[1:2], side_s[0:1], side_s[1:2])

    def lane_sum(value):
        return jnp.sum(value, axis=1, keepdims=True)

    corner = mixes(
        lane_sum(last[0:1] * edge_rows[0:1]), lane_sum(last[1:2] * edge_rows[0:1]),
        lane_sum(last[0:1] * edge_rows[1:2]), lane_sum(last[1:2] * edge_rows[1:2]),
    )
    corner_row = jnp.zeros((1, LANES), F32)
    for i in range(4):
        corner_row = jnp.where(lane == i, corner[i], corner_row)
    for i in range(8):
        edge_out[i] = edges[i]
    edge_out[8] = corner_row
    for i in range(9, devices):
        edge_out[i] = jnp.zeros((1, LANES), F32)

    pl.semaphore_wait(barrier, devices - 1)
    send_all(0, lambda p: rows_t.at[:, pl.ds(p * SUB, SUB), :], rows_in.at[me])
    send_all(1, lambda p: edge_out.at[p], edge_in.at[me])
    rows_in[me] = rows_t[:, pl.ds(me * SUB, SUB), :]
    edge_in[me] = edge_out[me]

    for k in range(4):
        loads[f"small{k}"].wait()
    logit_row = jnp.full((1, LANES), 0.0, F32)
    group_row = jnp.full((1, LANES), -1, jnp.int32)
    for s in range(sources):
        g = groups[s]
        logit_row = jnp.where(lane == s, logits[g], logit_row)
        group_row = jnp.where(lane == s, g, group_row)
    weight_row = jnp.where(lane < sources, jnp.exp(logit_row), 0.0)
    share_row = weight_row / jnp.sum(weight_row, axis=1, keepdims=True)

    loads["up"].wait()
    extra = (n - block) // step
    for b in range(blocks):
        start = extra - b * (block // step)
        for part in range(2):
            up_t[part, b * block : (b + 1) * block, :] = tab["up"][part, start : start + coarse, :].T

    wait_all(0, rows_in.at[most])
    gathered = rows_in[...].reshape(devices * 2 * SUB, rows)
    turned = product(split(gathered), both("wave_x")).reshape(devices, 2 * SUB, 2 * h)
    far_c, far_s = tab["far"][0], tab["far"][1]
    turned_c, turned_s = turned[:, :, :h], turned[:, :, h:]
    sum_c = jnp.sum(far_c * turned_c - far_s * turned_s, 0)
    sum_s = jnp.sum(far_s * turned_c + far_c * turned_s, 0)
    for i, value in enumerate(mixes(sum_c[:SUB], sum_c[SUB:], sum_s[:SUB], sum_s[SUB:])):
        chunk[me, i] = value

    def share(i, carry):
        copy_to(2, lax.rem(me + 2 * i, devices), chunk.at[me], chunk.at[me], near_sem.at[chip]).start()
        return carry

    lax.fori_loop(1, chips, share, 0)
    copy_to(2, partner, chunk.at[me], chunk.at[me]).start()
    wait_all(1, edge_in.at[most])
    edge_all[me] = jnp.sum(edge_in[...], 0)
    send_all(3, lambda p: edge_all.at[me], edge_all.at[me])

    loads["half_far"].wait()
    loads["half_x"].wait()
    loads["half_y"].wait()
    turn_c = column(tab["half_far"][0, me])
    turn_s = column(tab["half_far"][1, me])


    def relay(i, carry):
        peer = lax.rem(me + 2 * i, devices)
        wait_all(2, chunk.at[peer], near_sem.at[peer // 2])
        copy_to(2, partner, chunk.at[peer], chunk.at[peer]).start()
        return carry

    lax.fori_loop(1, chips, relay, 0)
    wait_all(2, chunk.at[pl.ds(0, chips)])
    wait_all(3, edge_all.at[most])
    shifted = []
    plain = []
    for i in range(4):
        ext[:h, :h] = chunk[:, i].reshape(h, h).T
        ext[h : h + 1, :h] = edge_all[i]
        ext[:h, h:] = column(edge_all[4 + i])
        ext[h : h + 1, h:] = jnp.broadcast_to(lane_sum(jnp.where(lane == i, edge_all[8], 0.0)), (1, LANES))
        plain = ext[...]
        moved = pltpu.roll(plain, 2 * h - 1, 1)
        if i in (0, 2):
            first, second = ext[:h, :h], None
            ext[...] = moved
            second = ext[1 : h + 1, :h]
        else:
            second = ext[1 : h + 1, :h]
            ext[...] = moved
            first = ext[:h, :h]
        data[i, 0] = first
        data[i, 1] = second

    def turn(slot, re, im, sign):
        s = turn_s if sign > 0 else -turn_s
        band[slot, 0] = re * turn_c - im * s
        band[slot, 1] = re * s + im * turn_c

    turn(0, data[0, 0], -data[2, 0], 1)
    turn(1, data[1, 0], -data[3, 0], 1)
    turn(2, data[1, 1], data[3, 1], -1)
    turn(3, data[0, 1], data[2, 1], -1)

    cutoff = radius[0]
    limit = (cutoff * cutoff).astype(F32)
    lane_index = lane.astype(F32)
    chunk_rows = [slice(c, c + 2 * SUB) for c in range(0, h, 2 * SUB)]
    row_index = lax.broadcasted_iota(jnp.int32, (2 * SUB, LANES), 0).astype(F32)

    def masks(s):
        first = ((points[0, s] - GRID // 2) * cutoff // shift_scale).astype(F32)
        second = ((points[1, s] - GRID // 2) * cutoff // shift_scale).astype(F32)
        col_p, col_m = lane_index + second, second - 1.0 - lane_index
        col_p, col_m = col_p * col_p, col_m * col_m

        def of(where):
            row_p = row_index + (first + where.start)
            row_m = (first - 1.0 - where.start) - row_index
            room_p, room_m = limit - row_p * row_p, limit - row_m * row_m
            return col_p <= room_p, col_m <= room_p, col_p <= room_m, col_m <= room_m

        return of

    def share_of(s):
        return lane_sum(jnp.where(lane == s, share_row, 0.0))

    def keep(ref, where, lanes, value):
        high, low = split(value)
        ref[0, where, lanes] = high
        ref[1, where, lanes] = low

    unroll = 8
    quarter = [slice(i * h, (i + 1) * h) for i in range(4)]
    image[...] = jnp.zeros_like(image)

    def mask_band(s, slot):
        kept = masks(s)
        dest = folded.at[slot]
        for where in chunk_rows:
            keeps = kept(where)
            low_where = slice(where.start + h, where.stop + h)
            pp, pm, mp, mm = (jnp.where(keeps[q], band[q, 0, where, :], 0.0) for q in range(4))
            ep, em, op, om = pp + mp, pm + mm, mp - pp, mm - pm
            keep(dest, where, quarter[0], ep + em)
            keep(dest, where, quarter[3], ep - em)
            keep(dest, low_where, quarter[1], om - op)
            keep(dest, low_where, quarter[2], op + om)
            pp, pm, mp, mm = (jnp.where(keeps[q], band[q, 1, where, :], 0.0) for q in range(4))
            ep, em, op, om = pp + mp, pm + mm, pp - mp, pm - mm
            keep(dest, where, quarter[1], em - ep)
            keep(dest, where, quarter[2], ep + em)
            keep(dest, low_where, quarter[0], op + om)
            keep(dest, low_where, quarter[3], op - om)

    def to_rows(slot):
        wide = product(both("half_x"), (folded[slot, 0], folded[slot, 1]))
        keep(wides.at[slot], slice(0, rows), slice(None), wide[:, : 2 * h])
        keep(wides.at[slot], slice(rows, 2 * rows), slice(None), wide[:, 2 * h :])

    def to_field(s, slot):
        field = product((wides[slot, 0], wides[slot, 1]), both("half_y"))
        fields[s] = field
        re, im = field[:rows], field[rows:]
        image[...] += share_of(s) * (re * re + im * im)

    def forward(i, carry):
        base = i * unroll
        for t in range(unroll + 2):
            if t < unroll:
                mask_band(base + t, t)
            if 0 <= t - 1 < unroll:
                to_rows(t - 1)
            if 0 <= t - 2 < unroll:
                to_field(base + t - 2, t - 2)
        return carry

    lax.fori_loop(0, sources // unroll, forward, 0)

    loads["target"].wait()
    squares = jnp.zeros((rows, LANES), F32)
    image_pair = split(image[...])
    for b in range(blocks):
        start = extra - b * (block // step)
        where = slice(b * block, (b + 1) * block)
        up = (tab["up"][0, start : start + coarse, :], tab["up"][1, start : start + coarse, :])
        intensity = product(image_pair, up)
        resist = 1.0 / (1.0 + jnp.exp(-steepness * (intensity - threshold)))
        misfit = resist - target[:, where].astype(F32)
        slope = (2.0 * steepness) * misfit * resist * (1.0 - resist)
        square = misfit * misfit
        squares = squares + square[:, :LANES] + square[:, LANES:]
        keep(slopes, slice(0, rows), where, slope)
    pull[...] = product((slopes[0], slopes[1]), (up_t[0], up_t[1]))
    squares = lane_sum(jnp.sum(squares, 0, keepdims=True))

    loads["half_yt"].wait()
    loads["half_xt"].wait()
    grads[...] = jnp.zeros_like(grads)
    half_xt = tab["half_xt"]

    def weigh(s, slot):
        dest = weighed.at[slot]
        total = jnp.zeros((2 * SUB, coarse), F32)
        for start in range(0, rows, 2 * SUB):
            where = slice(start, start + 2 * SUB)
            other = slice(start + rows, start + rows + 2 * SUB)
            weak, re, im = pull[where, :], fields[s, where, :], fields[s, other, :]
            down_r, down_i = weak * re, weak * im
            total = total + (down_r * re + down_i * im)
            keep(dest, where, slice(None), down_r)
            keep(dest, other, slice(None), down_i)
        total = total[:SUB] + total[SUB:]
        totals[s] = total[:, :h] + total[:, h : 2 * h] + total[:, 2 * h : 3 * h] + total[:, 3 * h :]

    def from_field(s, slot):
        settle = product((weighed[slot, 0], weighed[slot, 1]), both("half_yt")) * (2.0 * share_of(s))
        for part in range(2):
            high, low = split(settle[part * rows : (part + 1) * rows])
            settled[slot, :rows, part * 2 * h : (part + 1) * 2 * h] = high
            settled[slot, rows:, part * 2 * h : (part + 1) * 2 * h] = low

    def from_rows(s, slot):
        kept = masks(s)
        dims = (((1,), (0,)), ((), ()))
        full = lax.dot_general(half_xt[:, : 2 * rows], settled[slot], dims, preferred_element_type=F32)
        full = full + lax.dot_general(
            half_xt[:, 2 * rows :], settled[slot, :rows], dims, preferred_element_type=F32
        )
        for where in chunk_rows:
            keeps = kept(where)
            top, low = full[where], full[where.start + h : where.stop + h]
            ee_r, no_i, ee_i, eo_r = (top[:, q] for q in quarter)
            oe_i, oo_r, ne_r, oo_i = (low[:, q] for q in quarter)
            ep, em, op, om = ee_r + eo_r, ee_r - eo_r, oo_r - ne_r, -ne_r - oo_r
            for q, value in enumerate((ep + op, em + om, ep - op, em - om)):
                grads[q, 0, where, :] += jnp.where(keeps[q], value, 0.0)
            ep, em, op, om = ee_i - no_i, ee_i + no_i, oe_i + oo_i, oe_i - oo_i
            for q, value in enumerate((ep + op, em + om, ep - op, em - om)):
                grads[q, 1, where, :] += jnp.where(keeps[q], value, 0.0)

    def backward(i, carry):
        base = i * unroll
        for t in range(unroll + 2):
            if t < unroll:
                weigh(base + t, t)
            if 0 <= t - 1 < unroll:
                from_field(base + t - 1, t - 1)
            if 0 <= t - 2 < unroll:
                from_rows(base + t - 2, t - 2)
        return carry

    lax.fori_loop(0, sources // unroll, backward, 0)
    each = lane_sum(jnp.sum(totals[...], 1))
    own = lax.broadcasted_iota(jnp.int32, (sources, LANES), 0) == lane
    sums = jnp.sum(jnp.where(own, each, 0.0), 0, keepdims=True)
    sums = jnp.where(lane == sources, squares, sums)

    def unturn(slot, sign):
        s = turn_s if sign > 0 else -turn_s
        re, im = grads[slot, 0], grads[slot, 1]
        return re * turn_c + im * s, im * turn_c - re * s

    pp, pm, mp, mm = unturn(0, 1), unturn(1, 1), unturn(2, -1), unturn(3, -1)
    pieces = ((pp[0], mm[0]), (pm[0], mp[0]), (-pp[1], mm[1]), (-pm[1], mp[1]))
    last_row = jnp.zeros((1, LANES), F32)
    for i, (first, second) in enumerate(pieces):
        ext[...] = jnp.zeros_like(ext)
        if i in (0, 2):
            ext[1 : h + 1, :h] = second
            moved = pltpu.roll(ext[...], 1, 1)
            ext[...] = moved
            ext[:h, :h] += first
        else:
            ext[:h, :h] = first
            moved = pltpu.roll(ext[...], 1, 1)
            ext[...] = moved
            ext[1 : h + 1, :h] += second
        grad_t[i] = ext[:h, :h].T.reshape(chips, 2, SUB, h)
        copy_to(8, partner, grad_t.at[i, :, 1 - core], pair_in.at[i]).start()
        edge_back[i] = ext[h : h + 1, :h]
        edge_back[4 + i] = ext[:h, h:].T[0:1, :]
        last_row = jnp.where(lane == i, ext[h : h + 1, h : h + 1], last_row)
    edge_back[8] = last_row
    edge_back[9] = sums
    for i in range(10, devices):
        edge_back[i] = jnp.zeros((1, LANES), F32)

    send_all(5, lambda p: edge_back.at[p], edge_back_in.at[me])
    edge_back_in[me] = edge_back[me]
    wait_all(8, pair_in)
    for i in range(4):
        pair_sum[:, i] = grad_t[i, :, core] + pair_in[i]

    def hand_over(i, carry):
        peer = lax.rem(me + 2 * i, devices)
        copy_to(4, peer, pair_sum.at[peer // 2], grad_in.at[chip]).start()
        return carry

    lax.fori_loop(1, chips, hand_over, 0)
    grad_in[chip] = pair_sum[chip]
    wait_all(4, grad_in.at[pl.ds(0, chips - 1)])

    def unmix(u, v, wp, wm):
        return u + v, wp - wm, wp + wm, v - u

    mine = jnp.sum(grad_in[...], 0)
    cc, cs, sc, ss = unmix(mine[0], mine[1], mine[2], mine[3])
    sum_c = jnp.concatenate([cc, cs], 0)[None]
    sum_s = jnp.concatenate([sc, ss], 0)[None]
    back_c = far_c * sum_c + far_s * sum_s
    back_s = far_c * sum_s - far_s * sum_c
    turned = jnp.concatenate([back_c, back_s], 2).reshape(devices * 2 * SUB, 2 * h)
    gathered = product(split(turned), both("wave_x"), flip=True)
    back_rows[...] = gathered.reshape(devices, 2, SUB, rows)
    send_all(6, lambda p: back_rows.at[p], back_in.at[:, pl.ds(me * SUB, SUB), :])
    back_in[:, pl.ds(me * SUB, SUB), :] = back_rows[me]
    wait_all(5, edge_back_in.at[most])
    edge_back_all[me] = jnp.sum(edge_back_in[...], 0)
    send_all(7, lambda p: edge_back_all.at[me], edge_back_all.at[me])
    wait_all(7, edge_back_all.at[most])

    sums = edge_back_all[9]
    small_at = slice(2 * h + LANES, 2 * h + 2 * LANES)
    result[0:1, small_at] = sums * norming
    sums = jnp.where(lane < sources, sums, 0.0)
    result[1:2, small_at] = share_row * (sums - lane_sum(share_row * sums)) * norming
    result[2:3, small_at] = group_row.astype(F32)

    side_x = unmix(*(edge_back_all[i] for i in range(4)))
    side_y = unmix(*(edge_back_all[4 + i] for i in range(4)))
    corner = unmix(*(lane_sum(jnp.where(lane == i, edge_back_all[8], 0.0)) for i in range(4)))
    far_c, far_s = tab["far"][0, me], tab["far"][1, me]
    near = []
    for c, s in ((side_y[0], side_y[2]), (side_y[1], side_y[3])):
        near.append(jnp.concatenate([far_c * c + far_s * s, far_c * s - far_s * c], 1))
    near = jnp.concatenate(near + [jnp.zeros((SUB - 2, 2 * h), F32)], 0)
    last = product(split(near), both("wave_x"), flip=True)
    edge_c, edge_s = edge_rows[0:1], edge_rows[1:2]
    last_c = last[0:1] + corner[0] * edge_c + corner[2] * edge_s
    last_s = last[1:2] + corner[1] * edge_c + corner[3] * edge_s
    result[:, 2 * h : 2 * h + LANES] = column(last_c) * edge_c + column(last_s) * edge_s
    col_c, col_s = column(edge_c), column(edge_s)

    wait_all(6, back_in.at[:, pl.ds(0, h - SUB), :])
    part_c = back_in[0].T + col_c * side_x[0] + col_s * side_x[2]
    part_s = back_in[1].T + col_c * side_x[1] + col_s * side_x[3]
    result[:, :h] = part_c
    result[:, h : 2 * h] = part_s
    drain(0, rows_in.at[most])
    drain(1, edge_in.at[most])
    drain(2, chunk.at[most])
    drain(3, edge_all.at[most])
    drain(4, grad_in.at[pl.ds(0, chips - 1)])
    drain(5, edge_back_in.at[most])
    drain(6, back_in.at[:, pl.ds(0, h - SUB), :])
    drain(7, edge_back_all.at[most])
    drain(8, pair_in)


def closing(n, sources, result, wave, loss_hbm, grad_hbm, group_hbm, loss, group, out, out_sem):
    block = 2 * LANES
    blocks = n // block
    lane = lax.broadcasted_iota(jnp.int32, (1, LANES), 1)
    h = K // 2
    small = result.at[:, 2 * h + LANES :]
    loss[0] = jnp.sum(jnp.where(lane == sources, small[0:1, :], 0.0))
    for g in range(NG):
        group[g] = jnp.sum(jnp.where(small[2:3, :] == g, small[1:2, :], 0.0))
    stores = [
        pltpu.make_async_copy(loss, loss_hbm, out_sem.at[blocks]),
        pltpu.make_async_copy(group, group_hbm, out_sem.at[blocks + 1]),
    ]
    for store in stores:
        store.start()
    pair = split(result[:, : 2 * h])
    spread = result[:, 2 * h : 2 * h + LANES]
    adds = jnp.concatenate([spread, spread], 1)
    for b in range(blocks):
        where = slice(b * block, (b + 1) * block)
        out[:, where] = product(pair, (wave[0, :, where], wave[1, :, where])) + adds
        stores.append(pltpu.make_async_copy(out.at[:, where], grad_hbm.at[:, where], out_sem.at[b]))
        stores[-1].start()
    for store in stores:
        store.wait()


def fused(devices, mask_field, target_print, source_points, source_groups, group_logits, pupil_radius):
    rows, n = mask_field.shape
    h = K // 2
    coarse = 2 * K
    sources = source_points.shape[0]
    consts = tables(n, rows, devices)
    anywhere = pl.BlockSpec(memory_space=pltpu.HBM)
    vmem = lambda *shape: pltpu.VMEM(shape, F32)
    scratch = [pltpu.VMEM(consts[k].shape, consts[k].dtype) for k in NAMES] + [
        vmem(rows, n), pltpu.VMEM((rows, n), jnp.int32),
        vmem(2, h, rows), vmem(devices, 1, LANES), vmem(devices, 2, SUB, rows), vmem(devices, 1, LANES),
        vmem(devices, 4, SUB, h), vmem(devices, 1, LANES), vmem(h + SUB, 2 * h), vmem(4, 2, h, h),
        vmem(4, 2, h, h), vmem(sources, 2 * rows, coarse), vmem(rows, coarse), vmem(rows, coarse),
        vmem(4, 2, h, h), vmem(4, devices // 2, 2, SUB, h), vmem(devices, 1, LANES), vmem(devices // 2, 4, SUB, h),
        vmem(devices, 1, LANES), vmem(devices, 1, LANES), vmem(devices, 2, SUB, rows), vmem(2, h, rows),
        pltpu.VMEM((8, 2, 2 * h, coarse), BF16), pltpu.VMEM((8, 2, 2 * rows, 2 * h), BF16),
        pltpu.VMEM((8, 2, 2 * rows, coarse), BF16), pltpu.VMEM((8, 2 * rows, coarse), BF16),
        vmem(sources, SUB, LANES),
        pltpu.SMEM((2, sources), jnp.int32), pltpu.SMEM((sources,), jnp.int32), pltpu.SMEM((NG,), F32),
        pltpu.SMEM((1,), jnp.int32),
        vmem(4, devices // 2, SUB, h), vmem(devices // 2, 4, SUB, h),
        pltpu.VMEM((2, n, coarse), BF16), pltpu.VMEM((2, rows, n), BF16),
        pltpu.SemaphoreType.DMA((24,)),
        pltpu.SemaphoreType.DMA((9,)), pltpu.SemaphoreType.DMA((9,)), pltpu.SemaphoreType.DMA((devices // 2,)),
    ]
    arrays = [jnp.asarray(consts[k]) for k in NAMES]
    hold = lambda value: pltpu.with_memory_space_constraint(value, pltpu.HBM)
    inside = pl.BlockSpec(memory_space=pltpu.VMEM)
    (result,) = pl.pallas_call(
        functools.partial(kernel, devices, n),
        out_shape=(
            jax.ShapeDtypeStruct((rows, 2 * h + 2 * LANES), F32),
        ),
        in_specs=[anywhere] * (6 + len(NAMES)),
        out_specs=(inside,),
        scratch_shapes=scratch,
        compiler_params=pltpu.CompilerParams(
            collective_id=0, has_side_effects=True, vmem_limit_bytes=53 * 1024 * 1024
        ),
    )(*map(hold, (source_points.T, source_groups, group_logits)), pupil_radius,
      *map(hold, (mask_field, target_print, *arrays)))
    return pl.pallas_call(
        functools.partial(closing, n, sources),
        out_shape=(
            jax.ShapeDtypeStruct((1,), F32),
            jax.ShapeDtypeStruct((rows, n), F32),
            jax.ShapeDtypeStruct((NG,), F32),
        ),
        in_specs=[inside] * 2,
        out_specs=(anywhere, anywhere, anywhere),
        scratch_shapes=[
            pltpu.SMEM((1,), F32), pltpu.SMEM((NG,), F32), vmem(rows, n),
            pltpu.SemaphoreType.DMA((n // (2 * LANES) + 2,)),
        ],
        compiler_params=pltpu.CompilerParams(vmem_limit_bytes=8 * 1024 * 1024),
    )(result, arrays[0])


HIGH = lax.Precision.HIGH


def dot(form, left, right):
    return jnp.einsum(form, left, right, precision=HIGH, preferred_element_type=F32)


def waves(left, right, length):
    turns = angles(left, right, length)
    return np.cos(turns), np.sin(turns)


def shifted_waves(count, freq, length, device, devices):
    near = np.stack(waves(np.arange(count), freq, length)).astype(np.float32)
    far = np.stack(waves(np.arange(devices) * count, freq, length)).astype(np.float32)
    far = lax.dynamic_slice_in_dim(jnp.asarray(far), device, 1, axis=1)
    return far[0] * near[0] - far[1] * near[1], far[1] * near[0] + far[0] * near[1]


def exchange(blocks):
    return lax.all_to_all(blocks, "slab", 0, 0)


def plain(devices, mask_field, target_print, source_points, source_groups, group_logits, pupil_radius):
    rows, n = mask_field.shape
    sources = source_points.shape[0]
    coarse = 2 * K
    step = n // coarse
    cols = coarse // devices
    half = n // 2
    device = lax.axis_index("slab")
    freq = np.arange(K, dtype=np.int64) - K // 2
    order = np.concatenate([freq[freq % 2 == 0], freq[freq % 2 == 1]])
    kh = K // 2
    norming = 1.0 / (n * n)

    cos_y, sin_y = waves(np.arange(half), order, n)
    fold = [
        jnp.asarray(np.concatenate([t[:, p * kh : (p + 1) * kh] for t in (cos_y, sin_y)], 1), F32)
        for p in (0, 1)
    ]
    lag = np.mod(np.arange(n)[None, :] - step * np.arange(coarse)[:, None], n)
    response = np.zeros(n)
    for f in range(1, K):
        response += 2.0 * np.cos(2.0 * math.pi * np.mod(f * np.arange(n), n) / n)
    response = (response + 1.0) / coarse
    up = jnp.asarray(response[lag], F32)
    cos_c, sin_c = waves(freq, np.arange(coarse), coarse)
    wave_x = jnp.asarray(np.concatenate([cos_c, sin_c], 1), F32)
    loc_c, loc_s = shifted_waves(rows, freq, n, device, devices)
    loc = jnp.concatenate([loc_c, loc_s], 1)
    a, b = shifted_waves(cols, order, coarse, device, devices)
    lift = jnp.concatenate([jnp.concatenate([a, -b], 1), jnp.concatenate([b, a], 1)], 0)

    cutoff = pupil_radius[0]
    shifted = (source_points - GRID // 2) * cutoff // shift_scale
    first = jnp.asarray(freq, jnp.int32)[None, None, :] + shifted[:, 0, None, None]
    second = jnp.asarray(np.tile(order, 2), jnp.int32)[None, :, None] + shifted[:, 1, None, None]
    passed = first * first + second * second <= cutoff * cutoff

    near, away = mask_field[:, :half], mask_field[:, half:]
    even = dot("xy,yq->xq", near + away, fold[0])
    odd = dot("xy,yq->xq", near - away, fold[1])
    part_c = jnp.concatenate([even[:, :kh], odd[:, :kh]], 1)
    part_s = jnp.concatenate([even[:, kh:], odd[:, kh:]], 1)
    spec = dot("xq,xk->qk", jnp.concatenate([part_c, part_s], 1), loc)
    band = jnp.concatenate([spec[:K, :K] - spec[K:, K:], -(spec[:K, K:] + spec[K:, :K])], 0)
    band = jnp.sum(exchange(band.reshape(devices, 2 * K // devices, K)), 0)
    band = lax.all_gather(band, "slab", tiled=True)

    kept = jnp.where(passed, band[None], 0.0)
    wide = dot("aq,sqk->sak", lift, kept)
    both = dot("ak,kx->ax", wide.reshape(sources * 2 * cols, K), wave_x)
    both = both.reshape(sources, 2, cols, 2 * coarse)
    field_re = (both[:, 0, :, :coarse] - both[:, 1, :, coarse:]) * norming
    field_im = (both[:, 0, :, coarse:] + both[:, 1, :, :coarse]) * norming
    bright = field_re * field_re + field_im * field_im
    onehot = (source_groups[:, None] == jnp.arange(NG, dtype=jnp.int32)[None, :]).astype(F32)
    weights = jnp.exp(jnp.sum(onehot * group_logits[None, :], 1))
    share = weights / jnp.sum(weights)
    image = jnp.sum(share[:, None, None] * bright, 0)

    tall = dot("cm,mx->cx", image, up)
    tall = lax.all_to_all(tall, "slab", 1, 0, tiled=True)
    intensity = dot("cx,cy->xy", tall, up)
    resist = jax.nn.sigmoid(steepness * (intensity - threshold))
    misfit = resist - target_print.astype(F32)
    slope = (2.0 * steepness) * misfit * resist * (1.0 - resist)
    squares = jnp.sum(misfit * misfit)
    down = dot("xy,cy->cx", slope, up)
    down = lax.all_to_all(down, "slab", 0, 1, tiled=True)
    pull = dot("cx,mx->cm", down, up)

    per_source = jnp.sum(bright * pull[None], (1, 2))
    sums = jnp.concatenate([per_source, squares[None]])
    factor = (2.0 * norming) * share[:, None, None] * pull[None]
    back = jnp.stack([factor * field_re, factor * field_im], 1)
    low = dot("ax,kx->ak", back.reshape(sources * 2 * cols, coarse), wave_x[:, :coarse])
    lows = dot("ax,kx->ak", back.reshape(sources * 2 * cols, coarse), wave_x[:, coarse:])
    low = low.reshape(sources, 2, cols, K)
    lows = lows.reshape(sources, 2, cols, K)
    settle = jnp.concatenate([low[:, 0] + lows[:, 1], low[:, 1] - lows[:, 0]], 1)
    settle = dot("aq,sak->sqk", lift, settle)
    grad_band = jnp.sum(jnp.where(passed, settle, 0.0), 0).reshape(devices, 2 * K // devices, K)
    extra = jnp.pad(sums[None, :], ((0, 7), (0, K - sources - 1)))
    extra = jnp.broadcast_to(extra[None], (devices, 8, K))
    grad_band = jnp.sum(exchange(jnp.concatenate([grad_band, extra], 1)), 0)
    sums = grad_band[-8, : sources + 1]
    grad_band = lax.all_gather(grad_band[:-8], "slab", tiled=True)
    per_source, squares = sums[:-1], sums[-1]
    loss_value = (squares * norming).reshape(1)
    against = jnp.sum(share * per_source)
    source_pull = share * (per_source - against)
    group_grad = jnp.sum(onehot * source_pull[:, None], 0) * norming

    spread = dot("tk,qk->tq", jnp.concatenate([loc_c, loc_s], 0), grad_band)
    spread_re = spread[:rows, :K] - spread[rows:, K:]
    spread_im = spread[:rows, K:] + spread[rows:, :K]
    even = dot("xq,yq->xy", jnp.concatenate([spread_re[:, :kh], -spread_im[:, :kh]], 1), fold[0])
    odd = dot("xq,yq->xy", jnp.concatenate([spread_re[:, kh:], -spread_im[:, kh:]], 1), fold[1])
    mask_grad = jnp.concatenate([even + odd, even - odd], 1)
    return loss_value, mask_grad, group_grad


def on_device(devices, mask_field, *others):
    tiles = mask_field.shape[0] == LANES and K // 2 == LANES == SUB * devices and devices >= 10
    return (fused if tiles else plain)(devices, mask_field, *others)


def solution(mesh):
    in_specs = (
        P(("clip", "slab"), None),
        P(("clip", "slab"), None),
        P("clip", None),
        P("clip"),
        P("clip"),
        P("clip"),
    )
    out_specs = (P("clip"), P(("clip", "slab"), None), P("clip"))
    return jax.shard_map(
        functools.partial(on_device, mesh.shape["slab"]),
        mesh=mesh, in_specs=in_specs, out_specs=out_specs, check_vma=False,
    )
```

```python
import functools
import math

import jax
import jax.numpy as jnp
import numpy as np
from jax import lax
from jax.experimental import pallas as pl
from jax.experimental.pallas import tpu as pltpu
from jax.sharding import PartitionSpec as P

K = 256
GRID = 61
NG = 8

steepness = 8.0
threshold = 0.3
shift_scale = 45
F32 = jnp.float32
BF16 = jnp.bfloat16
LANES = 128
SUB = 8


def angles(left, right, length):
    turns = np.mod(np.asarray(left)[:, None] * np.asarray(right)[None, :], length)
    return 2.0 * math.pi * turns.astype(np.float64) / length


def halves(table):
    table = np.asarray(table, np.float32)
    high = table.astype(BF16)
    low = (table - high.astype(np.float32)).astype(BF16)
    return np.stack([high, low])


def split(value):
    high = value.astype(BF16)
    return high, (value - high.astype(F32)).astype(BF16)


def product(left, right, flip=False):
    dims = (((1,), (1 if flip else 0,)), ((), ()))
    one = lambda a, b: lax.dot_general(a, b, dims, preferred_element_type=F32)
    return one(left[0], right[0]) + one(left[1], right[0]) + one(left[0], right[1])


def tables(n, rows, devices):
    h = K // 2
    coarse = 2 * K
    step = n // coarse
    freq = np.arange(h)
    near = np.arange(rows)
    wave_y = angles(freq, np.arange(n), n)
    wave_y = np.concatenate([np.cos(wave_y), np.sin(wave_y)], 0)
    wave_x = angles(near, freq, n)
    wave_x = np.concatenate([np.cos(wave_x), np.sin(wave_x)], 1)
    half_x = angles(near, 2 * freq + 1, 2 * n)
    half_x = np.concatenate([np.cos(half_x), -np.sin(half_x)], 1)
    spots = step * np.arange(coarse // 2) + step // 2
    half_y = angles(2 * freq + 1, spots, 2 * n)
    half_y = [halves(np.cos(half_y)), halves(np.sin(half_y))]
    ahead = np.stack([np.concatenate([t[0], t[0], t[1]], 0) for t in half_y])
    behind = np.stack([
        np.block([[t[0].T, t[1].T], [t[0].T, np.zeros_like(t[0].T)]]) for t in half_y
    ])
    far = angles(rows * np.arange(devices), freq, n)
    far = np.stack([np.cos(far), np.sin(far)])[:, :, None, :].astype(np.float32)
    half_far = angles(rows * np.arange(devices), 2 * freq + 1, 2 * n)
    half_far = np.stack([np.cos(half_far), np.sin(half_far)]) / (n * n)
    half_far = half_far[:, :, None, :].astype(np.float32)
    block = 2 * LANES
    extra = n // step - block // step
    index = np.arange(coarse // 2 + extra)[:, None]
    spot = np.concatenate([step * (index - extra) + step // 2, -step * index - step // 2], 0)
    lag = np.mod(np.arange(block)[None, :] - spot, n)
    kernel = np.ones(n)
    for f in range(1, K):
        kernel += 2.0 * np.cos(2.0 * math.pi * np.mod(f * np.arange(n), n) / n)
    up = (kernel / coarse)[lag]
    edge = angles([h], np.arange(LANES), n)
    edge = np.concatenate([np.cos(edge), np.sin(edge)], 0)
    edge = np.concatenate([edge, np.zeros((SUB - 2, LANES))], 0)
    return {
        "wave_y": halves(wave_y),
        "wave_x": halves(wave_x),
        "half_x": halves(half_x),
        "half_xt": np.concatenate(list(halves(half_x.T)[[0, 0, 1]]), 1),
        "half_y": ahead,
        "half_yt": behind,
        "up": halves(up),
        "far": far,
        "half_far": half_far,
        "edge": edge.astype(np.float32),
    }


NAMES = ("wave_y", "wave_x", "half_x", "half_xt", "half_y", "half_yt", "up", "far", "half_far", "edge")


def kernel(devices, n, *refs):
    small_hbm, mask_hbm, target_hbm = refs[:4], refs[4], refs[5]
    sources_in = dict(zip(NAMES, refs[6 : 6 + len(NAMES)]))
    refs = refs[6 + len(NAMES) :]
    result = refs[0]
    refs = refs[1:]
    tab = dict(zip(NAMES, refs[: len(NAMES)]))
    refs = refs[len(NAMES) :]
    (mask, target, rows_t, edge_out, rows_in, edge_in, chunk, edge_all, ext, band, data, fields, image, pull,
     grads, grad_t, edge_back, grad_in, edge_back_in, edge_back_all, back_rows, back_in,
     folded, wides, weighed, settled, totals, points, groups, logits, radius,
     pair_in, pair_sum, up_t, slopes, local_sem, send_sem, recv_sem, near_sem) = refs
    h = K // 2
    coarse = 2 * K
    sources = points.shape[1]
    rows = mask.shape[0]
    block = 2 * LANES
    blocks = n // block
    step = n // coarse
    me = lax.axis_index("slab")
    norming = 1.0 / (n * n)
    chips = devices // 2
    core, chip = lax.rem(me, 2), me // 2
    partner = me + 1 - 2 * core
    most = pl.ds(0, devices - 1)

    loads = {}
    small = (points, groups, logits, radius)
    pieces = [slice(c, c + n // 4) for c in range(0, n, n // 4)]
    for i, (name, src, dst) in enumerate(
        [
            piece
            for k, where in enumerate(pieces)
            for piece in (
                (f"mask{k}", mask_hbm.at[:, where], mask.at[:, where]),
                (f"wave_y{k}", sources_in["wave_y"].at[:, :, where], tab["wave_y"].at[:, :, where]),
            )
        ]
        + [(f"small{k}", small_hbm[k], small[k]) for k in range(4)]
        + [(k, sources_in[k], tab[k]) for k in ("edge", "wave_x", "far", "half_far", "half_x", "half_y")]
        + [("up", sources_in["up"], tab["up"]), ("target", target_hbm, target)]
        + [(k, sources_in[k], tab[k]) for k in ("half_yt", "half_xt")]
    ):
        loads[name] = pltpu.make_async_copy(src, dst, local_sem.at[i])
        loads[name].start()

    barrier = pltpu.get_barrier_semaphore()

    def greet(i, carry):
        pl.semaphore_signal(barrier, inc=1, device_id={"slab": lax.rem(me + i, devices)})
        return carry

    lax.fori_loop(1, devices, greet, 0)

    def both(name):
        return tab[name][0], tab[name][1]

    def copy_to(phase, peer, src, dst, sem=None):
        return pltpu.make_async_remote_copy(
            src_ref=src, dst_ref=dst, send_sem=send_sem.at[phase],
            recv_sem=recv_sem.at[phase] if sem is None else sem, device_id={"slab": peer},
        )

    group = 4
    planes = devices // group
    lower = 1 - me // (group * (planes // 2))

    def plane_of(i):
        return lower * (planes - 1 - 2 * i) + i

    def send_all(phase, src_of, dst):
        for i in range(devices):
            peer = plane_of(i // group) * group + lax.rem(me + i % group, group)

            @pl.when(peer != me)
            def _():
                copy_to(phase, peer, src_of(peer), dst).start()

    def each_chip(act, reverse=False):
        for i in range(chips)[:: -1 if reverse else 1]:
            other = plane_of(i // 2) * 2 + lax.rem(chip + i % 2, 2)

            @pl.when(other != chip)
            def _():
                act(other * 2 + core)

    def wait_all(phase, ref, sem=None):
        copy_to(phase, partner, ref, ref, sem).wait_recv()

    def drain(phase, ref):
        copy_to(phase, partner, ref, ref).wait_send()

    lane = lax.broadcasted_iota(jnp.int32, (1, LANES), 1)

    def column(row):
        return jnp.broadcast_to(row, (LANES, LANES)).T

    transformed = 0.0
    for k, where in enumerate(pieces):
        loads[f"mask{k}"].wait()
        loads[f"wave_y{k}"].wait()
        wave = (tab["wave_y"][0, :, where], tab["wave_y"][1, :, where])
        transformed = transformed + product(split(mask[:, where]), wave, flip=True)
    rows_t[0] = transformed[:, :h].T
    rows_t[1] = transformed[:, h:].T
    loads["edge"].wait()
    loads["wave_x"].wait()
    loads["far"].wait()
    edge_rows = tab["edge"][...]
    edge_pair = split(edge_rows)
    summed = mask[:, :LANES]
    for b in range(1, n // LANES):
        summed = summed + mask[:, b * LANES : (b + 1) * LANES]
    side_x = product(edge_pair, split(transformed))
    last = product(edge_pair, split(summed), flip=True)
    side_y = product(split(last), both("wave_x"))
    far_c, far_s = tab["far"][0, me], tab["far"][1, me]
    side_c = far_c * side_y[:2, :h] - far_s * side_y[:2, h:]
    side_s = far_s * side_y[:2, :h] + far_c * side_y[:2, h:]

    def mixes(cc, cs, sc, ss):
        return cc - ss, cc + ss, sc + cs, sc - cs

    edges = mixes(side_x[0:1, :h], side_x[0:1, h:], side_x[1:2, :h], side_x[1:2, h:])
    edges = edges + mixes(side_c[0:1], side_c[1:2], side_s[0:1], side_s[1:2])

    def lane_sum(value):
        return jnp.sum(value, axis=1, keepdims=True)

    corner = mixes(
        lane_sum(last[0:1] * edge_rows[0:1]), lane_sum(last[1:2] * edge_rows[0:1]),
        lane_sum(last[0:1] * edge_rows[1:2]), lane_sum(last[1:2] * edge_rows[1:2]),
    )
    corner_row = jnp.zeros((1, LANES), F32)
    for i in range(4):
        corner_row = jnp.where(lane == i, corner[i], corner_row)
    for i in range(8):
        edge_out[i] = edges[i]
    edge_out[8] = corner_row
    for i in range(9, devices):
        edge_out[i] = jnp.zeros((1, LANES), F32)

    pl.semaphore_wait(barrier, devices - 1)
    send_all(1, lambda p: edge_out.at[p], edge_in.at[me])
    send_all(0, lambda p: rows_t.at[:, pl.ds(p * SUB, SUB), :], rows_in.at[me])
    rows_in[me] = rows_t[:, pl.ds(me * SUB, SUB), :]
    edge_in[me] = edge_out[me]

    for k in range(4):
        loads[f"small{k}"].wait()
    logit_row = jnp.full((1, LANES), 0.0, F32)
    group_row = jnp.full((1, LANES), -1, jnp.int32)
    for s in range(sources):
        g = groups[s]
        logit_row = jnp.where(lane == s, logits[g], logit_row)
        group_row = jnp.where(lane == s, g, group_row)
    weight_row = jnp.where(lane < sources, jnp.exp(logit_row), 0.0)
    share_row = weight_row / jnp.sum(weight_row, axis=1, keepdims=True)

    loads["up"].wait()
    extra = (n - block) // step

    def taps(b):
        first, second = extra - b * (block // step), extra + 2 * h + b * (block // step)
        return slice(first, first + 2 * h), slice(second, second + 2 * h)

    for b in range(blocks):
        for part in range(2):
            for side, spot in enumerate(taps(b)):
                up_t[part, b * block : (b + 1) * block, side * 2 * h : (side + 1) * 2 * h] = tab["up"][part, spot, :].T

    wait_all(1, edge_in.at[most])
    edge_all[me] = jnp.sum(edge_in[...], 0)
    send_all(3, lambda p: edge_all.at[me], edge_all.at[me])
    wait_all(0, rows_in.at[most])
    gathered = rows_in[...].reshape(devices * 2 * SUB, rows)
    turned = product(split(gathered), both("wave_x")).reshape(devices, 2 * SUB, 2 * h)
    far_c, far_s = tab["far"][0], tab["far"][1]
    turned_c, turned_s = turned[:, :, :h], turned[:, :, h:]
    sum_c = jnp.sum(far_c * turned_c - far_s * turned_s, 0)
    sum_s = jnp.sum(far_s * turned_c + far_c * turned_s, 0)
    for i, value in enumerate(mixes(sum_c[:SUB], sum_c[SUB:], sum_s[:SUB], sum_s[SUB:])):
        chunk[me, i] = value

    each_chip(lambda peer: copy_to(2, peer, chunk.at[me], chunk.at[me], near_sem.at[chip]).start())
    copy_to(2, partner, chunk.at[me], chunk.at[me]).start()

    loads["half_far"].wait()
    loads["half_x"].wait()
    loads["half_y"].wait()
    turn_c = column(tab["half_far"][0, me])
    turn_s = column(tab["half_far"][1, me])


    def relay(peer):
        wait_all(2, chunk.at[peer], near_sem.at[peer // 2])
        copy_to(2, partner, chunk.at[peer], chunk.at[peer]).start()

    each_chip(relay, reverse=True)
    wait_all(2, chunk.at[pl.ds(0, chips)])
    wait_all(3, edge_all.at[most])
    shifted = []
    plain = []
    for i in range(4):
        ext[:h, :h] = chunk[:, i].reshape(h, h).T
        ext[h : h + 1, :h] = edge_all[i]
        ext[:h, h:] = column(edge_all[4 + i])
        ext[h : h + 1, h:] = jnp.broadcast_to(lane_sum(jnp.where(lane == i, edge_all[8], 0.0)), (1, LANES))
        plain = ext[...]
        moved = pltpu.roll(plain, 2 * h - 1, 1)
        if i in (0, 2):
            first, second = ext[:h, :h], None
            ext[...] = moved
            second = ext[1 : h + 1, :h]
        else:
            second = ext[1 : h + 1, :h]
            ext[...] = moved
            first = ext[:h, :h]
        data[i, 0] = first
        data[i, 1] = second

    def turn(slot, re, im, sign):
        s = turn_s if sign > 0 else -turn_s
        band[slot, 0] = re * turn_c - im * s
        band[slot, 1] = re * s + im * turn_c

    turn(0, data[0, 0], -data[2, 0], 1)
    turn(1, data[1, 0], -data[3, 0], 1)
    turn(2, data[1, 1], data[3, 1], -1)
    turn(3, data[0, 1], data[2, 1], -1)

    cutoff = radius[0]
    limit = (cutoff * cutoff).astype(F32)
    lane_index = lane.astype(F32)
    chunk_rows = [slice(c, c + 2 * SUB) for c in range(0, h, 2 * SUB)]
    row_index = lax.broadcasted_iota(jnp.int32, (2 * SUB, LANES), 0).astype(F32)

    def masks(s):
        first = ((points[0, s] - GRID // 2) * cutoff // shift_scale).astype(F32)
        second = ((points[1, s] - GRID // 2) * cutoff // shift_scale).astype(F32)
        col_p, col_m = lane_index + second, second - 1.0 - lane_index
        col_p, col_m = col_p * col_p, col_m * col_m

        def of(where):
            row_p = row_index + (first + where.start)
            row_m = (first - 1.0 - where.start) - row_index
            room_p, room_m = limit - row_p * row_p, limit - row_m * row_m
            return col_p <= room_p, col_m <= room_p, col_p <= room_m, col_m <= room_m

        return of

    def share_of(s):
        return lane_sum(jnp.where(lane == s, share_row, 0.0))

    def keep(ref, where, lanes, value):
        high, low = split(value)
        ref[0, where, lanes] = high
        ref[1, where, lanes] = low

    unroll = 8
    quarter = [slice(i * h, (i + 1) * h) for i in range(4)]
    image[...] = jnp.zeros_like(image)

    def mask_band(s, slot):
        kept = masks(s)
        dest = folded.at[slot]
        for where in chunk_rows:
            keeps = kept(where)
            low_where = slice(where.start + h, where.stop + h)
            pp, pm, mp, mm = (jnp.where(keeps[q], band[q, 0, where, :], 0.0) for q in range(4))
            ep, em, op, om = pp + mp, pm + mm, mp - pp, mm - pm
            keep(dest, where, quarter[0], ep + em)
            keep(dest, where, quarter[3], ep - em)
            keep(dest, low_where, quarter[1], om - op)
            keep(dest, low_where, quarter[2], op + om)
            pp, pm, mp, mm = (jnp.where(keeps[q], band[q, 1, where, :], 0.0) for q in range(4))
            ep, em, op, om = pp + mp, pm + mm, pp - mp, pm - mm
            keep(dest, where, quarter[1], em - ep)
            keep(dest, where, quarter[2], ep + em)
            keep(dest, low_where, quarter[0], op + om)
            keep(dest, low_where, quarter[3], op - om)

    dims = (((1,), (0,)), ((), ()))

    def once(left, right):
        return lax.dot_general(left, right, dims, preferred_element_type=F32)

    def to_rows(slot):
        wide = product(both("half_x"), (folded[slot, 0], folded[slot, 1]))
        for part in range(2):
            for side in range(2):
                high, low = split(wide[:, quarter[2 * part + side]])
                wides[slot, side, part * rows : (part + 1) * rows, :h] = high
                wides[slot, side, part * rows : (part + 1) * rows, h:] = low

    def to_field(s, slot):
        even, odd = (
            once(wides[slot, side], tab["half_y"][side, : 2 * h])
            + once(wides[slot, side, :, :h], tab["half_y"][side, 2 * h :])
            for side in range(2)
        )
        weight = share_of(s)
        for side, field in enumerate((even + odd, even - odd)):
            where = slice(side * 2 * h, (side + 1) * 2 * h)
            fields[s, :, where] = field
            re, im = field[:rows], field[rows:]
            image[:, where] += weight * (re * re + im * im)

    def forward(i, carry):
        base = i * unroll
        for t in range(unroll + 2):
            if t < unroll:
                mask_band(base + t, t)
            if 0 <= t - 1 < unroll:
                to_rows(t - 1)
            if 0 <= t - 2 < unroll:
                to_field(base + t - 2, t - 2)
        return carry

    lax.fori_loop(0, sources // unroll, forward, 0)

    loads["target"].wait()
    squares = jnp.zeros((rows, LANES), F32)
    image_pair = split(image[...])
    for b in range(blocks):
        where = slice(b * block, (b + 1) * block)
        up = [jnp.concatenate([tab["up"][part, spot, :] for spot in taps(b)], 0) for part in range(2)]
        intensity = product(image_pair, up)
        resist = 1.0 / (1.0 + jnp.exp(-steepness * (intensity - threshold)))
        misfit = resist - target[:, where].astype(F32)
        slope = (2.0 * steepness) * misfit * resist * (1.0 - resist)
        square = misfit * misfit
        squares = squares + square[:, :LANES] + square[:, LANES:]
        keep(slopes, slice(0, rows), where, slope)
    pull[...] = product((slopes[0], slopes[1]), (up_t[0], up_t[1]))
    squares = lane_sum(jnp.sum(squares, 0, keepdims=True))

    loads["half_yt"].wait()
    loads["half_xt"].wait()
    grads[...] = jnp.zeros_like(grads)
    half_xt = tab["half_xt"]

    def weigh(s, slot):
        dest = weighed.at[slot]
        total = jnp.zeros((2 * SUB, coarse), F32)
        for start in range(0, rows, 2 * SUB):
            where = slice(start, start + 2 * SUB)
            other = slice(start + rows, start + rows + 2 * SUB)
            weak, re, im = pull[where, :], fields[s, where, :], fields[s, other, :]
            down_r, down_i = weak * re, weak * im
            total = total + (down_r * re + down_i * im)
            for spot, value in ((where, down_r), (other, down_i)):
                first, second = value[:, : 2 * h], value[:, 2 * h :]
                for side, pair in enumerate((first + second, first - second)):
                    high, low = split(pair)
                    dest[side, spot, : 2 * h] = high
                    dest[side, spot, 2 * h :] = low
        total = total[:SUB] + total[SUB:]
        totals[s] = total[:, :h] + total[:, h : 2 * h] + total[:, 2 * h : 3 * h] + total[:, 3 * h :]

    def from_field(s, slot):
        weight = 2.0 * share_of(s)
        for side in range(2):
            settle = once(weighed[slot, side], tab["half_yt"][side])
            settle = (settle[:, :h] + settle[:, h:]) * weight
            for part in range(2):
                high, low = split(settle[part * rows : (part + 1) * rows])
                settled[slot, :rows, quarter[2 * part + side]] = high
                settled[slot, rows:, quarter[2 * part + side]] = low

    def from_rows(s, slot):
        kept = masks(s)
        full = lax.dot_general(half_xt[:, : 2 * rows], settled[slot], dims, preferred_element_type=F32)
        full = full + lax.dot_general(
            half_xt[:, 2 * rows :], settled[slot, :rows], dims, preferred_element_type=F32
        )
        for where in chunk_rows:
            keeps = kept(where)
            top, low = full[where], full[where.start + h : where.stop + h]
            ee_r, no_i, ee_i, eo_r = (top[:, q] for q in quarter)
            oe_i, oo_r, ne_r, oo_i = (low[:, q] for q in quarter)
            ep, em, op, om = ee_r + eo_r, ee_r - eo_r, oo_r - ne_r, -ne_r - oo_r
            for q, value in enumerate((ep + op, em + om, ep - op, em - om)):
                grads[q, 0, where, :] += jnp.where(keeps[q], value, 0.0)
            ep, em, op, om = ee_i - no_i, ee_i + no_i, oe_i + oo_i, oe_i - oo_i
            for q, value in enumerate((ep + op, em + om, ep - op, em - om)):
                grads[q, 1, where, :] += jnp.where(keeps[q], value, 0.0)

    def backward(i, carry):
        base = i * unroll
        for t in range(unroll + 2):
            if t < unroll:
                weigh(base + t, t)
            if 0 <= t - 1 < unroll:
                from_field(base + t - 1, t - 1)
            if 0 <= t - 2 < unroll:
                from_rows(base + t - 2, t - 2)
        return carry

    lax.fori_loop(0, sources // unroll, backward, 0)
    each = lane_sum(jnp.sum(totals[...], 1))
    own = lax.broadcasted_iota(jnp.int32, (sources, LANES), 0) == lane
    sums = jnp.sum(jnp.where(own, each, 0.0), 0, keepdims=True)
    sums = jnp.where(lane == sources, squares, sums)

    def unturn(slot, sign):
        s = turn_s if sign > 0 else -turn_s
        re, im = grads[slot, 0], grads[slot, 1]
        return re * turn_c + im * s, im * turn_c - re * s

    pp, pm, mp, mm = unturn(0, 1), unturn(1, 1), unturn(2, -1), unturn(3, -1)
    pieces = ((pp[0], mm[0]), (pm[0], mp[0]), (-pp[1], mm[1]), (-pm[1], mp[1]))
    last_row = jnp.zeros((1, LANES), F32)
    for i, (first, second) in enumerate(pieces):
        ext[...] = jnp.zeros_like(ext)
        if i in (0, 2):
            ext[1 : h + 1, :h] = second
            moved = pltpu.roll(ext[...], 1, 1)
            ext[...] = moved
            ext[:h, :h] += first
        else:
            ext[:h, :h] = first
            moved = pltpu.roll(ext[...], 1, 1)
            ext[...] = moved
            ext[1 : h + 1, :h] += second
        grad_t[i] = ext[:h, :h].T.reshape(chips, 2, SUB, h)
        copy_to(8, partner, grad_t.at[i, :, 1 - core], pair_in.at[i]).start()
        edge_back[i] = ext[h : h + 1, :h]
        edge_back[4 + i] = ext[:h, h:].T[0:1, :]
        last_row = jnp.where(lane == i, ext[h : h + 1, h : h + 1], last_row)
    edge_back[8] = last_row
    edge_back[9] = sums
    for i in range(10, devices):
        edge_back[i] = jnp.zeros((1, LANES), F32)

    send_all(5, lambda p: edge_back.at[p], edge_back_in.at[me])
    edge_back_in[me] = edge_back[me]
    wait_all(8, pair_in)
    for i in range(4):
        pair_sum[:, i] = grad_t[i, :, core] + pair_in[i]

    each_chip(lambda peer: copy_to(4, peer, pair_sum.at[peer // 2], grad_in.at[chip]).start())
    grad_in[chip] = pair_sum[chip]
    wait_all(5, edge_back_in.at[most])
    edge_back_all[me] = jnp.sum(edge_back_in[...], 0)
    send_all(7, lambda p: edge_back_all.at[me], edge_back_all.at[me])
    wait_all(4, grad_in.at[pl.ds(0, chips - 1)])

    def unmix(u, v, wp, wm):
        return u + v, wp - wm, wp + wm, v - u

    mine = jnp.sum(grad_in[...], 0)
    cc, cs, sc, ss = unmix(mine[0], mine[1], mine[2], mine[3])
    sum_c = jnp.concatenate([cc, cs], 0)[None]
    sum_s = jnp.concatenate([sc, ss], 0)[None]
    back_c = far_c * sum_c + far_s * sum_s
    back_s = far_c * sum_s - far_s * sum_c
    turned = jnp.concatenate([back_c, back_s], 2).reshape(devices * 2 * SUB, 2 * h)
    gathered = product(split(turned), both("wave_x"), flip=True)
    back_rows[...] = gathered.reshape(devices, 2, SUB, rows)
    send_all(6, lambda p: back_rows.at[p], back_in.at[:, pl.ds(me * SUB, SUB), :])
    back_in[:, pl.ds(me * SUB, SUB), :] = back_rows[me]
    wait_all(7, edge_back_all.at[most])

    sums = edge_back_all[9]
    small_at = slice(2 * h + LANES, 2 * h + 2 * LANES)
    result[0:1, small_at] = sums * norming
    sums = jnp.where(lane < sources, sums, 0.0)
    result[1:2, small_at] = share_row * (sums - lane_sum(share_row * sums)) * norming
    result[2:3, small_at] = group_row.astype(F32)

    side_x = unmix(*(edge_back_all[i] for i in range(4)))
    side_y = unmix(*(edge_back_all[4 + i] for i in range(4)))
    corner = unmix(*(lane_sum(jnp.where(lane == i, edge_back_all[8], 0.0)) for i in range(4)))
    far_c, far_s = tab["far"][0, me], tab["far"][1, me]
    near = []
    for c, s in ((side_y[0], side_y[2]), (side_y[1], side_y[3])):
        near.append(jnp.concatenate([far_c * c + far_s * s, far_c * s - far_s * c], 1))
    near = jnp.concatenate(near + [jnp.zeros((SUB - 2, 2 * h), F32)], 0)
    last = product(split(near), both("wave_x"), flip=True)
    edge_c, edge_s = edge_rows[0:1], edge_rows[1:2]
    last_c = last[0:1] + corner[0] * edge_c + corner[2] * edge_s
    last_s = last[1:2] + corner[1] * edge_c + corner[3] * edge_s
    result[:, 2 * h : 2 * h + LANES] = column(last_c) * edge_c + column(last_s) * edge_s
    col_c, col_s = column(edge_c), column(edge_s)

    wait_all(6, back_in.at[:, pl.ds(0, h - SUB), :])
    part_c = back_in[0].T + col_c * side_x[0] + col_s * side_x[2]
    part_s = back_in[1].T + col_c * side_x[1] + col_s * side_x[3]
    result[:, :h] = part_c
    result[:, h : 2 * h] = part_s
    drain(0, rows_in.at[most])
    drain(1, edge_in.at[most])
    drain(2, chunk.at[most])
    drain(3, edge_all.at[most])
    drain(4, grad_in.at[pl.ds(0, chips - 1)])
    drain(5, edge_back_in.at[most])
    drain(6, back_in.at[:, pl.ds(0, h - SUB), :])
    drain(7, edge_back_all.at[most])
    drain(8, pair_in)


def closing(n, sources, result, wave, loss_hbm, grad_hbm, group_hbm, loss, group, out, out_sem):
    block = 2 * LANES
    blocks = n // block
    lane = lax.broadcasted_iota(jnp.int32, (1, LANES), 1)
    h = K // 2
    small = result.at[:, 2 * h + LANES :]
    loss[0] = jnp.sum(jnp.where(lane == sources, small[0:1, :], 0.0))
    for g in range(NG):
        group[g] = jnp.sum(jnp.where(small[2:3, :] == g, small[1:2, :], 0.0))
    stores = [
        pltpu.make_async_copy(loss, loss_hbm, out_sem.at[blocks]),
        pltpu.make_async_copy(group, group_hbm, out_sem.at[blocks + 1]),
    ]
    for store in stores:
        store.start()
    pair = split(result[:, : 2 * h])
    spread = result[:, 2 * h : 2 * h + LANES]
    adds = jnp.concatenate([spread, spread], 1)
    for b in range(blocks):
        where = slice(b * block, (b + 1) * block)
        out[:, where] = product(pair, (wave[0, :, where], wave[1, :, where])) + adds
        stores.append(pltpu.make_async_copy(out.at[:, where], grad_hbm.at[:, where], out_sem.at[b]))
        stores[-1].start()
    for store in stores:
        store.wait()


def fused(devices, mask_field, target_print, source_points, source_groups, group_logits, pupil_radius):
    rows, n = mask_field.shape
    h = K // 2
    coarse = 2 * K
    sources = source_points.shape[0]
    consts = tables(n, rows, devices)
    anywhere = pl.BlockSpec(memory_space=pltpu.HBM)
    vmem = lambda *shape: pltpu.VMEM(shape, F32)
    scratch = [pltpu.VMEM(consts[k].shape, consts[k].dtype) for k in NAMES] + [
        vmem(rows, n), pltpu.VMEM((rows, n), jnp.int32),
        vmem(2, h, rows), vmem(devices, 1, LANES), vmem(devices, 2, SUB, rows), vmem(devices, 1, LANES),
        vmem(devices, 4, SUB, h), vmem(devices, 1, LANES), vmem(h + SUB, 2 * h), vmem(4, 2, h, h),
        vmem(4, 2, h, h), vmem(sources, 2 * rows, coarse), vmem(rows, coarse), vmem(rows, coarse),
        vmem(4, 2, h, h), vmem(4, devices // 2, 2, SUB, h), vmem(devices, 1, LANES), vmem(devices // 2, 4, SUB, h),
        vmem(devices, 1, LANES), vmem(devices, 1, LANES), vmem(devices, 2, SUB, rows), vmem(2, h, rows),
        pltpu.VMEM((8, 2, 2 * h, coarse), BF16), pltpu.VMEM((8, 2, 2 * rows, 2 * h), BF16),
        pltpu.VMEM((8, 2, 2 * rows, coarse), BF16), pltpu.VMEM((8, 2 * rows, coarse), BF16),
        vmem(sources, SUB, LANES),
        pltpu.SMEM((2, sources), jnp.int32), pltpu.SMEM((sources,), jnp.int32), pltpu.SMEM((NG,), F32),
        pltpu.SMEM((1,), jnp.int32),
        vmem(4, devices // 2, SUB, h), vmem(devices // 2, 4, SUB, h),
        pltpu.VMEM((2, n, coarse), BF16), pltpu.VMEM((2, rows, n), BF16),
        pltpu.SemaphoreType.DMA((24,)),
        pltpu.SemaphoreType.DMA((9,)), pltpu.SemaphoreType.DMA((9,)), pltpu.SemaphoreType.DMA((devices // 2,)),
    ]
    arrays = [jnp.asarray(consts[k]) for k in NAMES]
    hold = lambda value: pltpu.with_memory_space_constraint(value, pltpu.HBM)
    inside = pl.BlockSpec(memory_space=pltpu.VMEM)
    (result,) = pl.pallas_call(
        functools.partial(kernel, devices, n),
        out_shape=(
            jax.ShapeDtypeStruct((rows, 2 * h + 2 * LANES), F32),
        ),
        in_specs=[anywhere] * (6 + len(NAMES)),
        out_specs=(inside,),
        scratch_shapes=scratch,
        compiler_params=pltpu.CompilerParams(
            collective_id=0, has_side_effects=True, vmem_limit_bytes=53 * 1024 * 1024
        ),
    )(*map(hold, (source_points.T, source_groups, group_logits)), pupil_radius,
      *map(hold, (mask_field, target_print, *arrays)))
    return pl.pallas_call(
        functools.partial(closing, n, sources),
        out_shape=(
            jax.ShapeDtypeStruct((1,), F32),
            jax.ShapeDtypeStruct((rows, n), F32),
            jax.ShapeDtypeStruct((NG,), F32),
        ),
        in_specs=[inside] * 2,
        out_specs=(anywhere, anywhere, anywhere),
        scratch_shapes=[
            pltpu.SMEM((1,), F32), pltpu.SMEM((NG,), F32), vmem(rows, n),
            pltpu.SemaphoreType.DMA((n // (2 * LANES) + 2,)),
        ],
        compiler_params=pltpu.CompilerParams(vmem_limit_bytes=8 * 1024 * 1024),
    )(result, arrays[0])


HIGH = lax.Precision.HIGH


def dot(form, left, right):
    return jnp.einsum(form, left, right, precision=HIGH, preferred_element_type=F32)


def waves(left, right, length):
    turns = angles(left, right, length)
    return np.cos(turns), np.sin(turns)


def shifted_waves(count, freq, length, device, devices):
    near = np.stack(waves(np.arange(count), freq, length)).astype(np.float32)
    far = np.stack(waves(np.arange(devices) * count, freq, length)).astype(np.float32)
    far = lax.dynamic_slice_in_dim(jnp.asarray(far), device, 1, axis=1)
    return far[0] * near[0] - far[1] * near[1], far[1] * near[0] + far[0] * near[1]


def exchange(blocks):
    return lax.all_to_all(blocks, "slab", 0, 0)


def plain(devices, mask_field, target_print, source_points, source_groups, group_logits, pupil_radius):
    rows, n = mask_field.shape
    sources = source_points.shape[0]
    coarse = 2 * K
    step = n // coarse
    cols = coarse // devices
    half = n // 2
    device = lax.axis_index("slab")
    freq = np.arange(K, dtype=np.int64) - K // 2
    order = np.concatenate([freq[freq % 2 == 0], freq[freq % 2 == 1]])
    kh = K // 2
    norming = 1.0 / (n * n)

    cos_y, sin_y = waves(np.arange(half), order, n)
    fold = [
        jnp.asarray(np.concatenate([t[:, p * kh : (p + 1) * kh] for t in (cos_y, sin_y)], 1), F32)
        for p in (0, 1)
    ]
    lag = np.mod(np.arange(n)[None, :] - step * np.arange(coarse)[:, None], n)
    response = np.zeros(n)
    for f in range(1, K):
        response += 2.0 * np.cos(2.0 * math.pi * np.mod(f * np.arange(n), n) / n)
    response = (response + 1.0) / coarse
    up = jnp.asarray(response[lag], F32)
    cos_c, sin_c = waves(freq, np.arange(coarse), coarse)
    wave_x = jnp.asarray(np.concatenate([cos_c, sin_c], 1), F32)
    loc_c, loc_s = shifted_waves(rows, freq, n, device, devices)
    loc = jnp.concatenate([loc_c, loc_s], 1)
    a, b = shifted_waves(cols, order, coarse, device, devices)
    lift = jnp.concatenate([jnp.concatenate([a, -b], 1), jnp.concatenate([b, a], 1)], 0)

    cutoff = pupil_radius[0]
    shifted = (source_points - GRID // 2) * cutoff // shift_scale
    first = jnp.asarray(freq, jnp.int32)[None, None, :] + shifted[:, 0, None, None]
    second = jnp.asarray(np.tile(order, 2), jnp.int32)[None, :, None] + shifted[:, 1, None, None]
    passed = first * first + second * second <= cutoff * cutoff

    near, away = mask_field[:, :half], mask_field[:, half:]
    even = dot("xy,yq->xq", near + away, fold[0])
    odd = dot("xy,yq->xq", near - away, fold[1])
    part_c = jnp.concatenate([even[:, :kh], odd[:, :kh]], 1)
    part_s = jnp.concatenate([even[:, kh:], odd[:, kh:]], 1)
    spec = dot("xq,xk->qk", jnp.concatenate([part_c, part_s], 1), loc)
    band = jnp.concatenate([spec[:K, :K] - spec[K:, K:], -(spec[:K, K:] + spec[K:, :K])], 0)
    band = jnp.sum(exchange(band.reshape(devices, 2 * K // devices, K)), 0)
    band = lax.all_gather(band, "slab", tiled=True)

    kept = jnp.where(passed, band[None], 0.0)
    wide = dot("aq,sqk->sak", lift, kept)
    both = dot("ak,kx->ax", wide.reshape(sources * 2 * cols, K), wave_x)
    both = both.reshape(sources, 2, cols, 2 * coarse)
    field_re = (both[:, 0, :, :coarse] - both[:, 1, :, coarse:]) * norming
    field_im = (both[:, 0, :, coarse:] + both[:, 1, :, :coarse]) * norming
    bright = field_re * field_re + field_im * field_im
    onehot = (source_groups[:, None] == jnp.arange(NG, dtype=jnp.int32)[None, :]).astype(F32)
    weights = jnp.exp(jnp.sum(onehot * group_logits[None, :], 1))
    share = weights / jnp.sum(weights)
    image = jnp.sum(share[:, None, None] * bright, 0)

    tall = dot("cm,mx->cx", image, up)
    tall = lax.all_to_all(tall, "slab", 1, 0, tiled=True)
    intensity = dot("cx,cy->xy", tall, up)
    resist = jax.nn.sigmoid(steepness * (intensity - threshold))
    misfit = resist - target_print.astype(F32)
    slope = (2.0 * steepness) * misfit * resist * (1.0 - resist)
    squares = jnp.sum(misfit * misfit)
    down = dot("xy,cy->cx", slope, up)
    down = lax.all_to_all(down, "slab", 0, 1, tiled=True)
    pull = dot("cx,mx->cm", down, up)

    per_source = jnp.sum(bright * pull[None], (1, 2))
    sums = jnp.concatenate([per_source, squares[None]])
    factor = (2.0 * norming) * share[:, None, None] * pull[None]
    back = jnp.stack([factor * field_re, factor * field_im], 1)
    low = dot("ax,kx->ak", back.reshape(sources * 2 * cols, coarse), wave_x[:, :coarse])
    lows = dot("ax,kx->ak", back.reshape(sources * 2 * cols, coarse), wave_x[:, coarse:])
    low = low.reshape(sources, 2, cols, K)
    lows = lows.reshape(sources, 2, cols, K)
    settle = jnp.concatenate([low[:, 0] + lows[:, 1], low[:, 1] - lows[:, 0]], 1)
    settle = dot("aq,sak->sqk", lift, settle)
    grad_band = jnp.sum(jnp.where(passed, settle, 0.0), 0).reshape(devices, 2 * K // devices, K)
    extra = jnp.pad(sums[None, :], ((0, 7), (0, K - sources - 1)))
    extra = jnp.broadcast_to(extra[None], (devices, 8, K))
    grad_band = jnp.sum(exchange(jnp.concatenate([grad_band, extra], 1)), 0)
    sums = grad_band[-8, : sources + 1]
    grad_band = lax.all_gather(grad_band[:-8], "slab", tiled=True)
    per_source, squares = sums[:-1], sums[-1]
    loss_value = (squares * norming).reshape(1)
    against = jnp.sum(share * per_source)
    source_pull = share * (per_source - against)
    group_grad = jnp.sum(onehot * source_pull[:, None], 0) * norming

    spread = dot("tk,qk->tq", jnp.concatenate([loc_c, loc_s], 0), grad_band)
    spread_re = spread[:rows, :K] - spread[rows:, K:]
    spread_im = spread[:rows, K:] + spread[rows:, :K]
    even = dot("xq,yq->xy", jnp.concatenate([spread_re[:, :kh], -spread_im[:, :kh]], 1), fold[0])
    odd = dot("xq,yq->xy", jnp.concatenate([spread_re[:, kh:], -spread_im[:, kh:]], 1), fold[1])
    mask_grad = jnp.concatenate([even + odd, even - odd], 1)
    return loss_value, mask_grad, group_grad


def on_device(devices, mask_field, *others):
    tiles = mask_field.shape[0] == LANES and K // 2 == LANES == SUB * devices and devices % 8 == 0 and devices >= 10
    return (fused if tiles else plain)(devices, mask_field, *others)


def solution(mesh):
    in_specs = (
        P(("clip", "slab"), None),
        P(("clip", "slab"), None),
        P("clip", None),
        P("clip"),
        P("clip"),
        P("clip"),
    )
    out_specs = (P("clip"), P(("clip", "slab"), None), P("clip"))
    return jax.shard_map(
        functools.partial(on_device, mesh.shape["slab"]),
        mesh=mesh, in_specs=in_specs, out_specs=out_specs, check_vma=False,
    )
```

```python
import functools
import math

import jax
import jax.numpy as jnp
import numpy as np
from jax import lax
from jax.experimental import pallas as pl
from jax.experimental.pallas import tpu as pltpu
from jax.sharding import PartitionSpec as P

K = 256
GRID = 61
NG = 8

steepness = 8.0
threshold = 0.3
shift_scale = 45
F32 = jnp.float32
BF16 = jnp.bfloat16
LANES = 128
SUB = 8


def angles(left, right, length):
    turns = np.mod(np.asarray(left)[:, None] * np.asarray(right)[None, :], length)
    return 2.0 * math.pi * turns.astype(np.float64) / length


def halves(table):
    table = np.asarray(table, np.float32)
    high = table.astype(BF16)
    low = (table - high.astype(np.float32)).astype(BF16)
    return np.stack([high, low])


def split(value):
    high = value.astype(BF16)
    return high, (value - high.astype(F32)).astype(BF16)


def product(left, right, flip=False):
    dims = (((1,), (1 if flip else 0,)), ((), ()))
    one = lambda a, b: lax.dot_general(a, b, dims, preferred_element_type=F32)
    return one(left[0], right[0]) + one(left[1], right[0]) + one(left[0], right[1])


def tables(n, rows, devices):
    h = K // 2
    coarse = 2 * K
    step = n // coarse
    freq = np.arange(h)
    near = np.arange(rows)
    wave_y = angles(freq, np.arange(n // 2), n)
    wave_y = np.concatenate([np.cos(wave_y), np.sin(wave_y)], 0)
    wave_x = angles(near, freq, n)
    wave_x = np.concatenate([np.cos(wave_x), np.sin(wave_x)], 1)
    half_x = angles(near, 2 * freq + 1, 2 * n)
    half_x = np.concatenate([np.cos(half_x), -np.sin(half_x)], 1)
    spots = step * np.arange(coarse // 2) + step // 2
    half_y = angles(2 * freq + 1, spots, 2 * n)
    half_y = [halves(np.cos(half_y)), halves(np.sin(half_y))]
    ahead = np.stack([np.concatenate([t[0], t[0], t[1]], 0) for t in half_y])
    behind = np.stack([
        np.block([[t[0].T, t[1].T], [t[0].T, np.zeros_like(t[0].T)]]) for t in half_y
    ])
    far = angles(rows * np.arange(devices), freq, n)
    far = np.stack([np.cos(far), np.sin(far)])[:, :, None, :].astype(np.float32)
    half_far = angles(rows * np.arange(devices), 2 * freq + 1, 2 * n)
    half_far = np.stack([np.cos(half_far), np.sin(half_far)]) / (n * n)
    half_far = half_far[:, :, None, :].astype(np.float32)
    block = 2 * LANES
    extra = n // step - block // step
    index = np.arange(coarse // 2 + extra)[:, None]
    spot = np.concatenate([step * (index - extra) + step // 2, -step * index - step // 2], 0)
    lag = np.mod(np.arange(block)[None, :] - spot, n)
    kernel = np.ones(n)
    for f in range(1, K):
        kernel += 2.0 * np.cos(2.0 * math.pi * np.mod(f * np.arange(n), n) / n)
    up = (kernel / coarse)[lag]
    edge = angles([h], np.arange(LANES), n)
    edge = np.concatenate([np.cos(edge), np.sin(edge)], 0)
    edge = np.concatenate([edge, np.zeros((SUB - 2, LANES))], 0)
    return {
        "wave_y": halves(wave_y),
        "wave_x": halves(wave_x),
        "half_x": halves(half_x),
        "half_xt": np.concatenate(list(halves(half_x.T)[[0, 0, 1]]), 1),
        "half_y": ahead,
        "half_yt": behind,
        "up": halves(up),
        "far": far,
        "half_far": half_far,
        "edge": edge.astype(np.float32),
    }


NAMES = ("wave_y", "wave_x", "half_x", "half_xt", "half_y", "half_yt", "up", "far", "half_far", "edge")


def kernel(devices, n, *refs):
    small_hbm, mask_hbm, target_hbm = refs[:4], refs[4], refs[5]
    sources_in = dict(zip(NAMES, refs[6 : 6 + len(NAMES)]))
    refs = refs[6 + len(NAMES) :]
    result = refs[0]
    refs = refs[1:]
    tab = dict(zip(NAMES, refs[: len(NAMES)]))
    refs = refs[len(NAMES) :]
    (mask, target, rows_t, edge_out, rows_in, edge_in, chunk, edge_all, exts, band, data, fields, image, pull,
     grads, grad_t, edge_back, grad_in, edge_back_in, edge_back_all, back_rows, back_in,
     folded, wides, weighed, settled, totals, keeps, points, groups, logits, radius,
     pair_in, pair_sum, up_t, slopes, local_sem, send_sem, recv_sem, near_sem) = refs
    h = K // 2
    coarse = 2 * K
    sources = points.shape[1]
    rows = mask.shape[0]
    block = 2 * LANES
    blocks = n // block
    step = n // coarse
    me = lax.axis_index("slab")
    norming = 1.0 / (n * n)
    chips = devices // 2
    core, chip = lax.rem(me, 2), me // 2
    partner = me + 1 - 2 * core
    most = pl.ds(0, devices - 1)

    loads = {}
    small = (points, groups, logits, radius)
    part = n // 8
    pieces = [(slice(c, c + part), slice(c + n // 2, c + n // 2 + part)) for c in range(0, n // 2, part)]
    for i, (name, src, dst) in enumerate(
        [
            piece
            for k, (where, away) in enumerate(pieces)
            for piece in (
                (f"near{k}", mask_hbm.at[:, where], mask.at[:, where]),
                (f"away{k}", mask_hbm.at[:, away], mask.at[:, away]),
                (f"wave_y{k}", sources_in["wave_y"].at[:, :, where], tab["wave_y"].at[:, :, where]),
            )
        ]
        + [(f"small{k}", small_hbm[k], small[k]) for k in range(4)]
        + [(k, sources_in[k], tab[k]) for k in ("edge", "wave_x", "far", "half_far", "half_x", "half_y")]
        + [("up", sources_in["up"], tab["up"]), ("target", target_hbm, target)]
        + [(k, sources_in[k], tab[k]) for k in ("half_yt", "half_xt")]
    ):
        loads[name] = pltpu.make_async_copy(src, dst, local_sem.at[i])
        loads[name].start()

    barrier = pltpu.get_barrier_semaphore()

    def greet(i, carry):
        pl.semaphore_signal(barrier, inc=1, device_id={"slab": lax.rem(me + i, devices)})
        return carry

    lax.fori_loop(1, devices, greet, 0)

    def both(name):
        return tab[name][0], tab[name][1]

    def copy_to(phase, peer, src, dst, sem=None):
        return pltpu.make_async_remote_copy(
            src_ref=src, dst_ref=dst, send_sem=send_sem.at[phase],
            recv_sem=recv_sem.at[phase] if sem is None else sem, device_id={"slab": peer},
        )

    group = 4
    planes = devices // group
    lower = 1 - me // (group * (planes // 2))

    def plane_of(i):
        return lower * (planes - 1 - 2 * i) + i

    def send_all(phase, src_of, dst):
        for i in range(devices):
            peer = plane_of(i // group) * group + lax.rem(me + i % group, group)

            @pl.when(peer != me)
            def _():
                copy_to(phase, peer, src_of(peer), dst).start()

    def each_chip(act, reverse=False):
        for i in range(chips)[:: -1 if reverse else 1]:
            other = plane_of(i // 2) * 2 + lax.rem(chip + i % 2, 2)

            @pl.when(other != chip)
            def _():
                act(other * 2 + core)

    def wait_all(phase, ref, sem=None):
        copy_to(phase, partner, ref, ref, sem).wait_recv()

    def drain(phase, ref):
        copy_to(phase, partner, ref, ref).wait_send()

    lane = lax.broadcasted_iota(jnp.int32, (1, LANES), 1)

    def column(row):
        return jnp.broadcast_to(row, (LANES, LANES)).T

    even = odd = 0.0
    for k, (where, away) in enumerate(pieces):
        for name in ("near", "away", "wave_y"):
            loads[f"{name}{k}"].wait()
        wave = (tab["wave_y"][0, :, where], tab["wave_y"][1, :, where])
        first, second = mask[:, where], mask[:, away]
        even = even + product(split(first + second), wave, flip=True)
        odd = odd + product(split(first - second), wave, flip=True)
    wide_lane = lax.broadcasted_iota(jnp.int32, (rows, 2 * h), 1)
    transformed = jnp.where(lax.rem(wide_lane, 2) == 0, even, odd)
    rows_t[0] = transformed[:, :h].T
    rows_t[1] = transformed[:, h:].T
    loads["edge"].wait()
    loads["wave_x"].wait()
    loads["far"].wait()
    edge_rows = tab["edge"][...]
    edge_pair = split(edge_rows)
    summed = mask[:, :LANES]
    for b in range(1, n // LANES):
        summed = summed + mask[:, b * LANES : (b + 1) * LANES]
    side_x = product(edge_pair, split(transformed))
    last = product(edge_pair, split(summed), flip=True)
    side_y = product(split(last), both("wave_x"))
    far_c, far_s = tab["far"][0, me], tab["far"][1, me]
    side_c = far_c * side_y[:2, :h] - far_s * side_y[:2, h:]
    side_s = far_s * side_y[:2, :h] + far_c * side_y[:2, h:]

    def mixes(cc, cs, sc, ss):
        return cc - ss, cc + ss, sc + cs, sc - cs

    edges = mixes(side_x[0:1, :h], side_x[0:1, h:], side_x[1:2, :h], side_x[1:2, h:])
    edges = edges + mixes(side_c[0:1], side_c[1:2], side_s[0:1], side_s[1:2])

    def lane_sum(value):
        return jnp.sum(value, axis=1, keepdims=True)

    corner = mixes(
        lane_sum(last[0:1] * edge_rows[0:1]), lane_sum(last[1:2] * edge_rows[0:1]),
        lane_sum(last[0:1] * edge_rows[1:2]), lane_sum(last[1:2] * edge_rows[1:2]),
    )
    corner_row = jnp.zeros((1, LANES), F32)
    for i in range(4):
        corner_row = jnp.where(lane == i, corner[i], corner_row)
    for i in range(8):
        edge_out[i] = edges[i]
    edge_out[8] = corner_row
    for i in range(9, devices):
        edge_out[i] = jnp.zeros((1, LANES), F32)

    pl.semaphore_wait(barrier, devices - 1)
    send_all(1, lambda p: edge_out.at[p], edge_in.at[me])
    send_all(0, lambda p: rows_t.at[:, pl.ds(p * SUB, SUB), :], rows_in.at[me])
    rows_in[me] = rows_t[:, pl.ds(me * SUB, SUB), :]
    edge_in[me] = edge_out[me]

    for k in range(4):
        loads[f"small{k}"].wait()
    logit_row = jnp.full((1, LANES), 0.0, F32)
    group_row = jnp.full((1, LANES), -1, jnp.int32)
    for s in range(sources):
        g = groups[s]
        logit_row = jnp.where(lane == s, logits[g], logit_row)
        group_row = jnp.where(lane == s, g, group_row)
    weight_row = jnp.where(lane < sources, jnp.exp(logit_row), 0.0)
    share_row = weight_row / jnp.sum(weight_row, axis=1, keepdims=True)

    loads["up"].wait()
    extra = (n - block) // step

    def taps(b):
        first, second = extra - b * (block // step), extra + 2 * h + b * (block // step)
        return slice(first, first + 2 * h), slice(second, second + 2 * h)

    for b in range(blocks):
        for part in range(2):
            for side, spot in enumerate(taps(b)):
                up_t[part, b * block : (b + 1) * block, side * 2 * h : (side + 1) * 2 * h] = tab["up"][part, spot, :].T
    cutoff = radius[0]
    limit = (cutoff * cutoff).astype(F32)
    lane_index = lane.astype(F32)
    chunk_rows = [slice(c, c + 2 * SUB) for c in range(0, h, 2 * SUB)]
    row_index = lax.broadcasted_iota(jnp.int32, (2 * SUB, LANES), 0).astype(F32)

    def masks(s):
        first = ((points[0, s] - GRID // 2) * cutoff // shift_scale).astype(F32)
        second = ((points[1, s] - GRID // 2) * cutoff // shift_scale).astype(F32)
        col_p, col_m = lane_index + second, second - 1.0 - lane_index
        col_p, col_m = col_p * col_p, col_m * col_m

        def of(where):
            row_p = row_index + (first + where.start)
            row_m = (first - 1.0 - where.start) - row_index
            room_p, room_m = limit - row_p * row_p, limit - row_m * row_m
            return col_p <= room_p, col_m <= room_p, col_p <= room_m, col_m <= room_m

        return of

    def fill(s, carry):
        kept = masks(s)
        for where in chunk_rows:
            for q, flag in enumerate(kept(where)):
                keeps[s, q, where, :] = jnp.where(flag, 1.0, 0.0)
        return carry

    lax.fori_loop(0, sources, fill, 0)

    wait_all(1, edge_in.at[most])
    edge_all[me] = jnp.sum(edge_in[...], 0)
    send_all(3, lambda p: edge_all.at[me], edge_all.at[me])
    wait_all(0, rows_in.at[most])
    gathered = rows_in[...].reshape(devices * 2 * SUB, rows)
    turned = product(split(gathered), both("wave_x")).reshape(devices, 2 * SUB, 2 * h)
    far_c, far_s = tab["far"][0], tab["far"][1]
    turned_c, turned_s = turned[:, :, :h], turned[:, :, h:]
    sum_c = jnp.sum(far_c * turned_c - far_s * turned_s, 0)
    sum_s = jnp.sum(far_s * turned_c + far_c * turned_s, 0)
    for i, value in enumerate(mixes(sum_c[:SUB], sum_c[SUB:], sum_s[:SUB], sum_s[SUB:])):
        chunk[me, i] = value

    each_chip(lambda peer: copy_to(2, peer, chunk.at[me], chunk.at[me], near_sem.at[chip]).start())
    copy_to(2, partner, chunk.at[me], chunk.at[me]).start()

    loads["half_far"].wait()
    loads["half_x"].wait()
    loads["half_y"].wait()
    turn_c = column(tab["half_far"][0, me])
    turn_s = column(tab["half_far"][1, me])


    def relay(peer):
        wait_all(2, chunk.at[peer], near_sem.at[peer // 2])
        copy_to(2, partner, chunk.at[peer], chunk.at[peer]).start()

    each_chip(relay, reverse=True)
    wait_all(2, chunk.at[pl.ds(0, chips)])
    wait_all(3, edge_all.at[most])
    shifted = []
    plain = []
    for i in range(4):
        ext = exts.at[i]
        ext[:h, :h] = chunk[:, i].reshape(h, h).T
        ext[h : h + 1, :h] = edge_all[i]
        ext[:h, h:] = column(edge_all[4 + i])
        ext[h : h + 1, h:] = jnp.broadcast_to(lane_sum(jnp.where(lane == i, edge_all[8], 0.0)), (1, LANES))
        plain = ext[...]
        moved = pltpu.roll(plain, 2 * h - 1, 1)
        if i in (0, 2):
            first, second = ext[:h, :h], None
            ext[...] = moved
            second = ext[1 : h + 1, :h]
        else:
            second = ext[1 : h + 1, :h]
            ext[...] = moved
            first = ext[:h, :h]
        data[i, 0] = first
        data[i, 1] = second

    def turn(slot, re, im, sign):
        s = turn_s if sign > 0 else -turn_s
        band[slot, 0] = re * turn_c - im * s
        band[slot, 1] = re * s + im * turn_c

    turn(0, data[0, 0], -data[2, 0], 1)
    turn(1, data[1, 0], -data[3, 0], 1)
    turn(2, data[1, 1], data[3, 1], -1)
    turn(3, data[0, 1], data[2, 1], -1)

    def share_of(s):
        return lane_sum(jnp.where(lane == s, share_row, 0.0))

    def keep(ref, where, lanes, value):
        high, low = split(value)
        ref[0, where, lanes] = high
        ref[1, where, lanes] = low

    unroll = 8
    quarter = [slice(i * h, (i + 1) * h) for i in range(4)]
    image[...] = jnp.zeros_like(image)

    def mask_band(s, slot):
        dest = folded.at[slot]
        for where in chunk_rows:
            kept = [keeps[s, q, where, :] for q in range(4)]
            low_where = slice(where.start + h, where.stop + h)
            pp, pm, mp, mm = (kept[q] * band[q, 0, where, :] for q in range(4))
            keep(dest, where, quarter[0], pp + mp)
            keep(dest, where, quarter[1], pm + mm)
            keep(dest, low_where, quarter[2], mp - pp)
            keep(dest, low_where, quarter[3], mm - pm)
            pp, pm, mp, mm = (kept[q] * band[q, 1, where, :] for q in range(4))
            keep(dest, where, quarter[2], pp + mp)
            keep(dest, where, quarter[3], pm + mm)
            keep(dest, low_where, quarter[0], pp - mp)
            keep(dest, low_where, quarter[1], pm - mm)

    dims = (((1,), (0,)), ((), ()))

    def once(left, right):
        return lax.dot_general(left, right, dims, preferred_element_type=F32)

    def to_rows(slot):
        wide = product(both("half_x"), (folded[slot, 0], folded[slot, 1]))
        p_r, m_r, p_i, m_i = (wide[:, q] for q in quarter)
        for part, sides in enumerate(((p_r + m_r, m_i - p_i), (p_i + m_i, p_r - m_r))):
            for side, value in enumerate(sides):
                high, low = split(value)
                wides[slot, side, part * rows : (part + 1) * rows, :h] = high
                wides[slot, side, part * rows : (part + 1) * rows, h:] = low

    def to_field(s, slot):
        even, odd = (
            once(wides[slot, side], tab["half_y"][side, : 2 * h])
            + once(wides[slot, side, :, :h], tab["half_y"][side, 2 * h :])
            for side in range(2)
        )
        weight = share_of(s)
        for side, field in enumerate((even + odd, even - odd)):
            where = slice(side * 2 * h, (side + 1) * 2 * h)
            fields[s, :, where] = field
            re, im = field[:rows], field[rows:]
            image[:, where] += weight * (re * re + im * im)

    def forward(i, carry):
        base = i * unroll
        for t in range(unroll + 2):
            if t < unroll:
                mask_band(base + t, t)
            if 0 <= t - 1 < unroll:
                to_rows(t - 1)
            if 0 <= t - 2 < unroll:
                to_field(base + t - 2, t - 2)
        return carry

    lax.fori_loop(0, sources // unroll, forward, 0)

    loads["target"].wait()
    squares = jnp.zeros((rows, LANES), F32)
    image_pair = split(image[...])
    for b in range(blocks):
        where = slice(b * block, (b + 1) * block)
        up = [jnp.concatenate([tab["up"][part, spot, :] for spot in taps(b)], 0) for part in range(2)]
        intensity = product(image_pair, up)
        resist = 1.0 / (1.0 + jnp.exp(-steepness * (intensity - threshold)))
        misfit = resist - target[:, where].astype(F32)
        slope = (2.0 * steepness) * misfit * resist * (1.0 - resist)
        square = misfit * misfit
        squares = squares + square[:, :LANES] + square[:, LANES:]
        keep(slopes, slice(0, rows), where, slope)
    pull[...] = product((slopes[0], slopes[1]), (up_t[0], up_t[1]))
    squares = lane_sum(jnp.sum(squares, 0, keepdims=True))

    loads["half_yt"].wait()
    loads["half_xt"].wait()
    grads[...] = jnp.zeros_like(grads)
    half_xt = tab["half_xt"]

    def weigh(s, slot):
        dest = weighed.at[slot]
        total = jnp.zeros((2 * SUB, coarse), F32)
        for start in range(0, rows, 2 * SUB):
            where = slice(start, start + 2 * SUB)
            other = slice(start + rows, start + rows + 2 * SUB)
            weak, re, im = pull[where, :], fields[s, where, :], fields[s, other, :]
            down_r, down_i = weak * re, weak * im
            total = total + (down_r * re + down_i * im)
            for spot, value in ((where, down_r), (other, down_i)):
                first, second = value[:, : 2 * h], value[:, 2 * h :]
                for side, pair in enumerate((first + second, first - second)):
                    high, low = split(pair)
                    dest[side, spot, : 2 * h] = high
                    dest[side, spot, 2 * h :] = low
        total = total[:SUB] + total[SUB:]
        totals[s] = total[:, :h] + total[:, h : 2 * h] + total[:, 2 * h : 3 * h] + total[:, 3 * h :]

    def from_field(s, slot):
        weight = 2.0 * share_of(s)
        sides = []
        for side in range(2):
            settle = once(weighed[slot, side], tab["half_yt"][side])
            sides.append((settle[:, :h] + settle[:, h:]) * weight)
        even_r, even_i, odd_i, odd_r = (side[part * rows : (part + 1) * rows] for side in sides for part in range(2))
        for q, value in enumerate((even_r + odd_r, even_r - odd_r, even_i - odd_i, even_i + odd_i)):
            high, low = split(value)
            settled[slot, :rows, quarter[q]] = high
            settled[slot, rows:, quarter[q]] = low

    def from_rows(s, slot):
        full = lax.dot_general(half_xt[:, : 2 * rows], settled[slot], dims, preferred_element_type=F32)
        full = full + lax.dot_general(
            half_xt[:, 2 * rows :], settled[slot, :rows], dims, preferred_element_type=F32
        )
        for where in chunk_rows:
            kept = [keeps[s, q, where, :] for q in range(4)]
            top, low = full[where], full[where.start + h : where.stop + h]
            sums_of = [top[:, q] for q in quarter]
            turns_of = [low[:, q] for q in quarter]
            for part in range(2):
                for side in range(2):
                    even, odd = sums_of[2 * part + side], turns_of[2 - 2 * part + side]
                    more, less = (even - odd, even + odd) if part == 0 else (even + odd, even - odd)
                    grads[side, part, where, :] += kept[side] * more
                    grads[2 + side, part, where, :] += kept[2 + side] * less

    def backward(i, carry):
        base = i * unroll
        for t in range(unroll + 2):
            if t < unroll:
                weigh(base + t, t)
            if 0 <= t - 1 < unroll:
                from_field(base + t - 1, t - 1)
            if 0 <= t - 2 < unroll:
                from_rows(base + t - 2, t - 2)
        return carry

    lax.fori_loop(0, sources // unroll, backward, 0)
    each = lane_sum(jnp.sum(totals[...], 1))
    own = lax.broadcasted_iota(jnp.int32, (sources, LANES), 0) == lane
    sums = jnp.sum(jnp.where(own, each, 0.0), 0, keepdims=True)
    sums = jnp.where(lane == sources, squares, sums)

    def unturn(slot, sign):
        s = turn_s if sign > 0 else -turn_s
        re, im = grads[slot, 0], grads[slot, 1]
        return re * turn_c + im * s, im * turn_c - re * s

    pp, pm, mp, mm = unturn(0, 1), unturn(1, 1), unturn(2, -1), unturn(3, -1)
    pieces = ((pp[0], mm[0]), (pm[0], mp[0]), (-pp[1], mm[1]), (-pm[1], mp[1]))
    last_row = jnp.zeros((1, LANES), F32)
    for i, (first, second) in enumerate(pieces):
        ext = exts.at[i]
        ext[...] = jnp.zeros((h + SUB, 2 * h), F32)
        if i in (0, 2):
            ext[1 : h + 1, :h] = second
            moved = pltpu.roll(ext[...], 1, 1)
            ext[...] = moved
            ext[:h, :h] += first
        else:
            ext[:h, :h] = first
            moved = pltpu.roll(ext[...], 1, 1)
            ext[...] = moved
            ext[1 : h + 1, :h] += second
        grad_t[i] = ext[:h, :h].T.reshape(chips, 2, SUB, h)
        copy_to(8, partner, grad_t.at[i, :, 1 - core], pair_in.at[i]).start()
        edge_back[i] = ext[h : h + 1, :h]
        edge_back[4 + i] = ext[:h, h:].T[0:1, :]
        last_row = jnp.where(lane == i, ext[h : h + 1, h : h + 1], last_row)
    edge_back[8] = last_row
    edge_back[9] = sums
    for i in range(10, devices):
        edge_back[i] = jnp.zeros((1, LANES), F32)

    send_all(5, lambda p: edge_back.at[p], edge_back_in.at[me])
    edge_back_in[me] = edge_back[me]
    wait_all(8, pair_in)
    for i in range(4):
        pair_sum[:, i] = grad_t[i, :, core] + pair_in[i]

    each_chip(lambda peer: copy_to(4, peer, pair_sum.at[peer // 2], grad_in.at[chip]).start())
    grad_in[chip] = pair_sum[chip]
    wait_all(5, edge_back_in.at[most])
    edge_back_all[me] = jnp.sum(edge_back_in[...], 0)
    send_all(7, lambda p: edge_back_all.at[me], edge_back_all.at[me])
    wait_all(4, grad_in.at[pl.ds(0, chips - 1)])

    def unmix(u, v, wp, wm):
        return u + v, wp - wm, wp + wm, v - u

    mine = jnp.sum(grad_in[...], 0)
    cc, cs, sc, ss = unmix(mine[0], mine[1], mine[2], mine[3])
    sum_c = jnp.concatenate([cc, cs], 0)[None]
    sum_s = jnp.concatenate([sc, ss], 0)[None]
    back_c = far_c * sum_c + far_s * sum_s
    back_s = far_c * sum_s - far_s * sum_c
    turned = jnp.concatenate([back_c, back_s], 2).reshape(devices * 2 * SUB, 2 * h)
    gathered = product(split(turned), both("wave_x"), flip=True)
    back_rows[...] = gathered.reshape(devices, 2, SUB, rows)
    send_all(6, lambda p: back_rows.at[p], back_in.at[:, pl.ds(me * SUB, SUB), :])
    back_in[:, pl.ds(me * SUB, SUB), :] = back_rows[me]
    wait_all(7, edge_back_all.at[most])

    sums = edge_back_all[9]
    small_at = slice(2 * h + LANES, 2 * h + 2 * LANES)
    result[0:1, small_at] = sums * norming
    sums = jnp.where(lane < sources, sums, 0.0)
    result[1:2, small_at] = share_row * (sums - lane_sum(share_row * sums)) * norming
    result[2:3, small_at] = group_row.astype(F32)

    side_x = unmix(*(edge_back_all[i] for i in range(4)))
    side_y = unmix(*(edge_back_all[4 + i] for i in range(4)))
    corner = unmix(*(lane_sum(jnp.where(lane == i, edge_back_all[8], 0.0)) for i in range(4)))
    far_c, far_s = tab["far"][0, me], tab["far"][1, me]
    near = []
    for c, s in ((side_y[0], side_y[2]), (side_y[1], side_y[3])):
        near.append(jnp.concatenate([far_c * c + far_s * s, far_c * s - far_s * c], 1))
    near = jnp.concatenate(near + [jnp.zeros((SUB - 2, 2 * h), F32)], 0)
    last = product(split(near), both("wave_x"), flip=True)
    edge_c, edge_s = edge_rows[0:1], edge_rows[1:2]
    last_c = last[0:1] + corner[0] * edge_c + corner[2] * edge_s
    last_s = last[1:2] + corner[1] * edge_c + corner[3] * edge_s
    result[:, 2 * h : 2 * h + LANES] = column(last_c) * edge_c + column(last_s) * edge_s
    col_c, col_s = column(edge_c), column(edge_s)

    wait_all(6, back_in.at[:, pl.ds(0, h - SUB), :])
    part_c = back_in[0].T + col_c * side_x[0] + col_s * side_x[2]
    part_s = back_in[1].T + col_c * side_x[1] + col_s * side_x[3]
    result[:, :h] = part_c
    result[:, h : 2 * h] = part_s
    drain(0, rows_in.at[most])
    drain(1, edge_in.at[most])
    drain(2, chunk.at[most])
    drain(3, edge_all.at[most])
    drain(4, grad_in.at[pl.ds(0, chips - 1)])
    drain(5, edge_back_in.at[most])
    drain(6, back_in.at[:, pl.ds(0, h - SUB), :])
    drain(7, edge_back_all.at[most])
    drain(8, pair_in)


def closing(n, sources, result, wave, loss_hbm, grad_hbm, group_hbm, loss, group, out, out_sem):
    block = 2 * LANES
    blocks = n // block
    lane = lax.broadcasted_iota(jnp.int32, (1, LANES), 1)
    h = K // 2
    small = result.at[:, 2 * h + LANES :]
    loss[0] = jnp.sum(jnp.where(lane == sources, small[0:1, :], 0.0))
    for g in range(NG):
        group[g] = jnp.sum(jnp.where(small[2:3, :] == g, small[1:2, :], 0.0))
    stores = [
        pltpu.make_async_copy(loss, loss_hbm, out_sem.at[blocks]),
        pltpu.make_async_copy(group, group_hbm, out_sem.at[blocks + 1]),
    ]
    for store in stores:
        store.start()
    value = result[:, : 2 * h]
    turn = lax.rem(lax.broadcasted_iota(jnp.int32, value.shape, 1), 2) == 0
    pairs = split(value), split(jnp.where(turn, value, -value))
    spread = result[:, 2 * h : 2 * h + LANES]
    adds = jnp.concatenate([spread, spread], 1)
    for b in range(blocks):
        where = slice(b * block, (b + 1) * block)
        side, start = divmod(b * block, n // 2)
        from_where = slice(start, start + block)
        out[:, where] = product(pairs[side], (wave[0, :, from_where], wave[1, :, from_where])) + adds
        stores.append(pltpu.make_async_copy(out.at[:, where], grad_hbm.at[:, where], out_sem.at[b]))
        stores[-1].start()
    for store in stores:
        store.wait()


def fused(devices, mask_field, target_print, source_points, source_groups, group_logits, pupil_radius):
    rows, n = mask_field.shape
    h = K // 2
    coarse = 2 * K
    sources = source_points.shape[0]
    consts = tables(n, rows, devices)
    anywhere = pl.BlockSpec(memory_space=pltpu.HBM)
    vmem = lambda *shape: pltpu.VMEM(shape, F32)
    scratch = [pltpu.VMEM(consts[k].shape, consts[k].dtype) for k in NAMES] + [
        vmem(rows, n), pltpu.VMEM((rows, n), jnp.int32),
        vmem(2, h, rows), vmem(devices, 1, LANES), vmem(devices, 2, SUB, rows), vmem(devices, 1, LANES),
        vmem(devices, 4, SUB, h), vmem(devices, 1, LANES), vmem(4, h + SUB, 2 * h), vmem(4, 2, h, h),
        vmem(4, 2, h, h), vmem(sources, 2 * rows, coarse), vmem(rows, coarse), vmem(rows, coarse),
        vmem(4, 2, h, h), vmem(4, devices // 2, 2, SUB, h), vmem(devices, 1, LANES), vmem(devices // 2, 4, SUB, h),
        vmem(devices, 1, LANES), vmem(devices, 1, LANES), vmem(devices, 2, SUB, rows), vmem(2, h, rows),
        pltpu.VMEM((8, 2, 2 * h, coarse), BF16), pltpu.VMEM((8, 2, 2 * rows, 2 * h), BF16),
        pltpu.VMEM((8, 2, 2 * rows, coarse), BF16), pltpu.VMEM((8, 2 * rows, coarse), BF16),
        vmem(sources, SUB, LANES), vmem(sources, 4, h, h),
        pltpu.SMEM((2, sources), jnp.int32), pltpu.SMEM((sources,), jnp.int32), pltpu.SMEM((NG,), F32),
        pltpu.SMEM((1,), jnp.int32),
        vmem(4, devices // 2, SUB, h), vmem(devices // 2, 4, SUB, h),
        pltpu.VMEM((2, n, coarse), BF16), pltpu.VMEM((2, rows, n), BF16),
        pltpu.SemaphoreType.DMA((26,)),
        pltpu.SemaphoreType.DMA((9,)), pltpu.SemaphoreType.DMA((9,)), pltpu.SemaphoreType.DMA((devices // 2,)),
    ]
    arrays = [jnp.asarray(consts[k]) for k in NAMES]
    hold = lambda value: pltpu.with_memory_space_constraint(value, pltpu.HBM)
    inside = pl.BlockSpec(memory_space=pltpu.VMEM)
    (result,) = pl.pallas_call(
        functools.partial(kernel, devices, n),
        out_shape=(
            jax.ShapeDtypeStruct((rows, 2 * h + 2 * LANES), F32),
        ),
        in_specs=[anywhere] * (6 + len(NAMES)),
        out_specs=(inside,),
        scratch_shapes=scratch,
        compiler_params=pltpu.CompilerParams(
            collective_id=0, has_side_effects=True, vmem_limit_bytes=53 * 1024 * 1024
        ),
    )(*map(hold, (source_points.T, source_groups, group_logits)), pupil_radius,
      *map(hold, (mask_field, target_print, *arrays)))
    return pl.pallas_call(
        functools.partial(closing, n, sources),
        out_shape=(
            jax.ShapeDtypeStruct((1,), F32),
            jax.ShapeDtypeStruct((rows, n), F32),
            jax.ShapeDtypeStruct((NG,), F32),
        ),
        in_specs=[inside] * 2,
        out_specs=(anywhere, anywhere, anywhere),
        scratch_shapes=[
            pltpu.SMEM((1,), F32), pltpu.SMEM((NG,), F32), vmem(rows, n),
            pltpu.SemaphoreType.DMA((n // (2 * LANES) + 2,)),
        ],
        compiler_params=pltpu.CompilerParams(vmem_limit_bytes=8 * 1024 * 1024),
    )(result, arrays[0])


HIGH = lax.Precision.HIGH


def dot(form, left, right):
    return jnp.einsum(form, left, right, precision=HIGH, preferred_element_type=F32)


def waves(left, right, length):
    turns = angles(left, right, length)
    return np.cos(turns), np.sin(turns)


def shifted_waves(count, freq, length, device, devices):
    near = np.stack(waves(np.arange(count), freq, length)).astype(np.float32)
    far = np.stack(waves(np.arange(devices) * count, freq, length)).astype(np.float32)
    far = lax.dynamic_slice_in_dim(jnp.asarray(far), device, 1, axis=1)
    return far[0] * near[0] - far[1] * near[1], far[1] * near[0] + far[0] * near[1]


def exchange(blocks):
    return lax.all_to_all(blocks, "slab", 0, 0)


def plain(devices, mask_field, target_print, source_points, source_groups, group_logits, pupil_radius):
    rows, n = mask_field.shape
    sources = source_points.shape[0]
    coarse = 2 * K
    step = n // coarse
    cols = coarse // devices
    half = n // 2
    device = lax.axis_index("slab")
    freq = np.arange(K, dtype=np.int64) - K // 2
    order = np.concatenate([freq[freq % 2 == 0], freq[freq % 2 == 1]])
    kh = K // 2
    norming = 1.0 / (n * n)

    cos_y, sin_y = waves(np.arange(half), order, n)
    fold = [
        jnp.asarray(np.concatenate([t[:, p * kh : (p + 1) * kh] for t in (cos_y, sin_y)], 1), F32)
        for p in (0, 1)
    ]
    lag = np.mod(np.arange(n)[None, :] - step * np.arange(coarse)[:, None], n)
    response = np.zeros(n)
    for f in range(1, K):
        response += 2.0 * np.cos(2.0 * math.pi * np.mod(f * np.arange(n), n) / n)
    response = (response + 1.0) / coarse
    up = jnp.asarray(response[lag], F32)
    cos_c, sin_c = waves(freq, np.arange(coarse), coarse)
    wave_x = jnp.asarray(np.concatenate([cos_c, sin_c], 1), F32)
    loc_c, loc_s = shifted_waves(rows, freq, n, device, devices)
    loc = jnp.concatenate([loc_c, loc_s], 1)
    a, b = shifted_waves(cols, order, coarse, device, devices)
    lift = jnp.concatenate([jnp.concatenate([a, -b], 1), jnp.concatenate([b, a], 1)], 0)

    cutoff = pupil_radius[0]
    shifted = (source_points - GRID // 2) * cutoff // shift_scale
    first = jnp.asarray(freq, jnp.int32)[None, None, :] + shifted[:, 0, None, None]
    second = jnp.asarray(np.tile(order, 2), jnp.int32)[None, :, None] + shifted[:, 1, None, None]
    passed = first * first + second * second <= cutoff * cutoff

    near, away = mask_field[:, :half], mask_field[:, half:]
    even = dot("xy,yq->xq", near + away, fold[0])
    odd = dot("xy,yq->xq", near - away, fold[1])
    part_c = jnp.concatenate([even[:, :kh], odd[:, :kh]], 1)
    part_s = jnp.concatenate([even[:, kh:], odd[:, kh:]], 1)
    spec = dot("xq,xk->qk", jnp.concatenate([part_c, part_s], 1), loc)
    band = jnp.concatenate([spec[:K, :K] - spec[K:, K:], -(spec[:K, K:] + spec[K:, :K])], 0)
    band = jnp.sum(exchange(band.reshape(devices, 2 * K // devices, K)), 0)
    band = lax.all_gather(band, "slab", tiled=True)

    kept = jnp.where(passed, band[None], 0.0)
    wide = dot("aq,sqk->sak", lift, kept)
    both = dot("ak,kx->ax", wide.reshape(sources * 2 * cols, K), wave_x)
    both = both.reshape(sources, 2, cols, 2 * coarse)
    field_re = (both[:, 0, :, :coarse] - both[:, 1, :, coarse:]) * norming
    field_im = (both[:, 0, :, coarse:] + both[:, 1, :, :coarse]) * norming
    bright = field_re * field_re + field_im * field_im
    onehot = (source_groups[:, None] == jnp.arange(NG, dtype=jnp.int32)[None, :]).astype(F32)
    weights = jnp.exp(jnp.sum(onehot * group_logits[None, :], 1))
    share = weights / jnp.sum(weights)
    image = jnp.sum(share[:, None, None] * bright, 0)

    tall = dot("cm,mx->cx", image, up)
    tall = lax.all_to_all(tall, "slab", 1, 0, tiled=True)
    intensity = dot("cx,cy->xy", tall, up)
    resist = jax.nn.sigmoid(steepness * (intensity - threshold))
    misfit = resist - target_print.astype(F32)
    slope = (2.0 * steepness) * misfit * resist * (1.0 - resist)
    squares = jnp.sum(misfit * misfit)
    down = dot("xy,cy->cx", slope, up)
    down = lax.all_to_all(down, "slab", 0, 1, tiled=True)
    pull = dot("cx,mx->cm", down, up)

    per_source = jnp.sum(bright * pull[None], (1, 2))
    sums = jnp.concatenate([per_source, squares[None]])
    factor = (2.0 * norming) * share[:, None, None] * pull[None]
    back = jnp.stack([factor * field_re, factor * field_im], 1)
    low = dot("ax,kx->ak", back.reshape(sources * 2 * cols, coarse), wave_x[:, :coarse])
    lows = dot("ax,kx->ak", back.reshape(sources * 2 * cols, coarse), wave_x[:, coarse:])
    low = low.reshape(sources, 2, cols, K)
    lows = lows.reshape(sources, 2, cols, K)
    settle = jnp.concatenate([low[:, 0] + lows[:, 1], low[:, 1] - lows[:, 0]], 1)
    settle = dot("aq,sak->sqk", lift, settle)
    grad_band = jnp.sum(jnp.where(passed, settle, 0.0), 0).reshape(devices, 2 * K // devices, K)
    extra = jnp.pad(sums[None, :], ((0, 7), (0, K - sources - 1)))
    extra = jnp.broadcast_to(extra[None], (devices, 8, K))
    grad_band = jnp.sum(exchange(jnp.concatenate([grad_band, extra], 1)), 0)
    sums = grad_band[-8, : sources + 1]
    grad_band = lax.all_gather(grad_band[:-8], "slab", tiled=True)
    per_source, squares = sums[:-1], sums[-1]
    loss_value = (squares * norming).reshape(1)
    against = jnp.sum(share * per_source)
    source_pull = share * (per_source - against)
    group_grad = jnp.sum(onehot * source_pull[:, None], 0) * norming

    spread = dot("tk,qk->tq", jnp.concatenate([loc_c, loc_s], 0), grad_band)
    spread_re = spread[:rows, :K] - spread[rows:, K:]
    spread_im = spread[:rows, K:] + spread[rows:, :K]
    even = dot("xq,yq->xy", jnp.concatenate([spread_re[:, :kh], -spread_im[:, :kh]], 1), fold[0])
    odd = dot("xq,yq->xy", jnp.concatenate([spread_re[:, kh:], -spread_im[:, kh:]], 1), fold[1])
    mask_grad = jnp.concatenate([even + odd, even - odd], 1)
    return loss_value, mask_grad, group_grad


def on_device(devices, mask_field, *others):
    tiles = mask_field.shape[0] == LANES and K // 2 == LANES == SUB * devices and devices % 8 == 0 and devices >= 10
    return (fused if tiles else plain)(devices, mask_field, *others)


def solution(mesh):
    in_specs = (
        P(("clip", "slab"), None),
        P(("clip", "slab"), None),
        P("clip", None),
        P("clip"),
        P("clip"),
        P("clip"),
    )
    out_specs = (P("clip"), P(("clip", "slab"), None), P("clip"))
    return jax.shard_map(
        functools.partial(on_device, mesh.shape["slab"]),
        mesh=mesh, in_specs=in_specs, out_specs=out_specs, check_vma=False,
    )
```

```python
import functools
import math

import jax
import jax.numpy as jnp
import numpy as np
from jax import lax
from jax.experimental import pallas as pl
from jax.experimental.pallas import tpu as pltpu
from jax.sharding import PartitionSpec as P

K = 256
GRID = 61
NG = 8

steepness = 8.0
threshold = 0.3
shift_scale = 45
F32 = jnp.float32
BF16 = jnp.bfloat16
LANES = 128
SUB = 8


def angles(left, right, length):
    turns = np.mod(np.asarray(left)[:, None] * np.asarray(right)[None, :], length)
    return 2.0 * math.pi * turns.astype(np.float64) / length


def halves(table):
    table = np.asarray(table, np.float32)
    high = table.astype(BF16)
    low = (table - high.astype(np.float32)).astype(BF16)
    return np.stack([high, low])


def split(value):
    high = value.astype(BF16)
    return high, (value - high.astype(F32)).astype(BF16)


def product(left, right, flip=False):
    dims = (((1,), (1 if flip else 0,)), ((), ()))
    one = lambda a, b: lax.dot_general(a, b, dims, preferred_element_type=F32)
    return one(left[0], right[0]) + one(left[1], right[0]) + one(left[0], right[1])


def tables(n, rows, devices):
    h = K // 2
    coarse = 2 * K
    step = n // coarse
    freq = np.arange(h)
    near = np.arange(rows)
    wave_y = angles(freq, np.arange(n // 2), n)
    wave_y = np.concatenate([np.cos(wave_y), np.sin(wave_y)], 0)
    wave_x = angles(near, freq, n)
    wave_x = np.concatenate([np.cos(wave_x), np.sin(wave_x)], 1)
    half_x = angles(near, 2 * freq + 1, 2 * n)
    half_x = np.concatenate([np.cos(half_x), -np.sin(half_x)], 1)
    spots = step * np.arange(coarse // 2) + step // 2
    half_y = angles(2 * freq + 1, spots, 2 * n)
    half_y = [halves(np.cos(half_y)), halves(np.sin(half_y))]
    ahead = np.stack([np.concatenate([t[0], t[0], t[1]], 0) for t in half_y])
    behind = np.stack([
        np.block([[t[0].T, t[1].T], [t[0].T, np.zeros_like(t[0].T)]]) for t in half_y
    ])
    far = angles(rows * np.arange(devices), freq, n)
    far = np.stack([np.cos(far), np.sin(far)])[:, :, None, :].astype(np.float32)
    half_far = angles(rows * np.arange(devices), 2 * freq + 1, 2 * n)
    half_far = np.stack([np.cos(half_far), np.sin(half_far)]) / (n * n)
    half_far = half_far[:, :, None, :].astype(np.float32)
    block = 2 * LANES
    extra = n // step - block // step
    index = np.arange(coarse // 2 + extra)[:, None]
    spot = np.concatenate([step * (index - extra) + step // 2, -step * index - step // 2], 0)
    lag = np.mod(np.arange(block)[None, :] - spot, n)
    kernel = np.ones(n)
    for f in range(1, K):
        kernel += 2.0 * np.cos(2.0 * math.pi * np.mod(f * np.arange(n), n) / n)
    up = (kernel / coarse)[lag]
    edge = angles([h], np.arange(LANES), n)
    edge = np.concatenate([np.cos(edge), np.sin(edge)], 0)
    edge = np.concatenate([edge, np.zeros((SUB - 2, LANES))], 0)
    return {
        "wave_y": halves(wave_y),
        "wave_x": halves(wave_x),
        "half_x": halves(half_x),
        "half_xt": np.concatenate(list(halves(half_x.T)[[0, 0, 1]]), 1),
        "half_y": ahead,
        "half_yt": behind,
        "up": halves(up),
        "far": far,
        "half_far": half_far,
        "edge": edge.astype(np.float32),
    }


NAMES = ("wave_y", "wave_x", "half_x", "half_xt", "half_y", "half_yt", "up", "far", "half_far", "edge")


def kernel(devices, n, *refs):
    small_hbm, mask_hbm, target_hbm = refs[:4], refs[4], refs[5]
    sources_in = dict(zip(NAMES, refs[6 : 6 + len(NAMES)]))
    refs = refs[6 + len(NAMES) :]
    result = refs[0]
    refs = refs[1:]
    tab = dict(zip(NAMES, refs[: len(NAMES)]))
    refs = refs[len(NAMES) :]
    (mask, target, rows_t, edge_out, rows_in, edge_in, chunk, edge_all, exts, band, data, fields, image, pull,
     grads, grad_t, edge_back, grad_in, edge_back_in, edge_back_all, back_rows, back_in,
     folded, wides, weighed, settled, totals, keeps, points, groups, logits, radius,
     pair_in, pair_sum, up_t, slopes, local_sem, send_sem, recv_sem, near_sem) = refs
    h = K // 2
    coarse = 2 * K
    sources = points.shape[1]
    rows = mask.shape[0]
    block = 2 * LANES
    blocks = n // block
    step = n // coarse
    me = lax.axis_index("slab")
    norming = 1.0 / (n * n)
    chips = devices // 2
    core, chip = lax.rem(me, 2), me // 2
    partner = me + 1 - 2 * core
    most = pl.ds(0, devices - 1)

    loads = {}
    small = (points, groups, logits, radius)
    late = ("up", "half_far", "half_x", "half_y", "target", "half_yt", "half_xt")
    part = n // 8
    pieces = [(slice(c, c + part), slice(c + n // 2, c + n // 2 + part)) for c in range(0, n // 2, part)]
    for i, (name, src, dst) in enumerate(
        [
            piece
            for k, (where, away) in enumerate(pieces)
            for piece in (
                (f"near{k}", mask_hbm.at[:, where], mask.at[:, where]),
                (f"away{k}", mask_hbm.at[:, away], mask.at[:, away]),
                (f"wave_y{k}", sources_in["wave_y"].at[:, :, where], tab["wave_y"].at[:, :, where]),
            )
        ]
        + [(f"small{k}", small_hbm[k], small[k]) for k in range(4)]
        + [(k, sources_in[k], tab[k]) for k in ("edge", "wave_x", "far", "half_far", "half_x", "half_y")]
        + [("up", sources_in["up"], tab["up"]), ("target", target_hbm, target)]
        + [(k, sources_in[k], tab[k]) for k in ("half_yt", "half_xt")]
    ):
        loads[name] = pltpu.make_async_copy(src, dst, local_sem.at[i])
        if name not in late:
            loads[name].start()

    barrier = pltpu.get_barrier_semaphore()

    def greet(i, carry):
        pl.semaphore_signal(barrier, inc=1, device_id={"slab": lax.rem(me + i, devices)})
        return carry

    lax.fori_loop(1, devices, greet, 0)

    def both(name):
        return tab[name][0], tab[name][1]

    def copy_to(phase, peer, src, dst, sem=None):
        return pltpu.make_async_remote_copy(
            src_ref=src, dst_ref=dst, send_sem=send_sem.at[phase],
            recv_sem=recv_sem.at[phase] if sem is None else sem, device_id={"slab": peer},
        )

    group = 4
    planes = devices // group
    lower = 1 - me // (group * (planes // 2))

    def plane_of(i):
        return lower * (planes - 1 - 2 * i) + i

    def send_all(phase, src_of, dst):
        for i in range(devices):
            peer = plane_of(i // group) * group + lax.rem(me + i % group, group)

            @pl.when(peer != me)
            def _():
                copy_to(phase, peer, src_of(peer), dst).start()

    def each_chip(act, reverse=False):
        for i in range(chips)[:: -1 if reverse else 1]:
            other = plane_of(i // 2) * 2 + lax.rem(chip + i % 2, 2)

            @pl.when(other != chip)
            def _():
                act(other * 2 + core)

    def wait_all(phase, ref, sem=None):
        copy_to(phase, partner, ref, ref, sem).wait_recv()

    def drain(phase, ref):
        copy_to(phase, partner, ref, ref).wait_send()

    lane = lax.broadcasted_iota(jnp.int32, (1, LANES), 1)

    def column(row):
        return jnp.broadcast_to(row, (LANES, LANES)).T

    even = odd = 0.0
    for k, (where, away) in enumerate(pieces):
        for name in ("near", "away", "wave_y"):
            loads[f"{name}{k}"].wait()
        wave = (tab["wave_y"][0, :, where], tab["wave_y"][1, :, where])
        first, second = mask[:, where], mask[:, away]
        even = even + product(split(first + second), wave, flip=True)
        odd = odd + product(split(first - second), wave, flip=True)
    for name in late:
        loads[name].start()
    wide_lane = lax.broadcasted_iota(jnp.int32, (rows, 2 * h), 1)
    transformed = jnp.where(lax.rem(wide_lane, 2) == 0, even, odd)
    rows_t[0] = transformed[:, :h].T
    rows_t[1] = transformed[:, h:].T
    loads["edge"].wait()
    loads["wave_x"].wait()
    loads["far"].wait()
    edge_rows = tab["edge"][...]
    edge_pair = split(edge_rows)
    summed = mask[:, :LANES]
    for b in range(1, n // LANES):
        summed = summed + mask[:, b * LANES : (b + 1) * LANES]
    side_x = product(edge_pair, split(transformed))
    last = product(edge_pair, split(summed), flip=True)
    side_y = product(split(last), both("wave_x"))
    far_c, far_s = tab["far"][0, me], tab["far"][1, me]
    side_c = far_c * side_y[:2, :h] - far_s * side_y[:2, h:]
    side_s = far_s * side_y[:2, :h] + far_c * side_y[:2, h:]

    def mixes(cc, cs, sc, ss):
        return cc - ss, cc + ss, sc + cs, sc - cs

    edges = mixes(side_x[0:1, :h], side_x[0:1, h:], side_x[1:2, :h], side_x[1:2, h:])
    edges = edges + mixes(side_c[0:1], side_c[1:2], side_s[0:1], side_s[1:2])

    def lane_sum(value):
        return jnp.sum(value, axis=1, keepdims=True)

    corner = mixes(
        lane_sum(last[0:1] * edge_rows[0:1]), lane_sum(last[1:2] * edge_rows[0:1]),
        lane_sum(last[0:1] * edge_rows[1:2]), lane_sum(last[1:2] * edge_rows[1:2]),
    )
    corner_row = jnp.zeros((1, LANES), F32)
    for i in range(4):
        corner_row = jnp.where(lane == i, corner[i], corner_row)
    for i in range(8):
        edge_out[i] = edges[i]
    edge_out[8] = corner_row
    for i in range(9, devices):
        edge_out[i] = jnp.zeros((1, LANES), F32)

    pl.semaphore_wait(barrier, devices - 1)
    send_all(1, lambda p: edge_out.at[p], edge_in.at[me])
    send_all(0, lambda p: rows_t.at[:, pl.ds(p * SUB, SUB), :], rows_in.at[me])
    rows_in[me] = rows_t[:, pl.ds(me * SUB, SUB), :]
    edge_in[me] = edge_out[me]

    for k in range(4):
        loads[f"small{k}"].wait()
    logit_row = jnp.full((1, LANES), 0.0, F32)
    group_row = jnp.full((1, LANES), -1, jnp.int32)
    for s in range(sources):
        g = groups[s]
        logit_row = jnp.where(lane == s, logits[g], logit_row)
        group_row = jnp.where(lane == s, g, group_row)
    weight_row = jnp.where(lane < sources, jnp.exp(logit_row), 0.0)
    share_row = weight_row / jnp.sum(weight_row, axis=1, keepdims=True)

    loads["up"].wait()
    extra = (n - block) // step

    def taps(b):
        first, second = extra - b * (block // step), extra + 2 * h + b * (block // step)
        return slice(first, first + 2 * h), slice(second, second + 2 * h)

    for b in range(blocks):
        for part in range(2):
            for side, spot in enumerate(taps(b)):
                up_t[part, b * block : (b + 1) * block, side * 2 * h : (side + 1) * 2 * h] = tab["up"][part, spot, :].T
    cutoff = radius[0]
    limit = (cutoff * cutoff).astype(F32)
    lane_index = lane.astype(F32)
    chunk_rows = [slice(c, c + 2 * SUB) for c in range(0, h, 2 * SUB)]
    row_index = lax.broadcasted_iota(jnp.int32, (2 * SUB, LANES), 0).astype(F32)

    def masks(s):
        first = ((points[0, s] - GRID // 2) * cutoff // shift_scale).astype(F32)
        second = ((points[1, s] - GRID // 2) * cutoff // shift_scale).astype(F32)
        col_p, col_m = lane_index + second, second - 1.0 - lane_index
        col_p, col_m = col_p * col_p, col_m * col_m

        def of(where):
            row_p = row_index + (first + where.start)
            row_m = (first - 1.0 - where.start) - row_index
            room_p, room_m = limit - row_p * row_p, limit - row_m * row_m
            return col_p <= room_p, col_m <= room_p, col_p <= room_m, col_m <= room_m

        return of

    def fill(s, carry):
        kept = masks(s)
        for where in chunk_rows:
            for q, flag in enumerate(kept(where)):
                keeps[s, q, where, :] = jnp.where(flag, 1.0, 0.0)
        return carry

    lax.fori_loop(0, sources, fill, 0)

    wait_all(1, edge_in.at[most])
    edge_all[me] = jnp.sum(edge_in[...], 0)
    send_all(3, lambda p: edge_all.at[me], edge_all.at[me])
    wait_all(0, rows_in.at[most])
    gathered = rows_in[...].reshape(devices * 2 * SUB, rows)
    turned = product(split(gathered), both("wave_x")).reshape(devices, 2 * SUB, 2 * h)
    far_c, far_s = tab["far"][0], tab["far"][1]
    turned_c, turned_s = turned[:, :, :h], turned[:, :, h:]
    sum_c = jnp.sum(far_c * turned_c - far_s * turned_s, 0)
    sum_s = jnp.sum(far_s * turned_c + far_c * turned_s, 0)
    for i, value in enumerate(mixes(sum_c[:SUB], sum_c[SUB:], sum_s[:SUB], sum_s[SUB:])):
        chunk[me, i] = value

    each_chip(lambda peer: copy_to(2, peer, chunk.at[me], chunk.at[me], near_sem.at[chip]).start())
    copy_to(2, partner, chunk.at[me], chunk.at[me]).start()

    loads["half_far"].wait()
    loads["half_x"].wait()
    loads["half_y"].wait()
    turn_c = column(tab["half_far"][0, me])
    turn_s = column(tab["half_far"][1, me])


    def relay(peer):
        wait_all(2, chunk.at[peer], near_sem.at[peer // 2])
        copy_to(2, partner, chunk.at[peer], chunk.at[peer]).start()

    each_chip(relay, reverse=True)
    wait_all(2, chunk.at[pl.ds(0, chips)])
    wait_all(3, edge_all.at[most])
    shifted = []
    plain = []
    for i in range(4):
        ext = exts.at[i]
        ext[:h, :h] = chunk[:, i].reshape(h, h).T
        ext[h : h + 1, :h] = edge_all[i]
        ext[:h, h:] = column(edge_all[4 + i])
        ext[h : h + 1, h:] = jnp.broadcast_to(lane_sum(jnp.where(lane == i, edge_all[8], 0.0)), (1, LANES))
        plain = ext[...]
        moved = pltpu.roll(plain, 2 * h - 1, 1)
        if i in (0, 2):
            first, second = ext[:h, :h], None
            ext[...] = moved
            second = ext[1 : h + 1, :h]
        else:
            second = ext[1 : h + 1, :h]
            ext[...] = moved
            first = ext[:h, :h]
        data[i, 0] = first
        data[i, 1] = second

    def turn(slot, re, im, sign):
        s = turn_s if sign > 0 else -turn_s
        band[slot, 0] = re * turn_c - im * s
        band[slot, 1] = re * s + im * turn_c

    turn(0, data[0, 0], -data[2, 0], 1)
    turn(1, data[1, 0], -data[3, 0], 1)
    turn(2, data[1, 1], data[3, 1], -1)
    turn(3, data[0, 1], data[2, 1], -1)

    def share_of(s):
        return lane_sum(jnp.where(lane == s, share_row, 0.0))

    def keep(ref, where, lanes, value):
        high, low = split(value)
        ref[0, where, lanes] = high
        ref[1, where, lanes] = low

    unroll = 8
    quarter = [slice(i * h, (i + 1) * h) for i in range(4)]
    image[...] = jnp.zeros_like(image)

    def mask_band(s, slot):
        dest = folded.at[slot]
        for where in chunk_rows:
            kept = [keeps[s, q, where, :] for q in range(4)]
            low_where = slice(where.start + h, where.stop + h)
            pp, pm, mp, mm = (kept[q] * band[q, 0, where, :] for q in range(4))
            keep(dest, where, quarter[0], pp + mp)
            keep(dest, where, quarter[1], pm + mm)
            keep(dest, low_where, quarter[2], mp - pp)
            keep(dest, low_where, quarter[3], mm - pm)
            pp, pm, mp, mm = (kept[q] * band[q, 1, where, :] for q in range(4))
            keep(dest, where, quarter[2], pp + mp)
            keep(dest, where, quarter[3], pm + mm)
            keep(dest, low_where, quarter[0], pp - mp)
            keep(dest, low_where, quarter[1], pm - mm)

    dims = (((1,), (0,)), ((), ()))

    def once(left, right):
        return lax.dot_general(left, right, dims, preferred_element_type=F32)

    def to_rows(slot):
        wide = product(both("half_x"), (folded[slot, 0], folded[slot, 1]))
        p_r, m_r, p_i, m_i = (wide[:, q] for q in quarter)
        for part, sides in enumerate(((p_r + m_r, m_i - p_i), (p_i + m_i, p_r - m_r))):
            for side, value in enumerate(sides):
                high, low = split(value)
                wides[slot, side, part * rows : (part + 1) * rows, :h] = high
                wides[slot, side, part * rows : (part + 1) * rows, h:] = low

    def to_field(s, slot):
        even, odd = (
            once(wides[slot, side], tab["half_y"][side, : 2 * h])
            + once(wides[slot, side, :, :h], tab["half_y"][side, 2 * h :])
            for side in range(2)
        )
        weight = share_of(s)
        for side, field in enumerate((even + odd, even - odd)):
            where = slice(side * 2 * h, (side + 1) * 2 * h)
            fields[s, :, where] = field
            re, im = field[:rows], field[rows:]
            image[:, where] += weight * (re * re + im * im)

    def forward(i, carry):
        base = i * unroll
        for t in range(unroll + 2):
            if t < unroll:
                mask_band(base + t, t)
            if 0 <= t - 1 < unroll:
                to_rows(t - 1)
            if 0 <= t - 2 < unroll:
                to_field(base + t - 2, t - 2)
        return carry

    lax.fori_loop(0, sources // unroll, forward, 0)

    loads["target"].wait()
    squares = jnp.zeros((rows, LANES), F32)
    image_pair = split(image[...])
    for b in range(blocks):
        where = slice(b * block, (b + 1) * block)
        up = [jnp.concatenate([tab["up"][part, spot, :] for spot in taps(b)], 0) for part in range(2)]
        intensity = product(image_pair, up)
        resist = 1.0 / (1.0 + jnp.exp(-steepness * (intensity - threshold)))
        misfit = resist - target[:, where].astype(F32)
        slope = (2.0 * steepness) * misfit * resist * (1.0 - resist)
        square = misfit * misfit
        squares = squares + square[:, :LANES] + square[:, LANES:]
        keep(slopes, slice(0, rows), where, slope)
    pull[...] = product((slopes[0], slopes[1]), (up_t[0], up_t[1]))
    squares = lane_sum(jnp.sum(squares, 0, keepdims=True))

    loads["half_yt"].wait()
    loads["half_xt"].wait()
    grads[...] = jnp.zeros_like(grads)
    half_xt = tab["half_xt"]

    def weigh(s, slot):
        dest = weighed.at[slot]
        total = jnp.zeros((2 * SUB, coarse), F32)
        for start in range(0, rows, 2 * SUB):
            where = slice(start, start + 2 * SUB)
            other = slice(start + rows, start + rows + 2 * SUB)
            weak, re, im = pull[where, :], fields[s, where, :], fields[s, other, :]
            down_r, down_i = weak * re, weak * im
            total = total + (down_r * re + down_i * im)
            for spot, value in ((where, down_r), (other, down_i)):
                first, second = value[:, : 2 * h], value[:, 2 * h :]
                for side, pair in enumerate((first + second, first - second)):
                    high, low = split(pair)
                    dest[side, spot, : 2 * h] = high
                    dest[side, spot, 2 * h :] = low
        total = total[:SUB] + total[SUB:]
        totals[s] = total[:, :h] + total[:, h : 2 * h] + total[:, 2 * h : 3 * h] + total[:, 3 * h :]

    def from_field(s, slot):
        weight = 2.0 * share_of(s)
        sides = []
        for side in range(2):
            settle = once(weighed[slot, side], tab["half_yt"][side])
            sides.append((settle[:, :h] + settle[:, h:]) * weight)
        even_r, even_i, odd_i, odd_r = (side[part * rows : (part + 1) * rows] for side in sides for part in range(2))
        for q, value in enumerate((even_r + odd_r, even_r - odd_r, even_i - odd_i, even_i + odd_i)):
            high, low = split(value)
            settled[slot, :rows, quarter[q]] = high
            settled[slot, rows:, quarter[q]] = low

    def from_rows(s, slot):
        full = lax.dot_general(half_xt[:, : 2 * rows], settled[slot], dims, preferred_element_type=F32)
        full = full + lax.dot_general(
            half_xt[:, 2 * rows :], settled[slot, :rows], dims, preferred_element_type=F32
        )
        for where in chunk_rows:
            kept = [keeps[s, q, where, :] for q in range(4)]
            top, low = full[where], full[where.start + h : where.stop + h]
            sums_of = [top[:, q] for q in quarter]
            turns_of = [low[:, q] for q in quarter]
            for part in range(2):
                for side in range(2):
                    even, odd = sums_of[2 * part + side], turns_of[2 - 2 * part + side]
                    more, less = (even - odd, even + odd) if part == 0 else (even + odd, even - odd)
                    grads[side, part, where, :] += kept[side] * more
                    grads[2 + side, part, where, :] += kept[2 + side] * less

    def backward(i, carry):
        base = i * unroll
        for t in range(unroll + 2):
            if t < unroll:
                weigh(base + t, t)
            if 0 <= t - 1 < unroll:
                from_field(base + t - 1, t - 1)
            if 0 <= t - 2 < unroll:
                from_rows(base + t - 2, t - 2)
        return carry

    lax.fori_loop(0, sources // unroll, backward, 0)
    each = lane_sum(jnp.sum(totals[...], 1))
    own = lax.broadcasted_iota(jnp.int32, (sources, LANES), 0) == lane
    sums = jnp.sum(jnp.where(own, each, 0.0), 0, keepdims=True)
    sums = jnp.where(lane == sources, squares, sums)

    def unturn(slot, sign):
        s = turn_s if sign > 0 else -turn_s
        re, im = grads[slot, 0], grads[slot, 1]
        return re * turn_c + im * s, im * turn_c - re * s

    pp, pm, mp, mm = unturn(0, 1), unturn(1, 1), unturn(2, -1), unturn(3, -1)
    pieces = ((pp[0], mm[0]), (pm[0], mp[0]), (-pp[1], mm[1]), (-pm[1], mp[1]))
    last_row = jnp.zeros((1, LANES), F32)
    for i, (first, second) in enumerate(pieces):
        ext = exts.at[i]
        ext[...] = jnp.zeros((h + SUB, 2 * h), F32)
        if i in (0, 2):
            ext[1 : h + 1, :h] = second
            moved = pltpu.roll(ext[...], 1, 1)
            ext[...] = moved
            ext[:h, :h] += first
        else:
            ext[:h, :h] = first
            moved = pltpu.roll(ext[...], 1, 1)
            ext[...] = moved
            ext[1 : h + 1, :h] += second
        grad_t[i] = ext[:h, :h].T.reshape(chips, 2, SUB, h)
        copy_to(8, partner, grad_t.at[i, :, 1 - core], pair_in.at[i]).start()
        edge_back[i] = ext[h : h + 1, :h]
        edge_back[4 + i] = ext[:h, h:].T[0:1, :]
        last_row = jnp.where(lane == i, ext[h : h + 1, h : h + 1], last_row)
    edge_back[8] = last_row
    edge_back[9] = sums
    for i in range(10, devices):
        edge_back[i] = jnp.zeros((1, LANES), F32)

    send_all(5, lambda p: edge_back.at[p], edge_back_in.at[me])
    edge_back_in[me] = edge_back[me]
    wait_all(8, pair_in)
    for i in range(4):
        pair_sum[:, i] = grad_t[i, :, core] + pair_in[i]

    each_chip(lambda peer: copy_to(4, peer, pair_sum.at[peer // 2], grad_in.at[chip]).start())
    grad_in[chip] = pair_sum[chip]
    wait_all(5, edge_back_in.at[most])
    edge_back_all[me] = jnp.sum(edge_back_in[...], 0)
    send_all(7, lambda p: edge_back_all.at[me], edge_back_all.at[me])
    wait_all(4, grad_in.at[pl.ds(0, chips - 1)])

    def unmix(u, v, wp, wm):
        return u + v, wp - wm, wp + wm, v - u

    mine = jnp.sum(grad_in[...], 0)
    cc, cs, sc, ss = unmix(mine[0], mine[1], mine[2], mine[3])
    sum_c = jnp.concatenate([cc, cs], 0)[None]
    sum_s = jnp.concatenate([sc, ss], 0)[None]
    back_c = far_c * sum_c + far_s * sum_s
    back_s = far_c * sum_s - far_s * sum_c
    turned = jnp.concatenate([back_c, back_s], 2).reshape(devices * 2 * SUB, 2 * h)
    gathered = product(split(turned), both("wave_x"), flip=True)
    back_rows[...] = gathered.reshape(devices, 2, SUB, rows)
    send_all(6, lambda p: back_rows.at[p], back_in.at[:, pl.ds(me * SUB, SUB), :])
    back_in[:, pl.ds(me * SUB, SUB), :] = back_rows[me]
    wait_all(7, edge_back_all.at[most])

    sums = edge_back_all[9]
    small_at = slice(2 * h + LANES, 2 * h + 2 * LANES)
    result[0:1, small_at] = sums * norming
    sums = jnp.where(lane < sources, sums, 0.0)
    result[1:2, small_at] = share_row * (sums - lane_sum(share_row * sums)) * norming
    result[2:3, small_at] = group_row.astype(F32)

    side_x = unmix(*(edge_back_all[i] for i in range(4)))
    side_y = unmix(*(edge_back_all[4 + i] for i in range(4)))
    corner = unmix(*(lane_sum(jnp.where(lane == i, edge_back_all[8], 0.0)) for i in range(4)))
    far_c, far_s = tab["far"][0, me], tab["far"][1, me]
    near = []
    for c, s in ((side_y[0], side_y[2]), (side_y[1], side_y[3])):
        near.append(jnp.concatenate([far_c * c + far_s * s, far_c * s - far_s * c], 1))
    near = jnp.concatenate(near + [jnp.zeros((SUB - 2, 2 * h), F32)], 0)
    last = product(split(near), both("wave_x"), flip=True)
    edge_c, edge_s = edge_rows[0:1], edge_rows[1:2]
    last_c = last[0:1] + corner[0] * edge_c + corner[2] * edge_s
    last_s = last[1:2] + corner[1] * edge_c + corner[3] * edge_s
    result[:, 2 * h : 2 * h + LANES] = column(last_c) * edge_c + column(last_s) * edge_s
    col_c, col_s = column(edge_c), column(edge_s)

    wait_all(6, back_in.at[:, pl.ds(0, h - SUB), :])
    part_c = back_in[0].T + col_c * side_x[0] + col_s * side_x[2]
    part_s = back_in[1].T + col_c * side_x[1] + col_s * side_x[3]
    result[:, :h] = part_c
    result[:, h : 2 * h] = part_s
    drain(0, rows_in.at[most])
    drain(1, edge_in.at[most])
    drain(2, chunk.at[most])
    drain(3, edge_all.at[most])
    drain(4, grad_in.at[pl.ds(0, chips - 1)])
    drain(5, edge_back_in.at[most])
    drain(6, back_in.at[:, pl.ds(0, h - SUB), :])
    drain(7, edge_back_all.at[most])
    drain(8, pair_in)


def closing(n, sources, result, wave, loss_hbm, grad_hbm, group_hbm, loss, group, out, out_sem):
    block = 2 * LANES
    blocks = n // block
    lane = lax.broadcasted_iota(jnp.int32, (1, LANES), 1)
    h = K // 2
    small = result.at[:, 2 * h + LANES :]
    loss[0] = jnp.sum(jnp.where(lane == sources, small[0:1, :], 0.0))
    for g in range(NG):
        group[g] = jnp.sum(jnp.where(small[2:3, :] == g, small[1:2, :], 0.0))
    stores = [
        pltpu.make_async_copy(loss, loss_hbm, out_sem.at[blocks]),
        pltpu.make_async_copy(group, group_hbm, out_sem.at[blocks + 1]),
    ]
    for store in stores:
        store.start()
    value = result[:, : 2 * h]
    turn = lax.rem(lax.broadcasted_iota(jnp.int32, value.shape, 1), 2) == 0
    pairs = split(value), split(jnp.where(turn, value, -value))
    spread = result[:, 2 * h : 2 * h + LANES]
    adds = jnp.concatenate([spread, spread], 1)
    for b in range(blocks):
        where = slice(b * block, (b + 1) * block)
        side, start = divmod(b * block, n // 2)
        from_where = slice(start, start + block)
        out[:, where] = product(pairs[side], (wave[0, :, from_where], wave[1, :, from_where])) + adds
        stores.append(pltpu.make_async_copy(out.at[:, where], grad_hbm.at[:, where], out_sem.at[b]))
        stores[-1].start()
    for store in stores:
        store.wait()


def fused(devices, mask_field, target_print, source_points, source_groups, group_logits, pupil_radius):
    rows, n = mask_field.shape
    h = K // 2
    coarse = 2 * K
    sources = source_points.shape[0]
    consts = tables(n, rows, devices)
    anywhere = pl.BlockSpec(memory_space=pltpu.HBM)
    vmem = lambda *shape: pltpu.VMEM(shape, F32)
    scratch = [pltpu.VMEM(consts[k].shape, consts[k].dtype) for k in NAMES] + [
        vmem(rows, n), pltpu.VMEM((rows, n), jnp.int32),
        vmem(2, h, rows), vmem(devices, 1, LANES), vmem(devices, 2, SUB, rows), vmem(devices, 1, LANES),
        vmem(devices, 4, SUB, h), vmem(devices, 1, LANES), vmem(4, h + SUB, 2 * h), vmem(4, 2, h, h),
        vmem(4, 2, h, h), vmem(sources, 2 * rows, coarse), vmem(rows, coarse), vmem(rows, coarse),
        vmem(4, 2, h, h), vmem(4, devices // 2, 2, SUB, h), vmem(devices, 1, LANES), vmem(devices // 2, 4, SUB, h),
        vmem(devices, 1, LANES), vmem(devices, 1, LANES), vmem(devices, 2, SUB, rows), vmem(2, h, rows),
        pltpu.VMEM((8, 2, 2 * h, coarse), BF16), pltpu.VMEM((8, 2, 2 * rows, 2 * h), BF16),
        pltpu.VMEM((8, 2, 2 * rows, coarse), BF16), pltpu.VMEM((8, 2 * rows, coarse), BF16),
        vmem(sources, SUB, LANES), vmem(sources, 4, h, h),
        pltpu.SMEM((2, sources), jnp.int32), pltpu.SMEM((sources,), jnp.int32), pltpu.SMEM((NG,), F32),
        pltpu.SMEM((1,), jnp.int32),
        vmem(4, devices // 2, SUB, h), vmem(devices // 2, 4, SUB, h),
        pltpu.VMEM((2, n, coarse), BF16), pltpu.VMEM((2, rows, n), BF16),
        pltpu.SemaphoreType.DMA((26,)),
        pltpu.SemaphoreType.DMA((9,)), pltpu.SemaphoreType.DMA((9,)), pltpu.SemaphoreType.DMA((devices // 2,)),
    ]
    arrays = [jnp.asarray(consts[k]) for k in NAMES]
    hold = lambda value: pltpu.with_memory_space_constraint(value, pltpu.HBM)
    inside = pl.BlockSpec(memory_space=pltpu.VMEM)
    (result,) = pl.pallas_call(
        functools.partial(kernel, devices, n),
        out_shape=(
            jax.ShapeDtypeStruct((rows, 2 * h + 2 * LANES), F32),
        ),
        in_specs=[anywhere] * (6 + len(NAMES)),
        out_specs=(inside,),
        scratch_shapes=scratch,
        compiler_params=pltpu.CompilerParams(
            collective_id=0, has_side_effects=True, vmem_limit_bytes=53 * 1024 * 1024
        ),
    )(*map(hold, (source_points.T, source_groups, group_logits)), pupil_radius,
      *map(hold, (mask_field, target_print, *arrays)))
    return pl.pallas_call(
        functools.partial(closing, n, sources),
        out_shape=(
            jax.ShapeDtypeStruct((1,), F32),
            jax.ShapeDtypeStruct((rows, n), F32),
            jax.ShapeDtypeStruct((NG,), F32),
        ),
        in_specs=[inside] * 2,
        out_specs=(anywhere, anywhere, anywhere),
        scratch_shapes=[
            pltpu.SMEM((1,), F32), pltpu.SMEM((NG,), F32), vmem(rows, n),
            pltpu.SemaphoreType.DMA((n // (2 * LANES) + 2,)),
        ],
        compiler_params=pltpu.CompilerParams(vmem_limit_bytes=8 * 1024 * 1024),
    )(result, arrays[0])


HIGH = lax.Precision.HIGH


def dot(form, left, right):
    return jnp.einsum(form, left, right, precision=HIGH, preferred_element_type=F32)


def waves(left, right, length):
    turns = angles(left, right, length)
    return np.cos(turns), np.sin(turns)


def shifted_waves(count, freq, length, device, devices):
    near = np.stack(waves(np.arange(count), freq, length)).astype(np.float32)
    far = np.stack(waves(np.arange(devices) * count, freq, length)).astype(np.float32)
    far = lax.dynamic_slice_in_dim(jnp.asarray(far), device, 1, axis=1)
    return far[0] * near[0] - far[1] * near[1], far[1] * near[0] + far[0] * near[1]


def exchange(blocks):
    return lax.all_to_all(blocks, "slab", 0, 0)


def plain(devices, mask_field, target_print, source_points, source_groups, group_logits, pupil_radius):
    rows, n = mask_field.shape
    sources = source_points.shape[0]
    coarse = 2 * K
    step = n // coarse
    cols = coarse // devices
    half = n // 2
    device = lax.axis_index("slab")
    freq = np.arange(K, dtype=np.int64) - K // 2
    order = np.concatenate([freq[freq % 2 == 0], freq[freq % 2 == 1]])
    kh = K // 2
    norming = 1.0 / (n * n)

    cos_y, sin_y = waves(np.arange(half), order, n)
    fold = [
        jnp.asarray(np.concatenate([t[:, p * kh : (p + 1) * kh] for t in (cos_y, sin_y)], 1), F32)
        for p in (0, 1)
    ]
    lag = np.mod(np.arange(n)[None, :] - step * np.arange(coarse)[:, None], n)
    response = np.zeros(n)
    for f in range(1, K):
        response += 2.0 * np.cos(2.0 * math.pi * np.mod(f * np.arange(n), n) / n)
    response = (response + 1.0) / coarse
    up = jnp.asarray(response[lag], F32)
    cos_c, sin_c = waves(freq, np.arange(coarse), coarse)
    wave_x = jnp.asarray(np.concatenate([cos_c, sin_c], 1), F32)
    loc_c, loc_s = shifted_waves(rows, freq, n, device, devices)
    loc = jnp.concatenate([loc_c, loc_s], 1)
    a, b = shifted_waves(cols, order, coarse, device, devices)
    lift = jnp.concatenate([jnp.concatenate([a, -b], 1), jnp.concatenate([b, a], 1)], 0)

    cutoff = pupil_radius[0]
    shifted = (source_points - GRID // 2) * cutoff // shift_scale
    first = jnp.asarray(freq, jnp.int32)[None, None, :] + shifted[:, 0, None, None]
    second = jnp.asarray(np.tile(order, 2), jnp.int32)[None, :, None] + shifted[:, 1, None, None]
    passed = first * first + second * second <= cutoff * cutoff

    near, away = mask_field[:, :half], mask_field[:, half:]
    even = dot("xy,yq->xq", near + away, fold[0])
    odd = dot("xy,yq->xq", near - away, fold[1])
    part_c = jnp.concatenate([even[:, :kh], odd[:, :kh]], 1)
    part_s = jnp.concatenate([even[:, kh:], odd[:, kh:]], 1)
    spec = dot("xq,xk->qk", jnp.concatenate([part_c, part_s], 1), loc)
    band = jnp.concatenate([spec[:K, :K] - spec[K:, K:], -(spec[:K, K:] + spec[K:, :K])], 0)
    band = jnp.sum(exchange(band.reshape(devices, 2 * K // devices, K)), 0)
    band = lax.all_gather(band, "slab", tiled=True)

    kept = jnp.where(passed, band[None], 0.0)
    wide = dot("aq,sqk->sak", lift, kept)
    both = dot("ak,kx->ax", wide.reshape(sources * 2 * cols, K), wave_x)
    both = both.reshape(sources, 2, cols, 2 * coarse)
    field_re = (both[:, 0, :, :coarse] - both[:, 1, :, coarse:]) * norming
    field_im = (both[:, 0, :, coarse:] + both[:, 1, :, :coarse]) * norming
    bright = field_re * field_re + field_im * field_im
    onehot = (source_groups[:, None] == jnp.arange(NG, dtype=jnp.int32)[None, :]).astype(F32)
    weights = jnp.exp(jnp.sum(onehot * group_logits[None, :], 1))
    share = weights / jnp.sum(weights)
    image = jnp.sum(share[:, None, None] * bright, 0)

    tall = dot("cm,mx->cx", image, up)
    tall = lax.all_to_all(tall, "slab", 1, 0, tiled=True)
    intensity = dot("cx,cy->xy", tall, up)
    resist = jax.nn.sigmoid(steepness * (intensity - threshold))
    misfit = resist - target_print.astype(F32)
    slope = (2.0 * steepness) * misfit * resist * (1.0 - resist)
    squares = jnp.sum(misfit * misfit)
    down = dot("xy,cy->cx", slope, up)
    down = lax.all_to_all(down, "slab", 0, 1, tiled=True)
    pull = dot("cx,mx->cm", down, up)

    per_source = jnp.sum(bright * pull[None], (1, 2))
    sums = jnp.concatenate([per_source, squares[None]])
    factor = (2.0 * norming) * share[:, None, None] * pull[None]
    back = jnp.stack([factor * field_re, factor * field_im], 1)
    low = dot("ax,kx->ak", back.reshape(sources * 2 * cols, coarse), wave_x[:, :coarse])
    lows = dot("ax,kx->ak", back.reshape(sources * 2 * cols, coarse), wave_x[:, coarse:])
    low = low.reshape(sources, 2, cols, K)
    lows = lows.reshape(sources, 2, cols, K)
    settle = jnp.concatenate([low[:, 0] + lows[:, 1], low[:, 1] - lows[:, 0]], 1)
    settle = dot("aq,sak->sqk", lift, settle)
    grad_band = jnp.sum(jnp.where(passed, settle, 0.0), 0).reshape(devices, 2 * K // devices, K)
    extra = jnp.pad(sums[None, :], ((0, 7), (0, K - sources - 1)))
    extra = jnp.broadcast_to(extra[None], (devices, 8, K))
    grad_band = jnp.sum(exchange(jnp.concatenate([grad_band, extra], 1)), 0)
    sums = grad_band[-8, : sources + 1]
    grad_band = lax.all_gather(grad_band[:-8], "slab", tiled=True)
    per_source, squares = sums[:-1], sums[-1]
    loss_value = (squares * norming).reshape(1)
    against = jnp.sum(share * per_source)
    source_pull = share * (per_source - against)
    group_grad = jnp.sum(onehot * source_pull[:, None], 0) * norming

    spread = dot("tk,qk->tq", jnp.concatenate([loc_c, loc_s], 0), grad_band)
    spread_re = spread[:rows, :K] - spread[rows:, K:]
    spread_im = spread[:rows, K:] + spread[rows:, :K]
    even = dot("xq,yq->xy", jnp.concatenate([spread_re[:, :kh], -spread_im[:, :kh]], 1), fold[0])
    odd = dot("xq,yq->xy", jnp.concatenate([spread_re[:, kh:], -spread_im[:, kh:]], 1), fold[1])
    mask_grad = jnp.concatenate([even + odd, even - odd], 1)
    return loss_value, mask_grad, group_grad


def on_device(devices, mask_field, *others):
    tiles = mask_field.shape[0] == LANES and K // 2 == LANES == SUB * devices and devices % 8 == 0 and devices >= 10
    return (fused if tiles else plain)(devices, mask_field, *others)


def solution(mesh):
    in_specs = (
        P(("clip", "slab"), None),
        P(("clip", "slab"), None),
        P("clip", None),
        P("clip"),
        P("clip"),
        P("clip"),
    )
    out_specs = (P("clip"), P(("clip", "slab"), None), P("clip"))
    return jax.shard_map(
        functools.partial(on_device, mesh.shape["slab"]),
        mesh=mesh, in_specs=in_specs, out_specs=out_specs, check_vma=False,
    )
```
